256 devices in a mesh: col: 32 (over z, y), row: 8 (over x, core).
Axes of the slice: x: 4, y: 4, z: 8, core: 2. Of those that a mesh axis runs over, the one named last changes fastest.
Arguments:
- mask: int32 [32768, 8192], P('row', 'col')
- user_emb: bfloat16 [32768, 256], P(('row', 'col'))
- item_emb: bfloat16 [8192, 256], P(('col', 'row'))
- queries: int32 [1024], replicated
Outputs:
- output 1: bfloat16 [32768, 256], P(('row', 'col'))
- output 2: bfloat16 [8192, 256], P(('col', 'row'))
- output 3: float32 [1024, 8192], P(None, ('col', 'row'))
All inputs are finite; a program needn't handle non-finite values.
Results may differ from the reference program's by a relative error of at most 0.00644127.
Values are sent between devices in bfloat16 or wider.
A program may use at most 768 MiB of HBM per device.

```python
import jax
import jax.numpy as jnp
from jax import lax

USERS = 32768
ITEMS = 8192
EMB = 256
LAYERS = 3
QUERIES = 1024


def draw_mask(key):
    k_noise, k_rows, k_cols = jax.random.split(key, 3)
    row_level = jax.random.randint(k_rows, (USERS,), 4, 33)
    col_level = jax.random.randint(k_cols, (ITEMS,), 4, 33)
    noise = jax.random.randint(k_noise, (USERS, ITEMS), 0, 1024)
    return (noise < row_level[:, None] * col_level[None, :]).astype(jnp.int32)


def setup_inputs(seed: int = 0) -> dict:
    key = jax.random.key(seed)
    k_mask, k_user, k_item, k_umean, k_imean, k_query = jax.random.split(key, 6)
    scale = EMB ** -0.25
    user_mean = jax.random.normal(k_umean, (EMB,), jnp.float32)
    item_mean = jax.random.normal(k_imean, (EMB,), jnp.float32)
    user_emb = ((jax.random.normal(k_user, (USERS, EMB), jnp.float32) + user_mean[None, :]) * scale).astype(jnp.bfloat16)
    item_emb = ((jax.random.normal(k_item, (ITEMS, EMB), jnp.float32) + item_mean[None, :]) * scale).astype(jnp.bfloat16)
    queries = jax.random.randint(k_query, (QUERIES,), 0, USERS).astype(jnp.int32)
    return {'mask': draw_mask(k_mask), 'user_emb': user_emb, 'item_emb': item_emb, 'queries': queries}


def norm_adjacency(mask):
    deg_user = jnp.maximum(jnp.sum(mask, axis=1), 1)
    deg_item = jnp.maximum(jnp.sum(mask, axis=0), 1)
    inv_user = lax.rsqrt(deg_user.astype(jnp.float32))
    inv_item = lax.rsqrt(deg_item.astype(jnp.float32))
    return (inv_user[:, None] * mask.astype(jnp.float32) * inv_item[None, :]).astype(jnp.bfloat16)


def reference(mask, user_emb, item_emb, queries):
    norm_adj = norm_adjacency(mask)

    def one_layer(carried, unused):
        user_cur, item_cur, user_sum, item_sum = carried
        user_next = jnp.dot(norm_adj, item_cur, preferred_element_type=jnp.float32).astype(jnp.bfloat16)
        item_next = lax.dot_general(norm_adj, user_cur, (((0,), (0,)), ((), ())), preferred_element_type=jnp.float32).astype(jnp.bfloat16)
        return (user_next, item_next, user_sum + user_next.astype(jnp.float32), item_sum + item_next.astype(jnp.float32)), None

    start_state = (user_emb, item_emb, user_emb.astype(jnp.float32), item_emb.astype(jnp.float32))
    end_state, unused_out = lax.scan(one_layer, start_state, None, length=LAYERS)
    final_user = (end_state[2] / (LAYERS + 1)).astype(jnp.bfloat16)
    final_item = (end_state[3] / (LAYERS + 1)).astype(jnp.bfloat16)
    picked = jnp.take(final_user, queries, axis=0)
    scores = lax.dot_general(picked, final_item, (((1,), (1,)), ((), ())), preferred_element_type=jnp.float32)
    return final_user, final_item, scores
```

```python
import jax
import jax.numpy as jnp
from jax import lax
from jax.experimental import pallas as pl
from jax.experimental.pallas import tpu as pltpu
from jax.sharding import PartitionSpec as P

LAYERS = 3
Z, Y, R = 8, 4, 8
G = Y * R
UB, IB = 128, 32
E = 256
NQ = 1024
QB = NQ // G
H = UB // 2
F32, BF16 = jnp.float32, jnp.bfloat16
MESH = pl.DeviceIdType.MESH
CONTRACT_ROWS = (((0,), (0,)), ((), ()))
CONTRACT_LANES = (((1,), (1,)), ((), ()))


def remote(src, dst, send_sem, recv_sem, col, row):
    return pltpu.make_async_remote_copy(src_ref=src, dst_ref=dst, send_sem=send_sem, recv_sem=recv_sem,
                                        device_id=(col, row), device_id_type=MESH)


def wait_bytes(ref, sem):
    pltpu.make_async_copy(ref, ref, sem).wait()


def kernel(mask_ref, user_ref, item_ref, query_ref, fu_ref, fi_ref, sc_ref,
           mask_v, msend, mrecv, adj, rs_send, rs_recv, cs_send, cs_recv, invu, invi,
           eu_pan, ei_pan, up, us, ur, ip, ir, qs, qr, qz, qzs, qall, usum, isum,
           load_sem, mask_ssem, mask_rsem, rs_ssem, rs_rsem, cs_ssem, cs_rsem,
           eu0_ssem, eu0_rsem, ei_ssem, ei_rsem, us_ssem, us_rsem, ip_ssem, ip_rsem,
           ag_ssem, ag_rsem, q_ssem, q_rsem):
    col = lax.axis_index('col')
    row = lax.axis_index('row')
    z, y = lax.div(col, Y), lax.rem(col, Y)
    me = y * R + row

    def zat(d):
        return lax.rem(z + (d % Z), Z)

    def plane():
        for slot in range(1, G):
            py = lax.rem(y + slot // R, Y)
            pr = lax.rem(row + slot % R, R)
            yield slot - 1, py, pr, py * R + pr

    order = [4, 3, -3, 2, -2, 1, -1, 0]

    barrier = pltpu.get_barrier_semaphore()
    for d in range(1, Z * Y):
        pl.semaphore_signal(barrier, inc=1, device_id=(lax.rem(col + d, Z * Y), row), device_id_type=MESH)
    for slot, py, pr, g in plane():
        if (slot + 1) % R:
            pl.semaphore_signal(barrier, inc=1, device_id=(z * Y + py, pr), device_id_type=MESH)

    loads = []
    for j, d in enumerate(order):
        zc = zat(d)
        load = pltpu.make_async_copy(mask_ref.at[pl.ds(zc * (Y * UB), Y * UB)], mask_v.at[j], load_sem.at[j])
        load.start()
        loads.append(load)
    ones_w = jnp.ones((8, E), BF16)
    ones_h = jnp.ones((8, UB), BF16)
    cs_send[...] = jnp.zeros_like(cs_send)
    for j, d in enumerate(order):
        zc = zat(d)
        loads[j].wait()
        for p in range(Y):
            block = mask_v[j, p * UB:(p + 1) * UB, :].astype(F32).astype(BF16)
            msend[p, j] = block
            sums = lax.dot_general(ones_w, block, CONTRACT_LANES, preferred_element_type=F32)
            rs_send[p, pl.ds(zc, 1), :] = sums[0:1]
            cs_send[...] += jnp.dot(ones_h, block, preferred_element_type=F32)
    cs_recv[me] = cs_send[...]
    eu_pan[0, z] = user_ref[...]
    ei_pan[0, me] = item_ref[...]

    pl.semaphore_wait(barrier, 31 + 28)

    for d in range(1, Z * Y):
        pc = lax.rem(col + d, Z * Y)
        remote(rs_send.at[lax.rem(pc, Y)], rs_recv.at[d - 1], rs_ssem, rs_rsem, pc, row).start()
    for slot, py, pr, g in plane():
        remote(cs_send, cs_recv.at[me], cs_ssem, cs_rsem, z * Y + py, pr).start()
    for slot, py, pr, g in plane():
        remote(item_ref, ei_pan.at[0, me], ei_ssem.at[0], ei_rsem.at[0], z * Y + py, pr).start()
    for d in range(1, Z):
        remote(user_ref, eu_pan.at[0, z], eu0_ssem, eu0_rsem, zat(d) * Y + y, row).start()
    for j in range(Z):
        for d in range(1, Y):
            py = lax.rem(y + d, Y)
            remote(msend.at[py, j], mrecv.at[j, d - 1], mask_ssem, mask_rsem.at[j], z * Y + py, row).start()

    wait_bytes(rs_recv, rs_rsem)
    deg = rs_send[y]
    for d in range(Z * Y - 1):
        deg = deg + rs_recv[d]
    invu[...] = lax.rsqrt(jnp.maximum(deg, 1.0))
    wait_bytes(cs_recv.at[pl.ds(0, G - 1)], cs_rsem)
    for s in range(Y):
        deg = cs_recv[s * R]
        for r in range(1, R):
            deg = deg + cs_recv[s * R + r]
        invi[s] = lax.rsqrt(jnp.maximum(deg, 1.0))

    def make_adj(j, zc):
        wait_bytes(mrecv.at[j], mask_rsem.at[j])
        iu = jnp.broadcast_to(invu[pl.ds(zc, 1), :], (UB, UB)).T
        iu = jnp.concatenate([iu, iu], axis=1)
        for d in range(Y):
            s = lax.rem(y + (Y - d), Y)
            m = (msend[y, j] if d == 0 else mrecv[j, d - 1]).astype(F32)
            adj[s, zc] = ((iu * m) * invi[s][0:1, :]).astype(BF16)

    def user_piece(k, j):
        zc = zat(order[j])
        if k == 0:
            make_adj(j, zc)
        acc = None
        for s in range(Y):
            t = jnp.dot(adj[s, zc], ei_pan[k, s * R:(s + 1) * R].reshape(R * IB, E), preferred_element_type=F32)
            acc = t if acc is None else acc + t
        up[j] = acc

    piece_of = {d: j for j, d in enumerate(order)}
    right, left = zat(1) * Y + y, zat(-1) * Y + y

    def item_parts(k):
        eu = eu_pan[k].reshape(Z * UB, E)
        for s in range(Y):
            part = lax.dot_general(adj[s].reshape(Z * UB, E), eu, CONTRACT_ROWS, preferred_element_type=F32)
            ip[k, s * R:(s + 1) * R] = part.reshape(R, IB, E)
        for slot, py, pr, g in plane():
            remote(ip.at[k, g], ir.at[k, slot], ip_ssem.at[k], ip_rsem.at[k], z * Y + py, pr).start()

    def item_total(k):
        wait_bytes(ir.at[k], ip_rsem.at[k])
        total = ip[k, me]
        for slot in range(G - 1):
            total = total + ir[k, slot]
        return total

    def user_total(k, before_last):
        def send(way, step, c):
            rows = pl.ds(c * H, H)
            remote(us.at[k, way, step, rows], ur.at[k, way, step, rows], us_ssem.at[k], us_rsem.at[k, way, step, c],
                   right if way == 0 else left, row).start()

        def got(way, step, c):
            rows = pl.ds(c * H, H)
            wait_bytes(ur.at[k, way, step, rows], us_rsem.at[k, way, step, c])
            return ur[k, way, step, c * H:(c + 1) * H]

        def own(way, step, c):
            j = piece_of[4 - step] if way == 0 or step == 0 else piece_of[step - 4]
            return up[j, c * H:(c + 1) * H]

        def emit(way, step, c, first):
            value = own(way, step, c)
            if not first:
                value = value + got(way, step - 1, c)
            us[k, way, step, c * H:(c + 1) * H] = value
            send(way, step, c)

        user_piece(k, 0)
        emit(0, 0, 0, True)
        emit(1, 0, 1, True)
        user_piece(k, 1)
        emit(0, 1, 1, True)
        user_piece(k, 2)
        emit(1, 1, 0, True)
        for step in range(1, 4):
            emit(0, step, 0, False)
            emit(1, step, 1, False)
            if step < 3:
                user_piece(k, 2 * step + 1)
                user_piece(k, 2 * step + 2)
                emit(0, step + 1, 1, False)
                emit(1, step + 1, 0, False)
        user_piece(k, 7)
        before_last()
        halves = []
        for c in range(2):
            halves.append(up[7, c * H:(c + 1) * H] + got(0, 3, c) + got(1, 3, c))
        return jnp.concatenate(halves, axis=0)

    def gather_user(k):
        def send(way, step, c):
            src = eu_pan.at[k, zat(-step if way == 0 else step), pl.ds(c * H, H)]
            remote(src, src, ag_ssem.at[k], ag_rsem.at[k, way, step, c], right if way == 0 else left, row).start()

        def got(way, step, c):
            dst = eu_pan.at[k, zat(-step - 1 if way == 0 else step + 1), pl.ds(c * H, H)]
            wait_bytes(dst, ag_rsem.at[k, way, step, c])

        def begin():
            for c in range(2):
                send(0, 0, c)
                send(1, 0, 1 - c)

        def rest():
            for step in range(3):
                for c in range(2):
                    for way in range(2):
                        cc = c if way == 0 else 1 - c
                        got(way, step, cc)
                        if step < 2 or c == 0:
                            send(way, step + 1, cc)
            got(0, 3, 0)
            got(1, 3, 1)

        return begin, rest

    usum[...] = user_ref[...].astype(F32)
    isum[...] = item_ref[...].astype(F32)
    wait_bytes(ei_pan.at[0, pl.ds(0, G - 1)], ei_rsem.at[0])

    for k in range(LAYERS):
        if k == 0:
            def start_items():
                wait_bytes(eu_pan.at[0, pl.ds(0, Z - 1)], eu0_rsem)
                item_parts(0)
            new_user = user_total(k, start_items).astype(BF16)
        else:
            item_parts(k)
            wait_bytes(ei_pan.at[k, pl.ds(0, G - 1)], ei_rsem.at[k])
            new_user = user_total(k, lambda: None).astype(BF16)
        usum[...] += new_user.astype(F32)
        if k + 1 < LAYERS:
            eu_pan[k + 1, z] = new_user
            begin, rest = gather_user(k + 1)
            begin()
            new_item = item_total(k).astype(BF16)
            isum[...] += new_item.astype(F32)
            ei_pan[k + 1, me] = new_item
            for slot, py, pr, g in plane():
                own = ei_pan.at[k + 1, me]
                remote(own, own, ei_ssem.at[k + 1], ei_rsem.at[k + 1], z * Y + py, pr).start()
            rest()

    final_user = (usum[...] / (LAYERS + 1)).astype(BF16)
    fu_ref[...] = final_user

    base = (row * (Z * Y) + col) * UB
    ids = lax.broadcasted_iota(jnp.int32, (UB, NQ), 0) + base
    hot = jnp.where(ids == query_ref[...], 1.0, 0.0).astype(BF16)
    qs[...] = lax.dot_general(hot, final_user, CONTRACT_ROWS, preferred_element_type=F32).astype(BF16).reshape(G, QB, E)
    for slot, py, pr, g in plane():
        remote(qs.at[g], qr.at[slot], q_ssem.at[0], q_rsem.at[0], z * Y + py, pr).start()

    new_item = item_total(LAYERS - 1).astype(BF16)
    final_item = ((isum[...] + new_item.astype(F32)) / (LAYERS + 1)).astype(BF16)
    fi_ref[...] = final_item

    wait_bytes(qr, q_rsem.at[0])
    total = qs[me].astype(F32)
    for slot in range(G - 1):
        total = total + qr[slot].astype(F32)
    qzs[...] = total.astype(BF16)
    for d in range(1, Z):
        remote(qzs, qz.at[d - 1], q_ssem.at[1], q_rsem.at[1], zat(d) * Y + y, row).start()
    wait_bytes(qz, q_rsem.at[1])
    for d in range(Z - 1):
        total = total + qz[d].astype(F32)
    qall[me] = total.astype(BF16)
    for slot, py, pr, g in plane():
        remote(qall.at[me], qall.at[me], q_ssem.at[2], q_rsem.at[2], z * Y + py, pr).start()
    wait_bytes(qall.at[pl.ds(0, G - 1)], q_rsem.at[2])
    sc_ref[...] = lax.dot_general(qall[...].reshape(NQ, E), final_item, CONTRACT_LANES, preferred_element_type=F32)

    wait_bytes(rs_recv, rs_ssem)
    wait_bytes(cs_recv.at[pl.ds(0, G - 1)], cs_ssem)
    wait_bytes(eu_pan.at[0, pl.ds(0, Z - 1)], eu0_ssem)
    wait_bytes(msend.at[pl.ds(0, Y - 1)], mask_ssem)
    for k in range(LAYERS):
        wait_bytes(ei_pan.at[k, pl.ds(0, G - 1)], ei_ssem.at[k])
        wait_bytes(ir.at[k], ip_ssem.at[k])
        wait_bytes(up.at[pl.ds(0, 7)], us_ssem.at[k])
        if k:
            wait_bytes(eu_pan.at[k, pl.ds(0, 7)], ag_ssem.at[k])
    wait_bytes(qr, q_ssem.at[0])
    wait_bytes(qz, q_ssem.at[1])
    wait_bytes(qall.at[pl.ds(0, G - 1)], q_ssem.at[2])


def propagate(mask, user, item, queries):
    dma = pltpu.SemaphoreType.DMA
    vmem = pl.BlockSpec(memory_space=pltpu.VMEM)
    L = LAYERS
    return pl.pallas_call(
        kernel,
        out_shape=(jax.ShapeDtypeStruct((UB, E), BF16), jax.ShapeDtypeStruct((IB, E), BF16),
                   jax.ShapeDtypeStruct((NQ, IB), F32)),
        in_specs=[pl.BlockSpec(memory_space=pl.ANY), vmem, vmem, vmem],
        out_specs=(vmem, vmem, vmem),
        scratch_shapes=[
            pltpu.VMEM((Z, Y * UB, E), jnp.int32),
            pltpu.VMEM((Y, Z, UB, E), BF16),
            pltpu.VMEM((Z, Y - 1, UB, E), BF16),
            pltpu.VMEM((Y, Z, UB, E), BF16),
            pltpu.VMEM((Y, Z, UB), F32),
            pltpu.VMEM((Z * Y - 1, Z, UB), F32),
            pltpu.VMEM((8, E), F32),
            pltpu.VMEM((G, 8, E), F32),
            pltpu.VMEM((Z, UB), F32),
            pltpu.VMEM((Y, 8, E), F32),
            pltpu.VMEM((L, Z, UB, E), BF16),
            pltpu.VMEM((L, G, IB, E), BF16),
            pltpu.VMEM((Z, UB, E), F32),
            pltpu.VMEM((L, 2, 4, UB, E), F32),
            pltpu.VMEM((L, 2, 4, UB, E), F32),
            pltpu.VMEM((L, G, IB, E), F32),
            pltpu.VMEM((L, G - 1, IB, E), F32),
            pltpu.VMEM((G, QB, E), BF16),
            pltpu.VMEM((G - 1, QB, E), BF16),
            pltpu.VMEM((Z - 1, QB, E), BF16),
            pltpu.VMEM((QB, E), BF16),
            pltpu.VMEM((G, QB, E), BF16),
            pltpu.VMEM((UB, E), F32),
            pltpu.VMEM((IB, E), F32),
            dma((Z,)), dma, dma((Z,)), dma, dma, dma, dma,
            dma, dma, dma((L,)), dma((L,)), dma((L,)), dma((L, 2, 4, 2)), dma((L,)), dma((L,)),
            dma((L,)), dma((L, 2, 4, 2)), dma((3,)), dma((3,)),
        ],
        compiler_params=pltpu.CompilerParams(collective_id=0, has_side_effects=True, vmem_limit_bytes=60 * 2**20),
    )(mask, user, item, queries.reshape(1, NQ))


def solution(mesh):
    return jax.shard_map(propagate, mesh=mesh,
                         in_specs=(P('row', 'col'), P(('row', 'col'), None), P(('col', 'row'), None), P()),
                         out_specs=(P(('row', 'col'), None), P(('col', 'row'), None), P(None, ('col', 'row'))),
                         check_vma=False)
```

```python
import jax
import jax.numpy as jnp
from jax import lax
from jax.experimental import pallas as pl
from jax.experimental.pallas import tpu as pltpu
from jax.sharding import PartitionSpec as P

LAYERS = 3
Z, Y, X = 8, 4, 4
R = 2 * X
G = Y * R
UB, IB = 128, 32
E = 256
NQ = 1024
QB = NQ // G
H = UB // 2
F32, BF16 = jnp.float32, jnp.bfloat16
MESH = pl.DeviceIdType.MESH
CONTRACT_ROWS = (((0,), (0,)), ((), ()))
CONTRACT_LANES = (((1,), (1,)), ((), ()))


def remote(src, dst, send_sem, recv_sem, col, row):
    return pltpu.make_async_remote_copy(src_ref=src, dst_ref=dst, send_sem=send_sem, recv_sem=recv_sem,
                                        device_id=(col, row), device_id_type=MESH)


def wait_bytes(ref, sem):
    pltpu.make_async_copy(ref, ref, sem).wait()


def kernel(mask_ref, user_ref, item_ref, query_ref, fu_ref, fi_ref, sc_ref,
           mask_v, msend, mrecv, adj, adjt, rs_send, rs_recv, cs_send, cs_recv, invu, invi,
           eu_pan, ei_pan, up, us, ur, ip, pr, iq, ir, hot, qs, qp, qt, qr, qz, qzs, qall, usum, isum,
           load_sem, mask_ssem, mask_rsem, rs_ssem, rs_rsem, cs_ssem, cs_rsem,
           eu0_ssem, eu0_rsem, ei_ssem, ei_rsem, fw_ssem, fw_rsem, us_ssem, us_rsem,
           pr_ssem, pr_rsem, ip_ssem, ip_rsem, ag_ssem, ag_rsem, q_ssem, q_rsem, qg_rsem, qf_rsem):
    col = lax.axis_index('col')
    row = lax.axis_index('row')
    z, y = lax.div(col, Y), lax.rem(col, Y)
    x, c = lax.div(row, 2), lax.rem(row, 2)
    other = 1 - c
    partner = x * 2 + other
    me = y * R + row
    spot = y * X + x

    def zat(d):
        return lax.rem(z + (d % Z), Z)

    def yat(d):
        return lax.rem(y + (d % Y), Y)

    def plane():
        for dy in (2, 1, 3, 0):
            for dx in (2, 1, 3, 0):
                if dy or dx:
                    yield dy * X + dx - 1, dy, yat(dy), lax.rem(x + dx, X)

    order = [4, 3, -3, 2, -2, 1, -1, 0]
    piece_of = {d: j for j, d in enumerate(order)}
    right, left = zat(1) * Y + y, zat(-1) * Y + y

    loads = []
    for j, d in enumerate(order):
        zc = zat(d)
        load = pltpu.make_async_copy(mask_ref.at[pl.ds(zc * (Y * UB), Y * UB)], mask_v.at[j], load_sem.at[j])
        load.start()
        loads.append(load)

    barrier = pltpu.get_barrier_semaphore()
    for d in range(1, Z * Y):
        pl.semaphore_signal(barrier, inc=1, device_id=(lax.rem(col + d, Z * Y), row), device_id_type=MESH)
    for dy in range(Y):
        for dr in range(1, R):
            pl.semaphore_signal(barrier, inc=1, device_id=(z * Y + yat(dy), lax.rem(row + dr, R)), device_id_type=MESH)

    ones_w = jnp.ones((8, E), BF16)
    colsum = jnp.zeros((8, E), F32)
    for j, d in enumerate(order):
        zc = zat(d)
        loads[j].wait()
        for p in range(Y):
            wide = mask_v[j, p * UB:(p + 1) * UB, :].astype(F32)
            block = wide.astype(BF16)
            msend[p, j] = block
            sums = lax.dot_general(ones_w, block, CONTRACT_LANES, preferred_element_type=F32)
            rs_send[p, pl.ds(zc, 1), :] = sums[0:1]
            colsum = colsum + jnp.sum(wide.reshape(UB // 8, 8, E), axis=0)
    cs_send[...] = jnp.sum(colsum, axis=0, keepdims=True)
    cs_recv[me] = cs_send[...]
    eu_pan[0, z] = user_ref[...]
    ei_pan[0, c, spot] = item_ref[...]

    pl.semaphore_wait(barrier, 31 + 28)

    for dy in range(Y):
        for dr in range(R):
            if dy or dr:
                remote(cs_send, cs_recv.at[me], cs_ssem, cs_rsem, z * Y + yat(dy), lax.rem(row + dr, R)).start()
    for d in range(1, Z * Y):
        pc = lax.rem(col + d, Z * Y)
        remote(rs_send.at[lax.rem(pc, Y)], rs_recv.at[d - 1], rs_ssem, rs_rsem, pc, row).start()
    for slot, dy, py, px in plane():
        remote(item_ref, ei_pan.at[0, c, spot], ei_ssem.at[0], ei_rsem.at[0, dy], z * Y + py, px * 2 + c).start()
    for d in range(1, Z):
        remote(user_ref, eu_pan.at[0, z], eu0_ssem, eu0_rsem, zat(d) * Y + y, row).start()
    for j in range(Z):
        for d in range(1, Y):
            py = yat(d)
            remote(msend.at[py, j], mrecv.at[j, d - 1], mask_ssem, mask_rsem.at[j], z * Y + py, row).start()

    usum[...] = user_ref[...].astype(F32)
    isum[...] = item_ref[...].astype(F32)
    base = (row * (Z * Y) + col) * UB
    ids = lax.broadcasted_iota(jnp.int32, (UB, NQ), 0) + base
    hot[...] = jnp.where(ids == query_ref[...], 1.0, 0.0).T.astype(BF16)

    wait_bytes(cs_recv.at[pl.ds(0, G - 1)], cs_rsem)
    for s in range(Y):
        deg = cs_recv[s * R]
        for r in range(1, R):
            deg = deg + cs_recv[s * R + r]
        invi[s] = lax.rsqrt(jnp.maximum(deg, 1.0))
    wait_bytes(rs_recv, rs_rsem)
    deg = rs_send[y]
    for d in range(Z * Y - 1):
        deg = deg + rs_recv[d]
    invu[...] = lax.rsqrt(jnp.maximum(deg, 1.0))

    def make_adj(j, zc):
        wait_bytes(mrecv.at[j], mask_rsem.at[j])
        iu = jnp.broadcast_to(invu[pl.ds(zc, 1), :], (UB, UB)).T
        iu = jnp.concatenate([iu, iu], axis=1)
        for d in range(Y):
            s = yat(-d)
            m = (msend[y, j] if d == 0 else mrecv[j, d - 1]).astype(F32)
            a = (iu * m) * invi[s]
            adj[s, zc] = a.astype(BF16)
            adjt[s, :, pl.ds(pl.multiple_of(zc * UB, UB), UB)] = a.T.astype(BF16)

    def user_piece(k, j):
        zc = zat(order[j])
        if k == 0:
            make_adj(j, zc)
        acc = None
        for s in range(Y):
            panel = jnp.concatenate([ei_pan[k, cc, s * X + xx] for xx in range(X) for cc in range(2)], axis=0)
            t = jnp.dot(adj[s, zc], panel, preferred_element_type=F32)
            acc = t if acc is None else acc + t
        up[j] = acc

    def item_parts(k):
        eu = eu_pan[k].reshape(Z * UB, E)
        for j, dy in enumerate((2, 1, 3, 0)):
            s = yat(dy)
            part = jnp.dot(adjt[s], eu, preferred_element_type=F32).reshape(X, 2, IB, E)
            for xx in range(X):
                for cc in range(2):
                    ip[k, cc, s * X + xx] = part[xx, cc]
            remote(ip.at[k, other, pl.ds(s * X, X)], pr.at[k, j], pr_ssem.at[k], pr_rsem.at[k, j], col, partner).start()
        for j, dy in enumerate((2, 1, 3, 0)):
            s = yat(dy)
            wait_bytes(pr.at[k, j], pr_rsem.at[k, j])
            iq[k, pl.ds(s * X, X)] = ip[k, c, pl.ds(s * X, X)] + pr[k, j]
            for slot, dy2, py, px in plane():
                if dy2 == dy:
                    remote(iq.at[k, s * X + px], ir.at[k, slot], ip_ssem.at[k], ip_rsem.at[k], z * Y + py, px * 2 + c).start()

    def item_total(k):
        wait_bytes(ir.at[k], ip_rsem.at[k])
        total = iq[k, spot]
        for slot in range(G // 2 - 1):
            total = total + ir[k, slot]
        return total

    def gather_plane(pan, ssem, rsem):
        for slot, dy, py, px in plane():
            remote(pan.at[c, spot], pan.at[c, spot], ssem, rsem.at[dy], z * Y + py, px * 2 + c).start()

    def forward_plane(pan, rsem, fssem, frsem):
        for dy in (0, 1, 3, 2):
            n = X - 1 if dy == 0 else X
            rows = pl.ds(yat(-dy) * X, X)
            wait_bytes(pan.at[c, pl.ds(0, n)], rsem.at[dy])
            remote(pan.at[c, rows], pan.at[c, rows], fssem, frsem.at[dy], col, partner).start()

    def wait_plane(pan, frsem):
        for dy in (0, 1, 3, 2):
            wait_bytes(pan.at[other, pl.ds(yat(-dy) * X, X)], frsem.at[dy])

    def user_total(k, hooks):
        def send(way, step, h):
            rows = pl.ds(h * H, H)
            remote(us.at[k, way, step, rows], ur.at[k, way, step, rows], us_ssem.at[k], us_rsem.at[k, way, step, h],
                   right if way == 0 else left, row).start()

        def got(way, step, h):
            rows = pl.ds(h * H, H)
            wait_bytes(ur.at[k, way, step, rows], us_rsem.at[k, way, step, h])
            return ur[k, way, step, h * H:(h + 1) * H]

        def emit(way, step, h, first):
            j = piece_of[4 - step] if way == 0 or step == 0 else piece_of[step - 4]
            value = up[j, h * H:(h + 1) * H]
            if not first:
                value = value + got(way, step - 1, h)
            us[k, way, step, h * H:(h + 1) * H] = value
            send(way, step, h)

        user_piece(k, 0)
        emit(0, 0, 0, True)
        emit(1, 0, 1, True)
        user_piece(k, 1)
        emit(0, 1, 1, True)
        user_piece(k, 2)
        emit(1, 1, 0, True)
        for step in range(1, 4):
            if step < 3:
                user_piece(k, 2 * step + 1)
                user_piece(k, 2 * step + 2)
            else:
                user_piece(k, 7)
            emit(0, step, 0, False)
            emit(1, step, 1, False)
            if step < 3:
                emit(0, step + 1, 1, False)
                emit(1, step + 1, 0, False)
            if step in hooks:
                hooks[step]()
        halves = []
        for h in range(2):
            halves.append(up[7, h * H:(h + 1) * H] + got(0, 3, h) + got(1, 3, h))
        new_user = jnp.concatenate(halves, axis=0).astype(BF16)
        usum[...] += new_user.astype(F32)
        return new_user

    def gather_user(k):
        def send(way, step, h):
            src = eu_pan.at[k, zat(-step if way == 0 else step), pl.ds(h * H, H)]
            remote(src, src, ag_ssem.at[k], ag_rsem.at[k, way, step, h], right if way == 0 else left, row).start()

        def got(way, step, h):
            dst = eu_pan.at[k, zat(-step - 1 if way == 0 else step + 1), pl.ds(h * H, H)]
            wait_bytes(dst, ag_rsem.at[k, way, step, h])

        def begin(new_user):
            eu_pan[k, z] = new_user
            for h in range(2):
                send(0, 0, h)
                send(1, 0, 1 - h)

        def hop(step):
            for h in range(2):
                for way in range(2):
                    hh = h if way == 0 else 1 - h
                    got(way, step, hh)
                    if step < 2 or h == 0:
                        send(way, step + 1, hh)

        def last():
            got(0, 3, 0)
            got(1, 3, 1)

        return begin, hop, last

    def items_next(k):
        new_item = item_total(k).astype(BF16)
        isum[...] += new_item.astype(F32)
        ei_pan[k + 1, c, spot] = new_item
        gather_plane(ei_pan.at[k + 1], ei_ssem.at[k + 1], ei_rsem.at[k + 1])

    def items_forward(k):
        forward_plane(ei_pan.at[k], ei_rsem.at[k], fw_ssem.at[k], fw_rsem.at[k])

    def items_wait(k):
        wait_plane(ei_pan.at[k], fw_rsem.at[k])

    items_forward(0)
    items_wait(0)
    new_user = user_total(0, {})
    begin1, hop1, last1 = gather_user(1)
    begin1(new_user)
    wait_bytes(eu_pan.at[0, pl.ds(0, Z - 1)], eu0_rsem)
    item_parts(0)
    for step in range(3):
        hop1(step)
    last1()
    item_parts(1)
    items_next(0)
    items_forward(1)
    items_wait(1)
    new_user = user_total(1, {2: lambda: items_next(1), 3: lambda: items_forward(2)})
    begin2, hop2, last2 = gather_user(2)
    begin2(new_user)
    items_wait(2)
    new_user = user_total(2, {1: lambda: hop2(0), 2: lambda: hop2(1), 3: lambda: hop2(2)})
    final_user = (usum[...] / (LAYERS + 1)).astype(BF16)
    fu_ref[...] = final_user

    qs[...] = jnp.dot(hot[...], final_user, preferred_element_type=F32).astype(BF16).reshape(2, G // 2, QB, E)
    to_partner = remote(qs.at[other], qp, q_ssem.at[0], q_rsem.at[0], col, partner)
    to_partner.start()
    last2()
    item_parts(2)
    to_partner.wait_recv()
    qt[...] = (qs[c].astype(F32) + qp[...].astype(F32)).astype(BF16)
    for slot, dy, py, px in plane():
        remote(qt.at[py * X + px], qr.at[slot], q_ssem.at[1], q_rsem.at[1], z * Y + py, px * 2 + c).start()
    wait_bytes(qr, q_rsem.at[1])
    total = qt[spot].astype(F32)
    for slot in range(G // 2 - 1):
        total = total + qr[slot].astype(F32)
    qzs[...] = total.astype(BF16)
    for d in (4, 3, 5, 2, 6, 1, 7):
        remote(qzs, qz.at[d - 1], q_ssem.at[2], q_rsem.at[2], zat(d) * Y + y, row).start()
    new_item = item_total(2).astype(BF16)
    final_item = ((isum[...] + new_item.astype(F32)) / (LAYERS + 1)).astype(BF16)
    fi_ref[...] = final_item
    wait_bytes(qz, q_rsem.at[2])
    for d in range(Z - 1):
        total = total + qz[d].astype(F32)
    qall[c, spot] = total.astype(BF16)
    gather_plane(qall, q_ssem.at[3], qg_rsem)
    forward_plane(qall, qg_rsem, q_ssem.at[4], qf_rsem)
    wait_plane(qall, qf_rsem)
    sc_ref[...] = lax.dot_general(qall[...].reshape(NQ, E), final_item, CONTRACT_LANES, preferred_element_type=F32)

    wait_bytes(rs_recv, rs_ssem)
    wait_bytes(cs_recv.at[pl.ds(0, G - 1)], cs_ssem)
    wait_bytes(eu_pan.at[0, pl.ds(0, Z - 1)], eu0_ssem)
    wait_bytes(msend.at[pl.ds(0, Y - 1)], mask_ssem)
    for k in range(LAYERS):
        wait_bytes(ei_pan.at[k, 0, pl.ds(0, G // 2 - 1)], ei_ssem.at[k])
        wait_bytes(ei_pan.at[k, 0], fw_ssem.at[k])
        wait_bytes(pr.at[k], pr_ssem.at[k])
        wait_bytes(ir.at[k], ip_ssem.at[k])
        wait_bytes(up.at[pl.ds(0, 7)], us_ssem.at[k])
        if k:
            wait_bytes(eu_pan.at[k, pl.ds(0, 7)], ag_ssem.at[k])
    to_partner.wait_send()
    wait_bytes(qr, q_ssem.at[1])
    wait_bytes(qz, q_ssem.at[2])
    wait_bytes(qr, q_ssem.at[3])
    wait_bytes(qt, q_ssem.at[4])


def propagate(mask, user, item, queries):
    dma = pltpu.SemaphoreType.DMA
    vmem = pl.BlockSpec(memory_space=pltpu.VMEM)
    L, N = LAYERS, G // 2
    return pl.pallas_call(
        kernel,
        out_shape=(jax.ShapeDtypeStruct((UB, E), BF16), jax.ShapeDtypeStruct((IB, E), BF16),
                   jax.ShapeDtypeStruct((NQ, IB), F32)),
        in_specs=[pl.BlockSpec(memory_space=pl.ANY), vmem, vmem, vmem],
        out_specs=(vmem, vmem, vmem),
        scratch_shapes=[
            pltpu.VMEM((Z, Y * UB, E), jnp.int32),
            pltpu.VMEM((Y, Z, UB, E), BF16),
            pltpu.VMEM((Z, Y - 1, UB, E), BF16),
            pltpu.VMEM((Y, Z, UB, E), BF16),
            pltpu.VMEM((Y, E, Z * UB), BF16),
            pltpu.VMEM((Y, Z, UB), F32),
            pltpu.VMEM((Z * Y - 1, Z, UB), F32),
            pltpu.VMEM((1, E), F32),
            pltpu.VMEM((G, 1, E), F32),
            pltpu.VMEM((Z, UB), F32),
            pltpu.VMEM((Y, 1, E), F32),
            pltpu.VMEM((L, Z, UB, E), BF16),
            pltpu.VMEM((L, 2, N, IB, E), BF16),
            pltpu.VMEM((Z, UB, E), F32),
            pltpu.VMEM((L, 2, 4, UB, E), F32),
            pltpu.VMEM((L, 2, 4, UB, E), F32),
            pltpu.VMEM((L, 2, N, IB, E), F32),
            pltpu.VMEM((L, Y, X, IB, E), F32),
            pltpu.VMEM((L, N, IB, E), F32),
            pltpu.VMEM((L, N - 1, IB, E), F32),
            pltpu.VMEM((NQ, UB), BF16),
            pltpu.VMEM((2, N, QB, E), BF16),
            pltpu.VMEM((N, QB, E), BF16),
            pltpu.VMEM((N, QB, E), BF16),
            pltpu.VMEM((N - 1, QB, E), BF16),
            pltpu.VMEM((Z - 1, QB, E), BF16),
            pltpu.VMEM((QB, E), BF16),
            pltpu.VMEM((2, N, QB, E), BF16),
            pltpu.VMEM((UB, E), F32),
            pltpu.VMEM((IB, E), F32),
            dma((Z,)), dma, dma((Z,)), dma, dma, dma, dma,
            dma, dma, dma((L,)), dma((L, Y)), dma((L,)), dma((L, Y)), dma((L,)), dma((L, 2, 4, 2)),
            dma((L,)), dma((L, Y)), dma((L,)), dma((L,)), dma((L,)), dma((L, 2, 4, 2)),
            dma((5,)), dma((3,)), dma((Y,)), dma((Y,)),
        ],
        compiler_params=pltpu.CompilerParams(collective_id=0, has_side_effects=True, vmem_limit_bytes=60 * 2**20),
    )(mask, user, item, queries.reshape(1, NQ))


def solution(mesh):
    return jax.shard_map(propagate, mesh=mesh,
                         in_specs=(P('row', 'col'), P(('row', 'col'), None), P(('col', 'row'), None), P()),
                         out_specs=(P(('row', 'col'), None), P(('col', 'row'), None), P(None, ('col', 'row'))),
                         check_vma=False)
```

```python
import jax
import jax.numpy as jnp
from jax import lax
from jax.experimental import pallas as pl
from jax.experimental.pallas import tpu as pltpu
from jax.sharding import PartitionSpec as P

LAYERS = 3
Z, Y, X = 8, 4, 4
R = 2 * X
G = Y * R
UB, IB = 128, 32
E = 256
NQ = 1024
QB = NQ // G
NH = 4
H = UB // NH
F32, BF16 = jnp.float32, jnp.bfloat16
MESH = pl.DeviceIdType.MESH
CONTRACT_ROWS = (((0,), (0,)), ((), ()))
CONTRACT_LANES = (((1,), (1,)), ((), ()))


def remote(src, dst, send_sem, recv_sem, col, row):
    return pltpu.make_async_remote_copy(src_ref=src, dst_ref=dst, send_sem=send_sem, recv_sem=recv_sem,
                                        device_id=(col, row), device_id_type=MESH)


def wait_bytes(ref, sem):
    pltpu.make_async_copy(ref, ref, sem).wait()


def kernel(mask_ref, user_ref, item_ref, query_ref, fu_ref, fi_ref, qall,
           mask_v, msend, mrecv, adj, adjt, rs_send, rs_recv, cs_send, cs_recv, invu, invi,
           eu_pan, ei_pan, up, us, ur, ip, pr, iq, ir, hot, qs, qp, qt, qr, qz, qzs, usum, isum,
           load_sem, mask_ssem, mask_rsem, rs_ssem, rs_rsem, cs_ssem, cs_rsem,
           eu0_ssem, eu0_rsem, ei_ssem, ei_rsem, fw_ssem, fw_rsem, us_ssem, us_rsem,
           pr_ssem, pr_rsem, ip_ssem, ip_rsem, ag_ssem, ag_rsem, q_ssem, q_rsem, qg_rsem, qf_rsem):
    col = lax.axis_index('col')
    row = lax.axis_index('row')
    z, y = lax.div(col, Y), lax.rem(col, Y)
    x, c = lax.div(row, 2), lax.rem(row, 2)
    other = 1 - c
    partner = x * 2 + other
    me = y * R + row
    spot = y * X + x

    def zat(d):
        return lax.rem(z + (d % Z), Z)

    def yat(d):
        return lax.rem(y + (d % Y), Y)

    def plane():
        for dy in (2, 1, 3, 0):
            for dx in (2, 1, 3, 0):
                if dy or dx:
                    yield dy * X + dx - 1, dy, yat(dy), lax.rem(x + dx, X)

    order = [4, 3, -3, 2, -2, 1, -1, 0]
    piece_of = {d: j for j, d in enumerate(order)}
    early = (list(range(NH // 2)), list(range(NH // 2, NH)))
    late = (early[1], early[0])
    right, left = zat(1) * Y + y, zat(-1) * Y + y

    loads = []
    for j, d in enumerate(order):
        zc = zat(d)
        load = pltpu.make_async_copy(mask_ref.at[pl.ds(zc * (Y * UB), Y * UB)], mask_v.at[j], load_sem.at[j])
        load.start()
        loads.append(load)

    barrier = pltpu.get_barrier_semaphore()
    for d in range(1, Z * Y):
        pl.semaphore_signal(barrier, inc=1, device_id=(lax.rem(col + d, Z * Y), row), device_id_type=MESH)
    for dy in range(Y):
        for dr in range(1, R):
            pl.semaphore_signal(barrier, inc=1, device_id=(z * Y + yat(dy), lax.rem(row + dr, R)), device_id_type=MESH)

    ones_w = jnp.ones((8, E), BF16)
    colsum = jnp.zeros((8, E), F32)
    for j, d in enumerate(order):
        zc = zat(d)
        loads[j].wait()
        for p in range(Y):
            wide = mask_v[j, p * UB:(p + 1) * UB, :].astype(F32)
            block = wide.astype(BF16)
            msend[p, j] = block
            sums = lax.dot_general(ones_w, block, CONTRACT_LANES, preferred_element_type=F32)
            rs_send[p, pl.ds(zc, 1), :] = sums[0:1]
            colsum = colsum + jnp.sum(wide.reshape(UB // 8, 8, E), axis=0)
    cs_send[...] = jnp.sum(colsum, axis=0, keepdims=True)
    cs_recv[me] = cs_send[...]
    eu_pan[0, z] = user_ref[...]
    ei_pan[0, c, spot] = item_ref[...]

    pl.semaphore_wait(barrier, 31 + 28)

    for dy in range(Y):
        for dr in range(R):
            if dy or dr:
                remote(cs_send, cs_recv.at[me], cs_ssem, cs_rsem, z * Y + yat(dy), lax.rem(row + dr, R)).start()
    for d in range(1, Z * Y):
        pc = lax.rem(col + d, Z * Y)
        remote(rs_send.at[lax.rem(pc, Y)], rs_recv.at[d - 1], rs_ssem, rs_rsem, pc, row).start()
    for slot, dy, py, px in plane():
        remote(item_ref, ei_pan.at[0, c, spot], ei_ssem.at[0], ei_rsem.at[0, dy], z * Y + py, px * 2 + c).start()
    for d in range(1, Z):
        remote(user_ref, eu_pan.at[0, z], eu0_ssem, eu0_rsem, zat(d) * Y + y, row).start()
    for j in range(Z):
        for d in range(1, Y):
            py = yat(d)
            remote(msend.at[py, j], mrecv.at[j, d - 1], mask_ssem, mask_rsem.at[j], z * Y + py, row).start()

    usum[...] = user_ref[...].astype(F32)
    isum[...] = item_ref[...].astype(F32)
    base = (row * (Z * Y) + col) * UB
    ids = lax.broadcasted_iota(jnp.int32, (UB, NQ), 0) + base
    hot[...] = jnp.where(ids == query_ref[...], 1.0, 0.0).T.astype(BF16)

    wait_bytes(cs_recv.at[pl.ds(0, G - 1)], cs_rsem)
    for s in range(Y):
        deg = cs_recv[s * R]
        for r in range(1, R):
            deg = deg + cs_recv[s * R + r]
        invi[s] = lax.rsqrt(jnp.maximum(deg, 1.0))
    wait_bytes(rs_recv, rs_rsem)
    deg = rs_send[y]
    for d in range(Z * Y - 1):
        deg = deg + rs_recv[d]
    invu[...] = lax.rsqrt(jnp.maximum(deg, 1.0))

    def make_adj(j, zc):
        wait_bytes(mrecv.at[j], mask_rsem.at[j])
        iu = jnp.broadcast_to(invu[pl.ds(zc, 1), :], (UB, UB)).T
        iu = jnp.concatenate([iu, iu], axis=1)
        for d in range(Y):
            s = yat(-d)
            m = (msend[y, j] if d == 0 else mrecv[j, d - 1]).astype(F32)
            a = (iu * m) * invi[s]
            adj[s, zc] = a.astype(BF16)
            adjt[s, :, pl.ds(pl.multiple_of(zc * UB, UB), UB)] = a.T.astype(BF16)

    def user_piece(k, j):
        zc = zat(order[j])
        if k == 0:
            make_adj(j, zc)
        acc = None
        for s in range(Y):
            panel = jnp.concatenate([ei_pan[k, cc, s * X + xx] for xx in range(X) for cc in range(2)], axis=0)
            t = jnp.dot(adj[s, zc], panel, preferred_element_type=F32)
            acc = t if acc is None else acc + t
        up[j] = acc

    def item_parts(k):
        eu = eu_pan[k].reshape(Z * UB, E)
        for j, dy in enumerate((2, 1, 3, 0)):
            s = yat(dy)
            part = jnp.dot(adjt[s], eu, preferred_element_type=F32).reshape(X, 2, IB, E)
            for xx in range(X):
                for cc in range(2):
                    ip[k, cc, s * X + xx] = part[xx, cc]
            remote(ip.at[k, other, pl.ds(s * X, X)], pr.at[k, j], pr_ssem.at[k], pr_rsem.at[k, j], col, partner).start()

    def item_send(k):
        for j, dy in enumerate((2, 1, 3, 0)):
            s = yat(dy)
            wait_bytes(pr.at[k, j], pr_rsem.at[k, j])
            iq[k, pl.ds(s * X, X)] = ip[k, c, pl.ds(s * X, X)] + pr[k, j]
            for slot, dy2, py, px in plane():
                if dy2 == dy:
                    remote(iq.at[k, s * X + px], ir.at[k, slot], ip_ssem.at[k], ip_rsem.at[k], z * Y + py, px * 2 + c).start()

    def item_total(k):
        wait_bytes(ir.at[k], ip_rsem.at[k])
        total = iq[k, spot]
        for slot in range(G // 2 - 1):
            total = total + ir[k, slot]
        return total

    def gather_plane(pan, ssem, rsem):
        for slot, dy, py, px in plane():
            remote(pan.at[c, spot], pan.at[c, spot], ssem, rsem.at[dy], z * Y + py, px * 2 + c).start()

    def forward_plane(pan, rsem, fssem, frsem):
        for dy in (0, 1, 3, 2):
            n = X - 1 if dy == 0 else X
            rows = pl.ds(yat(-dy) * X, X)
            wait_bytes(pan.at[c, pl.ds(0, n)], rsem.at[dy])
            remote(pan.at[c, rows], pan.at[c, rows], fssem, frsem.at[dy], col, partner).start()

    def wait_plane(pan, frsem):
        for dy in (0, 1, 3, 2):
            wait_bytes(pan.at[other, pl.ds(yat(-dy) * X, X)], frsem.at[dy])

    def user_total(k, hooks):
        def emit(way, step, h, first=False):
            rows = pl.ds(h * H, H)
            j = piece_of[4 - step] if way == 0 or step == 0 else piece_of[step - 4]
            value = up[j, h * H:(h + 1) * H]
            if not first:
                value = value + got(way, step - 1, h)
            us[k, way, step, h * H:(h + 1) * H] = value
            remote(us.at[k, way, step, rows], ur.at[k, way, step, rows], us_ssem.at[k], us_rsem.at[k, way, step, h],
                   right if way == 0 else left, row).start()

        def got(way, step, h):
            wait_bytes(ur.at[k, way, step, pl.ds(h * H, H)], us_rsem.at[k, way, step, h])
            return ur[k, way, step, h * H:(h + 1) * H]

        def hook(*at):
            if at in hooks:
                hooks[at]()

        user_piece(k, 0)
        for h in range(NH // 2):
            emit(0, 0, early[0][h], True)
            emit(1, 0, early[1][h], True)
        if k == 0:
            for step in range(1, 4):
                for way in range(2):
                    user_piece(k, 2 * step - 1 + way)
                    for h in early[way] + late[way]:
                        emit(way, step, h, step == 1 and h in late[way])
            user_piece(k, 7)
        else:
            for way in range(2):
                user_piece(k, 1 + way)
                for h in late[way]:
                    emit(way, 1, h, True)
            for step in range(1, 4):
                hook('before', step)
                if step < 3:
                    user_piece(k, 2 * step + 1)
                    user_piece(k, 2 * step + 2)
                else:
                    user_piece(k, 7)
                for h in range(NH // 2):
                    for way in range(2):
                        emit(way, step, early[way][h])
                if step < 3:
                    for h in range(NH // 2):
                        for way in range(2):
                            emit(way, step + 1, late[way][h])
                hook('after', step)
        parts = []
        for h in range(NH):
            parts.append(up[7, h * H:(h + 1) * H] + got(0, 3, h) + got(1, 3, h))
        new_user = jnp.concatenate(parts, axis=0).astype(BF16)
        usum[...] += new_user.astype(F32)
        return new_user

    def gather_user(k):
        def send(way, step, h):
            src = eu_pan.at[k, zat(-step if way == 0 else step), pl.ds(h * H, H)]
            remote(src, src, ag_ssem.at[k], ag_rsem.at[k, way, step, h], right if way == 0 else left, row).start()

        def got(way, step, h):
            dst = eu_pan.at[k, zat(-step - 1 if way == 0 else step + 1), pl.ds(h * H, H)]
            wait_bytes(dst, ag_rsem.at[k, way, step, h])

        def begin(new_user):
            eu_pan[k, z] = new_user
            for h in range(NH):
                for way in range(2):
                    send(way, 0, (early[way] + late[way])[h])

        def hop(step):
            for h in range(NH):
                for way in range(2):
                    hh = (early[way] + late[way])[h]
                    got(way, step, hh)
                    if step < 2 or h < NH // 2:
                        send(way, step + 1, hh)

        def last():
            for h in range(NH // 2):
                for way in range(2):
                    got(way, 3, early[way][h])

        return begin, hop, last

    def items_next(k):
        new_item = item_total(k).astype(BF16)
        isum[...] += new_item.astype(F32)
        ei_pan[k + 1, c, spot] = new_item
        gather_plane(ei_pan.at[k + 1], ei_ssem.at[k + 1], ei_rsem.at[k + 1])

    def items_forward(k):
        forward_plane(ei_pan.at[k], ei_rsem.at[k], fw_ssem.at[k], fw_rsem.at[k])

    def items_wait(k):
        wait_plane(ei_pan.at[k], fw_rsem.at[k])

    items_forward(0)
    items_wait(0)
    new_user = user_total(0, {})
    begin1, hop1, last1 = gather_user(1)
    begin1(new_user)
    wait_bytes(eu_pan.at[0, pl.ds(0, Z - 1)], eu0_rsem)
    item_parts(0)
    item_send(0)
    for step in range(3):
        hop1(step)
    last1()
    item_parts(1)
    items_next(0)
    item_send(1)
    items_forward(1)
    items_wait(1)
    new_user = user_total(1, {('after', 1): lambda: items_next(1), ('after', 3): lambda: items_forward(2)})
    begin2, hop2, last2 = gather_user(2)
    begin2(new_user)
    items_wait(2)

    def tail2():
        last2()
        item_parts(2)

    user_total(2, {('before', 1): lambda: hop2(0), ('before', 2): lambda: hop2(1), ('before', 3): lambda: hop2(2),
                   ('after', 3): tail2})
    final_user = (usum[...] / (LAYERS + 1)).astype(BF16)
    fu_ref[...] = final_user

    qs[...] = jnp.dot(hot[...], final_user, preferred_element_type=F32).astype(BF16).reshape(2, G // 2, QB, E)
    to_partner = remote(qs.at[other], qp, q_ssem.at[0], q_rsem.at[0], col, partner)
    to_partner.start()
    to_partner.wait_recv()
    qt[...] = (qs[c].astype(F32) + qp[...].astype(F32)).astype(BF16)
    for slot, dy, py, px in plane():
        remote(qt.at[py * X + px], qr.at[slot], q_ssem.at[1], q_rsem.at[1], z * Y + py, px * 2 + c).start()
    item_send(2)
    wait_bytes(qr, q_rsem.at[1])
    total = qt[spot].astype(F32)
    for slot in range(G // 2 - 1):
        total = total + qr[slot].astype(F32)
    qzs[...] = total.astype(BF16)
    for d in (4, 3, 5, 2, 6, 1, 7):
        remote(qzs, qz.at[d - 1], q_ssem.at[2], q_rsem.at[2], zat(d) * Y + y, row).start()
    wait_bytes(qz, q_rsem.at[2])
    for d in range(Z - 1):
        total = total + qz[d].astype(F32)
    qall[c, spot] = total.astype(BF16)
    gather_plane(qall, q_ssem.at[3], qg_rsem)
    new_item = item_total(2).astype(BF16)
    fi_ref[...] = ((isum[...] + new_item.astype(F32)) / (LAYERS + 1)).astype(BF16)
    forward_plane(qall, qg_rsem, q_ssem.at[4], qf_rsem)
    wait_plane(qall, qf_rsem)

    wait_bytes(rs_recv, rs_ssem)
    wait_bytes(cs_recv.at[pl.ds(0, G - 1)], cs_ssem)
    wait_bytes(eu_pan.at[0, pl.ds(0, Z - 1)], eu0_ssem)
    wait_bytes(msend.at[pl.ds(0, Y - 1)], mask_ssem)
    for k in range(LAYERS):
        wait_bytes(ei_pan.at[k, 0, pl.ds(0, G // 2 - 1)], ei_ssem.at[k])
        wait_bytes(ei_pan.at[k, 0], fw_ssem.at[k])
        wait_bytes(pr.at[k], pr_ssem.at[k])
        wait_bytes(ir.at[k], ip_ssem.at[k])
        wait_bytes(up.at[pl.ds(0, 7)], us_ssem.at[k])
        if k:
            wait_bytes(eu_pan.at[k, pl.ds(0, 7)], ag_ssem.at[k])
    to_partner.wait_send()
    wait_bytes(qr, q_ssem.at[1])
    wait_bytes(qz, q_ssem.at[2])
    wait_bytes(qr, q_ssem.at[3])
    wait_bytes(qt, q_ssem.at[4])


def finish(user_ref, item_ref, picked_ref, fu_ref, fi_ref, sc_ref):
    fu_ref[...] = user_ref[...]
    fi_ref[...] = item_ref[...]
    sc_ref[...] = lax.dot_general(item_ref[...], picked_ref[...], CONTRACT_LANES, preferred_element_type=F32)


def propagate(mask, user, item, queries):
    dma = pltpu.SemaphoreType.DMA
    vmem = pl.BlockSpec(memory_space=pltpu.VMEM)
    L, N = LAYERS, G // 2
    final_user, final_item, picked = pl.pallas_call(
        kernel,
        out_shape=(jax.ShapeDtypeStruct((UB, E), BF16), jax.ShapeDtypeStruct((IB, E), BF16),
                   jax.ShapeDtypeStruct((2, N, QB, E), BF16)),
        in_specs=[pl.BlockSpec(memory_space=pl.ANY), vmem, vmem, vmem],
        out_specs=(vmem, vmem, vmem),
        scratch_shapes=[
            pltpu.VMEM((Z, Y * UB, E), jnp.int32),
            pltpu.VMEM((Y, Z, UB, E), BF16),
            pltpu.VMEM((Z, Y - 1, UB, E), BF16),
            pltpu.VMEM((Y, Z, UB, E), BF16),
            pltpu.VMEM((Y, E, Z * UB), BF16),
            pltpu.VMEM((Y, Z, UB), F32),
            pltpu.VMEM((Z * Y - 1, Z, UB), F32),
            pltpu.VMEM((1, E), F32),
            pltpu.VMEM((G, 1, E), F32),
            pltpu.VMEM((Z, UB), F32),
            pltpu.VMEM((Y, 1, E), F32),
            pltpu.VMEM((L, Z, UB, E), BF16),
            pltpu.VMEM((L, 2, N, IB, E), BF16),
            pltpu.VMEM((Z, UB, E), F32),
            pltpu.VMEM((L, 2, 4, UB, E), F32),
            pltpu.VMEM((L, 2, 4, UB, E), F32),
            pltpu.VMEM((L, 2, N, IB, E), F32),
            pltpu.VMEM((L, Y, X, IB, E), F32),
            pltpu.VMEM((L, N, IB, E), F32),
            pltpu.VMEM((L, N - 1, IB, E), F32),
            pltpu.VMEM((NQ, UB), BF16),
            pltpu.VMEM((2, N, QB, E), BF16),
            pltpu.VMEM((N, QB, E), BF16),
            pltpu.VMEM((N, QB, E), BF16),
            pltpu.VMEM((N - 1, QB, E), BF16),
            pltpu.VMEM((Z - 1, QB, E), BF16),
            pltpu.VMEM((QB, E), BF16),
            pltpu.VMEM((UB, E), F32),
            pltpu.VMEM((IB, E), F32),
            dma((Z,)), dma, dma((Z,)), dma, dma, dma, dma,
            dma, dma, dma((L,)), dma((L, Y)), dma((L,)), dma((L, Y)), dma((L,)), dma((L, 2, 4, NH)),
            dma((L,)), dma((L, Y)), dma((L,)), dma((L,)), dma((L,)), dma((L, 2, 4, NH)),
            dma((5,)), dma((3,)), dma((Y,)), dma((Y,)),
        ],
        compiler_params=pltpu.CompilerParams(collective_id=0, has_side_effects=True, vmem_limit_bytes=60 * 2**20),
    )(mask, user, item, queries.reshape(1, NQ))
    final_user, final_item, scores = pl.pallas_call(
        finish,
        out_shape=(jax.ShapeDtypeStruct((UB, E), BF16), jax.ShapeDtypeStruct((IB, E), BF16),
                   jax.ShapeDtypeStruct((IB, NQ), F32)),
        in_specs=[vmem, vmem, vmem],
        out_specs=(vmem, vmem, vmem),
    )(final_user, final_item, picked.reshape(NQ, E))
    return final_user, final_item, scores.T


def solution(mesh):
    return jax.shard_map(propagate, mesh=mesh,
                         in_specs=(P('row', 'col'), P(('row', 'col'), None), P(('col', 'row'), None), P()),
                         out_specs=(P(('row', 'col'), None), P(('col', 'row'), None), P(None, ('col', 'row'))),
                         check_vma=False)
```

```python
import jax
import jax.numpy as jnp
from jax import lax
from jax.experimental import pallas as pl
from jax.experimental.pallas import tpu as pltpu
from jax.sharding import PartitionSpec as P

LAYERS = 3
Z, Y, X = 8, 4, 4
R = 2 * X
G = Y * R
UB, IB = 128, 32
E = 256
NQ = 1024
QB = NQ // G
NH = 4
H = UB // NH
F32, BF16 = jnp.float32, jnp.bfloat16
MESH = pl.DeviceIdType.MESH
CONTRACT_ROWS = (((0,), (0,)), ((), ()))
CONTRACT_LANES = (((1,), (1,)), ((), ()))


def remote(src, dst, send_sem, recv_sem, col, row):
    return pltpu.make_async_remote_copy(src_ref=src, dst_ref=dst, send_sem=send_sem, recv_sem=recv_sem,
                                        device_id=(col, row), device_id_type=MESH)


def wait_bytes(ref, sem):
    pltpu.make_async_copy(ref, ref, sem).wait()


def kernel(mask_ref, user_ref, item_ref, query_ref, fu_hbm, fi_hbm, q_hbm,
           mask_v, msend, mrecv, adj, adjt, rs_send, rs_recv, cs_send, cs_recv, invu, invi,
           eu_pan, ei_pan, up, us, ur, ip, pr, iq, ir, hot, qs, qp, qt, qr, qz, qzs, qall, fu_v, fi_v, usum, isum,
           load_sem, mask_ssem, mask_rsem, rs_ssem, rs_rsem, cs_ssem, cs_rsem,
           eu0_ssem, eu0_rsem, ei_ssem, ei_rsem, fw_ssem, fw_rsem, us_ssem, us_rsem,
           pr_ssem, pr_rsem, ip_ssem, ip_rsem, ag_ssem, ag_rsem, q_ssem, q_rsem, qg_rsem, qf_rsem, out_sem):
    col = lax.axis_index('col')
    row = lax.axis_index('row')
    z, y = lax.div(col, Y), lax.rem(col, Y)
    x, c = lax.div(row, 2), lax.rem(row, 2)
    other = 1 - c
    partner = x * 2 + other
    me = y * R + row
    spot = y * X + x

    def zat(d):
        return lax.rem(z + (d % Z), Z)

    def yat(d):
        return lax.rem(y + (d % Y), Y)

    def plane():
        for dy in (2, 1, 3, 0):
            for dx in (2, 1, 3, 0):
                if dy or dx:
                    yield dy * X + dx - 1, dy, yat(dy), lax.rem(x + dx, X)

    order = [4, 3, -3, 2, -2, 1, -1, 0]
    piece_of = {d: j for j, d in enumerate(order)}
    early = (list(range(NH // 2)), list(range(NH // 2, NH)))
    late = (early[1], early[0])
    right, left = zat(1) * Y + y, zat(-1) * Y + y

    loads = []
    for j, d in enumerate(order):
        zc = zat(d)
        load = pltpu.make_async_copy(mask_ref.at[pl.ds(zc * (Y * UB), Y * UB)], mask_v.at[j], load_sem.at[j])
        load.start()
        loads.append(load)

    barrier = pltpu.get_barrier_semaphore()
    for d in range(1, Z * Y):
        pl.semaphore_signal(barrier, inc=1, device_id=(lax.rem(col + d, Z * Y), row), device_id_type=MESH)
    for dy in range(Y):
        for dr in range(1, R):
            pl.semaphore_signal(barrier, inc=1, device_id=(z * Y + yat(dy), lax.rem(row + dr, R)), device_id_type=MESH)

    ones_w = jnp.ones((8, E), BF16)
    colsum = jnp.zeros((8, E), F32)
    for j, d in enumerate(order):
        zc = zat(d)
        loads[j].wait()
        for p in range(Y):
            wide = mask_v[j, p * UB:(p + 1) * UB, :].astype(F32)
            block = wide.astype(BF16)
            msend[p, j] = block
            sums = lax.dot_general(ones_w, block, CONTRACT_LANES, preferred_element_type=F32)
            rs_send[p, pl.ds(zc, 1), :] = sums[0:1]
            colsum = colsum + jnp.sum(wide.reshape(UB // 8, 8, E), axis=0)
    cs_send[...] = jnp.sum(colsum, axis=0, keepdims=True)
    cs_recv[me] = cs_send[...]
    eu_pan[0, z] = user_ref[...]
    ei_pan[0, c, spot] = item_ref[...]

    pl.semaphore_wait(barrier, 31 + 28)

    for dy in range(Y):
        for dr in range(R):
            if dy or dr:
                remote(cs_send, cs_recv.at[me], cs_ssem, cs_rsem, z * Y + yat(dy), lax.rem(row + dr, R)).start()
    for d in range(1, Z * Y):
        pc = lax.rem(col + d, Z * Y)
        remote(rs_send.at[lax.rem(pc, Y)], rs_recv.at[d - 1], rs_ssem, rs_rsem, pc, row).start()
    for slot, dy, py, px in plane():
        remote(item_ref, ei_pan.at[0, c, spot], ei_ssem.at[0], ei_rsem.at[0, dy], z * Y + py, px * 2 + c).start()
    for d in range(1, Z):
        remote(user_ref, eu_pan.at[0, z], eu0_ssem, eu0_rsem, zat(d) * Y + y, row).start()
    for j in range(Z):
        for d in range(1, Y):
            py = yat(d)
            remote(msend.at[py, j], mrecv.at[j, d - 1], mask_ssem, mask_rsem.at[j], z * Y + py, row).start()

    usum[...] = user_ref[...].astype(F32)
    isum[...] = item_ref[...].astype(F32)
    base = (row * (Z * Y) + col) * UB
    ids = lax.broadcasted_iota(jnp.int32, (UB, NQ), 0) + base
    hot[...] = jnp.where(ids == query_ref[...], 1.0, 0.0).T.astype(BF16)

    wait_bytes(cs_recv.at[pl.ds(0, G - 1)], cs_rsem)
    for s in range(Y):
        deg = cs_recv[s * R]
        for r in range(1, R):
            deg = deg + cs_recv[s * R + r]
        invi[s] = lax.rsqrt(jnp.maximum(deg, 1.0))
    wait_bytes(rs_recv, rs_rsem)
    deg = rs_send[y]
    for d in range(Z * Y - 1):
        deg = deg + rs_recv[d]
    invu[...] = lax.rsqrt(jnp.maximum(deg, 1.0))

    def make_adj(j, zc):
        wait_bytes(mrecv.at[j], mask_rsem.at[j])
        iu = jnp.broadcast_to(invu[pl.ds(zc, 1), :], (UB, UB)).T
        iu = jnp.concatenate([iu, iu], axis=1)
        for d in range(Y):
            s = yat(-d)
            m = (msend[y, j] if d == 0 else mrecv[j, d - 1]).astype(F32)
            a = (iu * m) * invi[s]
            adj[s, zc] = a.astype(BF16)
            adjt[s, :, pl.ds(pl.multiple_of(zc * UB, UB), UB)] = a.T.astype(BF16)

    def user_piece(k, j):
        zc = zat(order[j])
        if k == 0:
            make_adj(j, zc)
        acc = None
        for s in range(Y):
            panel = jnp.concatenate([ei_pan[k, cc, s * X + xx] for xx in range(X) for cc in range(2)], axis=0)
            t = jnp.dot(adj[s, zc], panel, preferred_element_type=F32)
            acc = t if acc is None else acc + t
        up[j] = acc

    def item_parts(k):
        eu = eu_pan[k].reshape(Z * UB, E)
        for j, dy in enumerate((2, 1, 3, 0)):
            s = yat(dy)
            part = jnp.dot(adjt[s], eu, preferred_element_type=F32).reshape(X, 2, IB, E)
            for xx in range(X):
                for cc in range(2):
                    ip[k, cc, s * X + xx] = part[xx, cc]
            remote(ip.at[k, other, pl.ds(s * X, X)], pr.at[k, j], pr_ssem.at[k], pr_rsem.at[k, j], col, partner).start()

    def item_send(k):
        for j, dy in enumerate((2, 1, 3, 0)):
            s = yat(dy)
            wait_bytes(pr.at[k, j], pr_rsem.at[k, j])
            iq[k, pl.ds(s * X, X)] = ip[k, c, pl.ds(s * X, X)] + pr[k, j]
            for slot, dy2, py, px in plane():
                if dy2 == dy:
                    remote(iq.at[k, s * X + px], ir.at[k, slot], ip_ssem.at[k], ip_rsem.at[k], z * Y + py, px * 2 + c).start()

    def item_total(k):
        wait_bytes(ir.at[k], ip_rsem.at[k])
        total = iq[k, spot]
        for slot in range(G // 2 - 1):
            total = total + ir[k, slot]
        return total

    def gather_plane(pan, ssem, rsem):
        for slot, dy, py, px in plane():
            remote(pan.at[c, spot], pan.at[c, spot], ssem, rsem.at[dy], z * Y + py, px * 2 + c).start()

    def forward_plane(pan, rsem, fssem, frsem):
        for dy in (0, 1, 3, 2):
            n = X - 1 if dy == 0 else X
            rows = pl.ds(yat(-dy) * X, X)
            wait_bytes(pan.at[c, pl.ds(0, n)], rsem.at[dy])
            remote(pan.at[c, rows], pan.at[c, rows], fssem, frsem.at[dy], col, partner).start()

    def wait_plane(pan, frsem):
        for dy in (0, 1, 3, 2):
            wait_bytes(pan.at[other, pl.ds(yat(-dy) * X, X)], frsem.at[dy])

    def user_total(k, hooks):
        def emit(way, step, h, first=False):
            rows = pl.ds(h * H, H)
            j = piece_of[4 - step] if way == 0 or step == 0 else piece_of[step - 4]
            value = up[j, h * H:(h + 1) * H]
            if not first:
                value = value + got(way, step - 1, h)
            us[k, way, step, h * H:(h + 1) * H] = value
            remote(us.at[k, way, step, rows], ur.at[k, way, step, rows], us_ssem.at[k], us_rsem.at[k, way, step, h],
                   right if way == 0 else left, row).start()

        def got(way, step, h):
            wait_bytes(ur.at[k, way, step, pl.ds(h * H, H)], us_rsem.at[k, way, step, h])
            return ur[k, way, step, h * H:(h + 1) * H]

        def hook(*at):
            if at in hooks:
                hooks[at]()

        user_piece(k, 0)
        for h in range(NH // 2):
            emit(0, 0, early[0][h], True)
            emit(1, 0, early[1][h], True)
        if k == 0:
            for step in range(1, 4):
                for way in range(2):
                    user_piece(k, 2 * step - 1 + way)
                    for h in early[way] + late[way]:
                        emit(way, step, h, step == 1 and h in late[way])
            user_piece(k, 7)
            hook('own')
        else:
            for way in range(2):
                user_piece(k, 1 + way)
                for h in late[way]:
                    emit(way, 1, h, True)
            for step in range(1, 4):
                hook('before', step)
                if step < 3:
                    user_piece(k, 2 * step + 1)
                    user_piece(k, 2 * step + 2)
                else:
                    user_piece(k, 7)
                for h in range(NH // 2):
                    for way in range(2):
                        emit(way, step, early[way][h])
                if step < 3:
                    for h in range(NH // 2):
                        for way in range(2):
                            emit(way, step + 1, late[way][h])
                hook('after', step)
        parts = []
        for h in range(NH):
            parts.append(up[7, h * H:(h + 1) * H] + got(0, 3, h) + got(1, 3, h))
        new_user = jnp.concatenate(parts, axis=0).astype(BF16)
        usum[...] += new_user.astype(F32)
        return new_user

    def gather_user(k):
        def send(way, step, h):
            src = eu_pan.at[k, zat(-step if way == 0 else step), pl.ds(h * H, H)]
            remote(src, src, ag_ssem.at[k], ag_rsem.at[k, way, step, h], right if way == 0 else left, row).start()

        def got(way, step, h):
            dst = eu_pan.at[k, zat(-step - 1 if way == 0 else step + 1), pl.ds(h * H, H)]
            wait_bytes(dst, ag_rsem.at[k, way, step, h])

        def begin(new_user):
            eu_pan[k, z] = new_user
            for h in range(NH):
                for way in range(2):
                    send(way, 0, (early[way] + late[way])[h])

        def hop(step):
            for h in range(NH):
                for way in range(2):
                    hh = (early[way] + late[way])[h]
                    got(way, step, hh)
                    if step < 2 or h < NH // 2:
                        send(way, step + 1, hh)

        def last():
            for h in range(NH // 2):
                for way in range(2):
                    got(way, 3, early[way][h])

        return begin, hop, last

    def items_next(k):
        new_item = item_total(k).astype(BF16)
        isum[...] += new_item.astype(F32)
        ei_pan[k + 1, c, spot] = new_item
        gather_plane(ei_pan.at[k + 1], ei_ssem.at[k + 1], ei_rsem.at[k + 1])

    def items_forward(k):
        forward_plane(ei_pan.at[k], ei_rsem.at[k], fw_ssem.at[k], fw_rsem.at[k])

    def items_wait(k):
        wait_plane(ei_pan.at[k], fw_rsem.at[k])

    def items0():
        wait_bytes(eu_pan.at[0, pl.ds(0, Z - 1)], eu0_rsem)
        item_parts(0)
        item_send(0)

    items_forward(0)
    items_wait(0)
    new_user = user_total(0, {('own',): items0})
    begin1, hop1, last1 = gather_user(1)
    begin1(new_user)
    hop1(0)
    hop1(1)
    items_next(0)
    hop1(2)
    last1()
    item_parts(1)
    items_forward(1)
    item_send(1)
    items_wait(1)
    new_user = user_total(1, {('after', 2): lambda: items_next(1)})
    begin2, hop2, last2 = gather_user(2)
    begin2(new_user)
    items_forward(2)
    items_wait(2)

    def tail2():
        last2()
        item_parts(2)

    user_total(2, {('before', 1): lambda: hop2(0), ('before', 2): lambda: hop2(1), ('before', 3): lambda: hop2(2),
                   ('after', 3): tail2})
    final_user = (usum[...] / (LAYERS + 1)).astype(BF16)
    fu_v[...] = final_user
    outs = [pltpu.make_async_copy(fu_v, fu_hbm, out_sem.at[0])]
    outs[0].start()

    qs[...] = jnp.dot(hot[...], final_user, preferred_element_type=F32).astype(BF16).reshape(2, G // 2, QB, E)
    to_partner = remote(qs.at[other], qp, q_ssem.at[0], q_rsem.at[0], col, partner)
    to_partner.start()
    to_partner.wait_recv()
    qt[...] = (qs[c].astype(F32) + qp[...].astype(F32)).astype(BF16)
    for slot, dy, py, px in plane():
        remote(qt.at[py * X + px], qr.at[slot], q_ssem.at[1], q_rsem.at[1], z * Y + py, px * 2 + c).start()
    item_send(2)
    wait_bytes(qr, q_rsem.at[1])
    total = qt[spot].astype(F32)
    for slot in range(G // 2 - 1):
        total = total + qr[slot].astype(F32)
    qzs[...] = total.astype(BF16)
    for d in (4, 3, 5, 2, 6, 1, 7):
        remote(qzs, qz.at[d - 1], q_ssem.at[2], q_rsem.at[2], zat(d) * Y + y, row).start()
    wait_bytes(qz, q_rsem.at[2])
    for d in range(Z - 1):
        total = total + qz[d].astype(F32)
    qall[c, spot] = total.astype(BF16)
    gather_plane(qall, q_ssem.at[3], qg_rsem)
    new_item = item_total(2).astype(BF16)
    fi_v[...] = ((isum[...] + new_item.astype(F32)) / (LAYERS + 1)).astype(BF16)
    outs.append(pltpu.make_async_copy(fi_v, fi_hbm, out_sem.at[1]))
    outs[1].start()
    forward_plane(qall, qg_rsem, q_ssem.at[4], qf_rsem)
    outs.append(pltpu.make_async_copy(qall.at[c], q_hbm.at[c], out_sem.at[2]))
    outs[2].start()
    wait_plane(qall, qf_rsem)
    outs.append(pltpu.make_async_copy(qall.at[other], q_hbm.at[other], out_sem.at[3]))
    outs[3].start()

    wait_bytes(rs_recv, rs_ssem)
    wait_bytes(cs_recv.at[pl.ds(0, G - 1)], cs_ssem)
    wait_bytes(eu_pan.at[0, pl.ds(0, Z - 1)], eu0_ssem)
    wait_bytes(msend.at[pl.ds(0, Y - 1)], mask_ssem)
    for k in range(LAYERS):
        wait_bytes(ei_pan.at[k, 0, pl.ds(0, G // 2 - 1)], ei_ssem.at[k])
        wait_bytes(ei_pan.at[k, 0], fw_ssem.at[k])
        wait_bytes(pr.at[k], pr_ssem.at[k])
        wait_bytes(ir.at[k], ip_ssem.at[k])
        wait_bytes(up.at[pl.ds(0, 7)], us_ssem.at[k])
        if k:
            wait_bytes(eu_pan.at[k, pl.ds(0, 7)], ag_ssem.at[k])
    to_partner.wait_send()
    wait_bytes(qr, q_ssem.at[1])
    wait_bytes(qz, q_ssem.at[2])
    wait_bytes(qr, q_ssem.at[3])
    wait_bytes(qt, q_ssem.at[4])
    for out in outs:
        out.wait()


def finish(user_ref, item_ref, picked_ref, fu_ref, fi_ref, sc_ref):
    fu_ref[...] = user_ref[...]
    fi_ref[...] = item_ref[...]
    sc_ref[...] = lax.dot_general(item_ref[...], picked_ref[...], CONTRACT_LANES, preferred_element_type=F32)


def propagate(mask, user, item, queries):
    dma = pltpu.SemaphoreType.DMA
    vmem, hbm = pl.BlockSpec(memory_space=pltpu.VMEM), pl.BlockSpec(memory_space=pl.ANY)
    L, N = LAYERS, G // 2
    final_user, final_item, picked = pl.pallas_call(
        kernel,
        out_shape=(jax.ShapeDtypeStruct((UB, E), BF16), jax.ShapeDtypeStruct((IB, E), BF16),
                   jax.ShapeDtypeStruct((2, N, QB, E), BF16)),
        in_specs=[hbm, vmem, vmem, vmem],
        out_specs=(hbm, hbm, hbm),
        scratch_shapes=[
            pltpu.VMEM((Z, Y * UB, E), jnp.int32),
            pltpu.VMEM((Y, Z, UB, E), BF16),
            pltpu.VMEM((Z, Y - 1, UB, E), BF16),
            pltpu.VMEM((Y, Z, UB, E), BF16),
            pltpu.VMEM((Y, E, Z * UB), BF16),
            pltpu.VMEM((Y, Z, UB), F32),
            pltpu.VMEM((Z * Y - 1, Z, UB), F32),
            pltpu.VMEM((1, E), F32),
            pltpu.VMEM((G, 1, E), F32),
            pltpu.VMEM((Z, UB), F32),
            pltpu.VMEM((Y, 1, E), F32),
            pltpu.VMEM((L, Z, UB, E), BF16),
            pltpu.VMEM((L, 2, N, IB, E), BF16),
            pltpu.VMEM((Z, UB, E), F32),
            pltpu.VMEM((L, 2, 4, UB, E), F32),
            pltpu.VMEM((L, 2, 4, UB, E), F32),
            pltpu.VMEM((L, 2, N, IB, E), F32),
            pltpu.VMEM((L, Y, X, IB, E), F32),
            pltpu.VMEM((L, N, IB, E), F32),
            pltpu.VMEM((L, N - 1, IB, E), F32),
            pltpu.VMEM((NQ, UB), BF16),
            pltpu.VMEM((2, N, QB, E), BF16),
            pltpu.VMEM((N, QB, E), BF16),
            pltpu.VMEM((N, QB, E), BF16),
            pltpu.VMEM((N - 1, QB, E), BF16),
            pltpu.VMEM((Z - 1, QB, E), BF16),
            pltpu.VMEM((QB, E), BF16),
            pltpu.VMEM((2, N, QB, E), BF16),
            pltpu.VMEM((UB, E), BF16),
            pltpu.VMEM((IB, E), BF16),
            pltpu.VMEM((UB, E), F32),
            pltpu.VMEM((IB, E), F32),
            dma((Z,)), dma, dma((Z,)), dma, dma, dma, dma,
            dma, dma, dma((L,)), dma((L, Y)), dma((L,)), dma((L, Y)), dma((L,)), dma((L, 2, 4, NH)),
            dma((L,)), dma((L, Y)), dma((L,)), dma((L,)), dma((L,)), dma((L, 2, 4, NH)),
            dma((5,)), dma((3,)), dma((Y,)), dma((Y,)), dma((4,)),
        ],
        compiler_params=pltpu.CompilerParams(collective_id=0, has_side_effects=True, vmem_limit_bytes=60 * 2**20),
    )(mask, user, item, queries.reshape(1, NQ))
    final_user, final_item, scores = pl.pallas_call(
        finish,
        out_shape=(jax.ShapeDtypeStruct((UB, E), BF16), jax.ShapeDtypeStruct((IB, E), BF16),
                   jax.ShapeDtypeStruct((IB, NQ), F32)),
        in_specs=[vmem, vmem, vmem],
        out_specs=(vmem, vmem, vmem),
    )(final_user, final_item, picked.reshape(NQ, E))
    return final_user, final_item, scores.T


def solution(mesh):
    return jax.shard_map(propagate, mesh=mesh,
                         in_specs=(P('row', 'col'), P(('row', 'col'), None), P(('col', 'row'), None), P()),
                         out_specs=(P(('row', 'col'), None), P(('col', 'row'), None), P(None, ('col', 'row'))),
                         check_vma=False)
```

```python
import jax
import jax.numpy as jnp
from jax import lax
from jax.experimental import pallas as pl
from jax.experimental.pallas import tpu as pltpu
from jax.sharding import PartitionSpec as P

LAYERS = 3
Z, Y, X = 8, 4, 4
R = 2 * X
G = Y * R
UB, IB = 128, 32
E = 256
NQ = 1024
QB = NQ // G
NH = 4
H = UB // NH
F32, BF16 = jnp.float32, jnp.bfloat16
MESH = pl.DeviceIdType.MESH
CONTRACT_ROWS = (((0,), (0,)), ((), ()))
CONTRACT_LANES = (((1,), (1,)), ((), ()))


def remote(src, dst, send_sem, recv_sem, col, row):
    return pltpu.make_async_remote_copy(src_ref=src, dst_ref=dst, send_sem=send_sem, recv_sem=recv_sem,
                                        device_id=(col, row), device_id_type=MESH)


def wait_bytes(ref, sem):
    pltpu.make_async_copy(ref, ref, sem).wait()


def kernel(mask_ref, user_ref, item_ref, query_ref, fu_hbm, fi_hbm, q_hbm,
           mask_v, msend, mrecv, adj, adjt, rs_send, rs_y, rs_z, cs_send, cs_row, cs_y, invu, invi,
           eu_pan, ei_pan, up, us, ur, ip, pr, iq, ir, hot, qs, qp, qt, qr, qz, qzs, qall, fu_v, fi_v, usum, isum,
           load_sem, mask_ssem, mask_rsem, rs_ssem, rs_rsem, rz_rsem, cs_ssem, cs_rsem, ei_ssem, ei_rsem, fw_ssem, fw_rsem, us_ssem, us_rsem,
           pr_ssem, pr_rsem, ip_ssem, ip_rsem, ag_ssem, ag_rsem, q_ssem, q_rsem, qg_rsem, qf_rsem, out_sem):
    col = lax.axis_index('col')
    row = lax.axis_index('row')
    z, y = lax.div(col, Y), lax.rem(col, Y)
    x, c = lax.div(row, 2), lax.rem(row, 2)
    other = 1 - c
    partner = x * 2 + other
    spot = x * Y + y

    def zat(d):
        return lax.rem(z + (d % Z), Z)

    def yat(d):
        return lax.rem(y + (d % Y), Y)

    def xat(d):
        return lax.rem(x + (d % X), X)

    def plane():
        for dx in (2, 1, 3, 0):
            for dy in (2, 1, 3, 0):
                if dy or dx:
                    yield dx * Y + dy - 1, dx, yat(dy), xat(dx)

    order = [4, 3, -3, 2, -2, 1, -1, 0]
    piece_of = {d: j for j, d in enumerate(order)}
    early = (list(range(NH // 2)), list(range(NH // 2, NH)))
    late = (early[1], early[0])
    right, left = zat(1) * Y + y, zat(-1) * Y + y

    loads = []
    for j, d in enumerate(order):
        zc = zat(d)
        load = pltpu.make_async_copy(mask_ref.at[pl.ds(zc * (Y * UB), Y * UB)], mask_v.at[j], load_sem.at[j])
        load.start()
        loads.append(load)

    barrier = pltpu.get_barrier_semaphore()
    for d in range(1, R):
        pl.semaphore_signal(barrier, inc=1, device_id=(col, lax.rem(row + d, R)), device_id_type=MESH)
    for d in range(1, Y):
        pl.semaphore_signal(barrier, inc=1, device_id=(z * Y + yat(d), row), device_id_type=MESH)
    for peer in (right, left):
        pl.semaphore_signal(barrier, inc=1, device_id=(peer, row), device_id_type=MESH)

    ones_w = jnp.ones((8, E), BF16)
    colsum = jnp.zeros((8, E), F32)
    for j, d in enumerate(order):
        zc = zat(d)
        loads[j].wait()
        for p in range(Y):
            wide = mask_v[j, p * UB:(p + 1) * UB, :].astype(F32)
            block = wide.astype(BF16)
            msend[p, j] = block
            sums = lax.dot_general(ones_w, block, CONTRACT_LANES, preferred_element_type=F32)
            rs_send[p, pl.ds(zc, 1), :] = sums[0:1]
            colsum = colsum + jnp.sum(wide.reshape(UB // 8, 8, E), axis=0)
    cs_send[...] = jnp.sum(colsum, axis=0, keepdims=True)
    cs_row[row] = cs_send[...]
    ei_pan[0, c, spot] = item_ref[...]

    pl.semaphore_wait(barrier, R - 1 + Y - 1 + 2)

    def send_mask(j):
        for d in range(1, Y):
            py = yat(d)
            remote(msend.at[py, j], mrecv.at[j, d - 1], mask_ssem, mask_rsem.at[j], z * Y + py, row).start()

    def gather_user(k):
        def send(way, step, h):
            src = eu_pan.at[k, zat(-step if way == 0 else step), pl.ds(h * H, H)]
            remote(src, src, ag_ssem.at[k], ag_rsem.at[way, step, h], right if way == 0 else left, row).start()

        def got(way, step, h):
            dst = eu_pan.at[k, zat(-step - 1 if way == 0 else step + 1), pl.ds(h * H, H)]
            wait_bytes(dst, ag_rsem.at[way, step, h])

        def begin(new_user):
            eu_pan[k, z] = new_user
            for h in range(NH):
                for way in range(2):
                    send(way, 0, (early[way] + late[way])[h])

        def hop(step):
            for h in range(NH):
                for way in range(2):
                    hh = (early[way] + late[way])[h]
                    got(way, step, hh)
                    if step < 2 or h < NH // 2:
                        send(way, step + 1, hh)

        def last():
            for h in range(NH // 2):
                for way in range(2):
                    got(way, 3, early[way][h])

        return begin, hop, last

    def degree_send(way, step):
        src = rs_z.at[zat(-step if way == 0 else step)]
        remote(src, src, rs_ssem.at[1], rz_rsem.at[way, step], right if way == 0 else left, row).start()

    def degree_hop(step):
        for way in range(2):
            if step < 3 or way == 0:
                wait_bytes(rs_z.at[zat(-step - 1 if way == 0 else step + 1)], rz_rsem.at[way, step])
            if step < 2 or (step < 3 and way == 0):
                degree_send(way, step + 1)

    for d in range(1, Y):
        remote(rs_send.at[yat(d)], rs_y.at[d - 1], rs_ssem.at[0], rs_rsem, z * Y + yat(d), row).start()
    for d in range(1, R):
        remote(cs_send, cs_row.at[row], cs_ssem.at[0], cs_rsem.at[0], col, lax.rem(row + d, R)).start()
    for d in range(1, Y):
        remote(item_ref, ei_pan.at[0, c, spot], ei_ssem.at[0], ei_rsem.at[0, 0], z * Y + yat(d), row).start()
    send_mask(0)
    begin0, hop0, last0 = gather_user(0)
    begin0(user_ref[...])
    send_mask(1)

    usum[...] = user_ref[...].astype(F32)
    isum[...] = item_ref[...].astype(F32)
    wait_bytes(rs_y, rs_rsem)
    rs_z[z] = rs_send[y] + rs_y[0] + rs_y[1] + rs_y[2]
    for way in range(2):
        degree_send(way, 0)

    wait_bytes(ei_pan.at[0, c, pl.ds(0, Y - 1)], ei_rsem.at[0, 0])
    own = ei_pan.at[0, c, pl.ds(x * Y, Y)]
    for d in range(1, X):
        remote(own, own, ei_ssem.at[0], ei_rsem.at[0, d], col, xat(d) * 2 + c).start()
    remote(own, own, fw_ssem.at[0], fw_rsem.at[0, 0], col, partner).start()

    wait_bytes(cs_row.at[pl.ds(0, R - 1)], cs_rsem.at[0])
    deg = cs_row[0]
    for r in range(1, R):
        deg = deg + cs_row[r]
    cs_y[y] = deg
    for d in range(1, Y):
        remote(cs_y.at[y], cs_y.at[y], cs_ssem.at[1], cs_rsem.at[1], z * Y + yat(d), row).start()
    for j in range(2, Z):
        send_mask(j)

    base = (row * (Z * Y) + col) * UB
    ids = lax.broadcasted_iota(jnp.int32, (UB, NQ), 0) + base
    hot[...] = jnp.where(ids == query_ref[...], 1.0, 0.0).T.astype(BF16)

    degree_hop(0)
    degree_hop(1)
    hop0(0)
    degree_hop(2)
    hop0(1)
    for d in (1, 3, 2):
        rows = pl.ds(xat(-d) * Y, Y)
        wait_bytes(ei_pan.at[0, c, rows], ei_rsem.at[0, d])
        remote(ei_pan.at[0, c, rows], ei_pan.at[0, c, rows], fw_ssem.at[0], fw_rsem.at[0, d], col, partner).start()
    wait_bytes(cs_y.at[pl.ds(0, Y - 1)], cs_rsem.at[1])
    for s in range(Y):
        invi[s] = lax.rsqrt(jnp.maximum(cs_y[s], 1.0))
    degree_hop(3)
    deg = rs_z[0]
    for d in range(1, Z):
        deg = deg + rs_z[d]
    invu[...] = lax.rsqrt(jnp.maximum(deg, 1.0))

    def make_adj(j, zc):
        wait_bytes(mrecv.at[j], mask_rsem.at[j])
        iu = jnp.broadcast_to(invu[pl.ds(zc, 1), :], (UB, UB)).T
        iu = jnp.concatenate([iu, iu], axis=1)
        for d in range(Y):
            s = yat(-d)
            m = (msend[y, j] if d == 0 else mrecv[j, d - 1]).astype(F32)
            a = (iu * m) * invi[s]
            adj[s, zc] = a.astype(BF16)
            adjt[s, :, pl.ds(pl.multiple_of(zc * UB, UB), UB)] = a.T.astype(BF16)

    def user_piece(k, j):
        zc = zat(order[j])
        if k == 0:
            make_adj(j, zc)
        acc = None
        for s in range(Y):
            panel = jnp.concatenate([ei_pan[k, cc, xx * Y + s] for xx in range(X) for cc in range(2)], axis=0)
            t = jnp.dot(adj[s, zc], panel, preferred_element_type=F32)
            acc = t if acc is None else acc + t
        up[j] = acc

    def item_parts(k):
        eu = eu_pan[k].reshape(Z * UB, E)
        for j, dy in enumerate((2, 1, 3, 0)):
            s = yat(dy)
            part = jnp.dot(adjt[s], eu, preferred_element_type=F32).reshape(X, 2, IB, E)
            for xx in range(X):
                for cc in range(2):
                    ip[k, cc, s * X + xx] = part[xx, cc]
            remote(ip.at[k, other, pl.ds(s * X, X)], pr.at[k, j], pr_ssem.at[k], pr_rsem.at[k, j], col, partner).start()

    def item_send(k):
        for j, dy in enumerate((2, 1, 3, 0)):
            s = yat(dy)
            wait_bytes(pr.at[k, j], pr_rsem.at[k, j])
            iq[k, pl.ds(s * X, X)] = ip[k, c, pl.ds(s * X, X)] + pr[k, j]
            for dx in (2, 1, 3, 0):
                if dy or dx:
                    px = xat(dx)
                    remote(iq.at[k, s * X + px], ir.at[k, dy * X + dx - 1], ip_ssem.at[k], ip_rsem.at[k],
                           z * Y + s, px * 2 + c).start()

    def item_total(k):
        wait_bytes(ir.at[k], ip_rsem.at[k])
        total = iq[k, y * X + x]
        for slot in range(G // 2 - 1):
            total = total + ir[k, slot]
        return total

    def gather_plane(pan, ssem, rsem):
        for slot, dx, py, px in plane():
            remote(pan.at[c, spot], pan.at[c, spot], ssem, rsem.at[dx], z * Y + py, px * 2 + c).start()

    def forward_plane(pan, rsem, fssem, frsem):
        for dx in (0, 1, 3, 2):
            rows = pl.ds(xat(-dx) * Y, Y)
            wait_bytes(pan.at[c, pl.ds(0, Y if dx else Y - 1)], rsem.at[dx])
            remote(pan.at[c, rows], pan.at[c, rows], fssem, frsem.at[dx], col, partner).start()

    def wait_plane(pan, frsem):
        for dx in (0, 1, 3, 2):
            wait_bytes(pan.at[other, pl.ds(xat(-dx) * Y, Y)], frsem.at[dx])

    def user_total(k, hooks):
        def emit(way, step, h, first=False):
            rows = pl.ds(h * H, H)
            j = piece_of[4 - step] if way == 0 or step == 0 else piece_of[step - 4]
            value = up[j, h * H:(h + 1) * H]
            if not first:
                value = value + got(way, step - 1, h)
            us[k, way, step, h * H:(h + 1) * H] = value
            remote(us.at[k, way, step, rows], ur.at[k, way, step, rows], us_ssem.at[k], us_rsem.at[way, step, h],
                   right if way == 0 else left, row).start()

        def got(way, step, h):
            wait_bytes(ur.at[k, way, step, pl.ds(h * H, H)], us_rsem.at[way, step, h])
            return ur[k, way, step, h * H:(h + 1) * H]

        def hook(*at):
            if at in hooks:
                hooks[at]()

        user_piece(k, 0)
        for h in range(NH // 2):
            emit(0, 0, early[0][h], True)
            emit(1, 0, early[1][h], True)
        if k == 0:
            hook('piece', 0)
            for step in range(1, 4):
                for way in range(2):
                    user_piece(k, 2 * step - 1 + way)
                    for h in early[way] + late[way]:
                        emit(way, step, h, step == 1 and h in late[way])
                hook('piece', step)
            user_piece(k, 7)
            hook('own')
        else:
            for way in range(2):
                user_piece(k, 1 + way)
                for h in late[way]:
                    emit(way, 1, h, True)
            for step in range(1, 4):
                hook('before', step)
                if step < 3:
                    user_piece(k, 2 * step + 1)
                    user_piece(k, 2 * step + 2)
                else:
                    user_piece(k, 7)
                for h in range(NH // 2):
                    for way in range(2):
                        emit(way, step, early[way][h])
                if step < 3:
                    for h in range(NH // 2):
                        for way in range(2):
                            emit(way, step + 1, late[way][h])
                hook('after', step)
        parts = []
        for h in range(NH):
            parts.append(up[7, h * H:(h + 1) * H] + got(0, 3, h) + got(1, 3, h))
        new_user = jnp.concatenate(parts, axis=0).astype(BF16)
        usum[...] += new_user.astype(F32)
        return new_user

    def items_next(k):
        new_item = item_total(k).astype(BF16)
        isum[...] += new_item.astype(F32)
        ei_pan[k + 1, c, spot] = new_item
        gather_plane(ei_pan.at[k + 1], ei_ssem.at[k + 1], ei_rsem.at[k + 1])

    def items_forward(k):
        forward_plane(ei_pan.at[k], ei_rsem.at[k], fw_ssem.at[k], fw_rsem.at[k])

    def items_wait(k):
        wait_plane(ei_pan.at[k], fw_rsem.at[k])

    def items0():
        item_parts(0)
        item_send(0)

    items_wait(0)
    new_user = user_total(0, {('piece', 0): lambda: hop0(2), ('piece', 1): last0, ('own',): items0})
    begin1, hop1, last1 = gather_user(1)
    begin1(new_user)
    hop1(0)
    hop1(1)
    items_next(0)
    hop1(2)
    last1()
    item_parts(1)
    items_forward(1)
    item_send(1)
    items_wait(1)
    new_user = user_total(1, {('after', 2): lambda: items_next(1)})
    begin2, hop2, last2 = gather_user(2)
    begin2(new_user)
    items_forward(2)
    items_wait(2)

    def tail2():
        last2()
        item_parts(2)

    user_total(2, {('before', 1): lambda: hop2(0), ('before', 2): lambda: hop2(1), ('before', 3): lambda: hop2(2),
                   ('after', 3): tail2})
    final_user = (usum[...] / (LAYERS + 1)).astype(BF16)
    fu_v[...] = final_user
    outs = [pltpu.make_async_copy(fu_v, fu_hbm, out_sem.at[0])]
    outs[0].start()

    qs[...] = jnp.dot(hot[...], final_user, preferred_element_type=F32).astype(BF16).reshape(2, G // 2, QB, E)
    to_partner = remote(qs.at[other], qp, q_ssem.at[0], q_rsem.at[0], col, partner)
    to_partner.start()
    to_partner.wait_recv()
    qt[...] = (qs[c].astype(F32) + qp[...].astype(F32)).astype(BF16)
    for slot, dx, py, px in plane():
        remote(qt.at[px * Y + py], qr.at[slot], q_ssem.at[1], q_rsem.at[1], z * Y + py, px * 2 + c).start()
    item_send(2)
    wait_bytes(qr, q_rsem.at[1])
    total = qt[spot].astype(F32)
    for slot in range(G // 2 - 1):
        total = total + qr[slot].astype(F32)
    qzs[...] = total.astype(BF16)
    for d in (4, 3, 5, 2, 6, 1, 7):
        remote(qzs, qz.at[d - 1], q_ssem.at[2], q_rsem.at[2], zat(d) * Y + y, row).start()
    wait_bytes(qz, q_rsem.at[2])
    for d in range(Z - 1):
        total = total + qz[d].astype(F32)
    qall[c, spot] = total.astype(BF16)
    gather_plane(qall, q_ssem.at[3], qg_rsem)
    new_item = item_total(2).astype(BF16)
    fi_v[...] = ((isum[...] + new_item.astype(F32)) / (LAYERS + 1)).astype(BF16)
    outs.append(pltpu.make_async_copy(fi_v, fi_hbm, out_sem.at[1]))
    outs[1].start()
    forward_plane(qall, qg_rsem, q_ssem.at[4], qf_rsem)
    outs.append(pltpu.make_async_copy(qall.at[c], q_hbm.at[c], out_sem.at[2]))
    outs[2].start()
    wait_plane(qall, qf_rsem)
    outs.append(pltpu.make_async_copy(qall.at[other], q_hbm.at[other], out_sem.at[3]))
    outs[3].start()

    wait_bytes(rs_y, rs_ssem.at[0])
    wait_bytes(rs_z.at[pl.ds(0, Z - 1)], rs_ssem.at[1])
    wait_bytes(cs_row.at[pl.ds(0, R - 1)], cs_ssem.at[0])
    wait_bytes(cs_y.at[pl.ds(0, Y - 1)], cs_ssem.at[1])
    wait_bytes(msend.at[pl.ds(0, Y - 1)], mask_ssem)
    for k in range(LAYERS):
        wait_bytes(ei_pan.at[k, 0, pl.ds(0, G // 2 - 1)], ei_ssem.at[k])
        wait_bytes(ei_pan.at[k, 0], fw_ssem.at[k])
        wait_bytes(pr.at[k], pr_ssem.at[k])
        wait_bytes(ir.at[k], ip_ssem.at[k])
        wait_bytes(up.at[pl.ds(0, 7)], us_ssem.at[k])
        wait_bytes(eu_pan.at[k, pl.ds(0, 7)], ag_ssem.at[k])
    to_partner.wait_send()
    wait_bytes(qr, q_ssem.at[1])
    wait_bytes(qz, q_ssem.at[2])
    wait_bytes(qr, q_ssem.at[3])
    wait_bytes(qt, q_ssem.at[4])
    for out in outs:
        out.wait()


def finish(user_ref, item_ref, picked_ref, fu_ref, fi_ref, sc_ref):
    fu_ref[...] = user_ref[...]
    fi_ref[...] = item_ref[...]
    sc_ref[...] = lax.dot_general(item_ref[...], picked_ref[...], CONTRACT_LANES, preferred_element_type=F32)


def propagate(mask, user, item, queries):
    dma = pltpu.SemaphoreType.DMA
    vmem, hbm = pl.BlockSpec(memory_space=pltpu.VMEM), pl.BlockSpec(memory_space=pl.ANY)
    L, N = LAYERS, G // 2
    final_user, final_item, picked = pl.pallas_call(
        kernel,
        out_shape=(jax.ShapeDtypeStruct((UB, E), BF16), jax.ShapeDtypeStruct((IB, E), BF16),
                   jax.ShapeDtypeStruct((2, N, QB, E), BF16)),
        in_specs=[hbm, vmem, vmem, vmem],
        out_specs=(hbm, hbm, hbm),
        scratch_shapes=[
            pltpu.VMEM((Z, Y * UB, E), jnp.int32),
            pltpu.VMEM((Y, Z, UB, E), BF16),
            pltpu.VMEM((Z, Y - 1, UB, E), BF16),
            pltpu.VMEM((Y, Z, UB, E), BF16),
            pltpu.VMEM((Y, E, Z * UB), BF16),
            pltpu.VMEM((Y, Z, UB), F32),
            pltpu.VMEM((Y - 1, Z, UB), F32),
            pltpu.VMEM((Z, Z, UB), F32),
            pltpu.VMEM((1, E), F32),
            pltpu.VMEM((R, 1, E), F32),
            pltpu.VMEM((Y, 1, E), F32),
            pltpu.VMEM((Z, UB), F32),
            pltpu.VMEM((Y, 1, E), F32),
            pltpu.VMEM((L, Z, UB, E), BF16),
            pltpu.VMEM((L, 2, N, IB, E), BF16),
            pltpu.VMEM((Z, UB, E), F32),
            pltpu.VMEM((L, 2, 4, UB, E), F32),
            pltpu.VMEM((L, 2, 4, UB, E), F32),
            pltpu.VMEM((L, 2, N, IB, E), F32),
            pltpu.VMEM((L, Y, X, IB, E), F32),
            pltpu.VMEM((L, N, IB, E), F32),
            pltpu.VMEM((L, N - 1, IB, E), F32),
            pltpu.VMEM((NQ, UB), BF16),
            pltpu.VMEM((2, N, QB, E), BF16),
            pltpu.VMEM((N, QB, E), BF16),
            pltpu.VMEM((N, QB, E), BF16),
            pltpu.VMEM((N - 1, QB, E), BF16),
            pltpu.VMEM((Z - 1, QB, E), BF16),
            pltpu.VMEM((QB, E), BF16),
            pltpu.VMEM((2, N, QB, E), BF16),
            pltpu.VMEM((UB, E), BF16),
            pltpu.VMEM((IB, E), BF16),
            pltpu.VMEM((UB, E), F32),
            pltpu.VMEM((IB, E), F32),
            dma((Z,)), dma, dma((Z,)),
            dma((2,)), dma, dma((2, 4)),
            dma((2,)), dma((2,)),
            dma((L,)), dma((L, X)), dma((L,)), dma((L, X)),
            dma((L,)), dma((2, 4, NH)),
            dma((L,)), dma((L, Y)), dma((L,)), dma((L,)),
            dma((L,)), dma((2, 4, NH)),
            dma((5,)), dma((3,)), dma((X,)), dma((X,)),
            dma((4,)),
        ],
        compiler_params=pltpu.CompilerParams(collective_id=0, has_side_effects=True, vmem_limit_bytes=60 * 2**20),
    )(mask, user, item, queries.reshape(1, NQ))
    final_user, final_item, scores = pl.pallas_call(
        finish,
        out_shape=(jax.ShapeDtypeStruct((UB, E), BF16), jax.ShapeDtypeStruct((IB, E), BF16),
                   jax.ShapeDtypeStruct((IB, NQ), F32)),
        in_specs=[vmem, vmem, vmem],
        out_specs=(vmem, vmem, vmem),
    )(final_user, final_item, picked.reshape(NQ, E))
    return final_user, final_item, scores.T


def solution(mesh):
    return jax.shard_map(propagate, mesh=mesh,
                         in_specs=(P('row', 'col'), P(('row', 'col'), None), P(('col', 'row'), None), P()),
                         out_specs=(P(('row', 'col'), None), P(('col', 'row'), None), P(None, ('col', 'row'))),
                         check_vma=False)
```

```python
import jax
import jax.numpy as jnp
from jax import lax
from jax.experimental import pallas as pl
from jax.experimental.pallas import tpu as pltpu
from jax.sharding import PartitionSpec as P

LAYERS = 3
Z, Y, X = 8, 4, 4
R = 2 * X
G = Y * R
UB, IB = 128, 32
E = 256
NQ = 1024
QB = NQ // G
NH = 4
H = UB // NH
F32, BF16 = jnp.float32, jnp.bfloat16
MESH = pl.DeviceIdType.MESH
CONTRACT_ROWS = (((0,), (0,)), ((), ()))
CONTRACT_LANES = (((1,), (1,)), ((), ()))


def remote(src, dst, send_sem, recv_sem, col, row):
    return pltpu.make_async_remote_copy(src_ref=src, dst_ref=dst, send_sem=send_sem, recv_sem=recv_sem,
                                        device_id=(col, row), device_id_type=MESH)


def wait_bytes(ref, sem):
    pltpu.make_async_copy(ref, ref, sem).wait()


def kernel(mask_ref, user_ref, item_ref, query_ref, fu_hbm, fi_hbm, q_hbm,
           mask_v, msend, mrecv, adj, adjt, rs_send, rs_y, rs_z, cs_send, cs_row, cs_y, invu, invi,
           eu_pan, ei_pan, up, macc, us, ur, ip, pr, iq, ir, hot, qs, qp, qt, qr, qz, qzs, qall, fu_v, fi_v, usum, isum,
           load_sem, mask_ssem, mask_rsem, rs_ssem, rs_rsem, rz_rsem, cs_ssem, cs_rsem, ei_ssem, ei_rsem, fw_ssem, fw_rsem, us_ssem, us_rsem,
           pr_ssem, pr_rsem, ip_ssem, ip_rsem, ag_ssem, ag_rsem, q_ssem, q_rsem, qg_rsem, qf_rsem, out_sem):
    col = lax.axis_index('col')
    row = lax.axis_index('row')
    z, y = lax.div(col, Y), lax.rem(col, Y)
    x, c = lax.div(row, 2), lax.rem(row, 2)
    other = 1 - c
    partner = x * 2 + other
    spot = x * Y + y

    def zat(d):
        return lax.rem(z + (d % Z), Z)

    def yat(d):
        return lax.rem(y + (d % Y), Y)

    def xat(d):
        return lax.rem(x + (d % X), X)

    def plane():
        for dx in (2, 1, 3, 0):
            for dy in (2, 1, 3, 0):
                if dy or dx:
                    yield dx * Y + dy - 1, dx, yat(dy), xat(dx)

    order = [4, 3, -3, 2, -2, 1, -1, 0]
    piece_of = {d: j for j, d in enumerate(order)}
    early = (list(range(NH // 2)), list(range(NH // 2, NH)))
    late = (early[1], early[0])
    right, left = zat(1) * Y + y, zat(-1) * Y + y

    loads = []
    for j, d in enumerate(order):
        zc = zat(d)
        load = pltpu.make_async_copy(mask_ref.at[pl.ds(zc * (Y * UB), Y * UB)], mask_v.at[j], load_sem.at[j])
        load.start()
        loads.append(load)

    barrier = pltpu.get_barrier_semaphore()
    for d in range(1, R):
        pl.semaphore_signal(barrier, inc=1, device_id=(col, lax.rem(row + d, R)), device_id_type=MESH)
    for d in range(1, Y):
        pl.semaphore_signal(barrier, inc=1, device_id=(z * Y + yat(d), row), device_id_type=MESH)
    for d in range(1, Z):
        pl.semaphore_signal(barrier, inc=1, device_id=(zat(d) * Y + y, row), device_id_type=MESH)

    ones_w = jnp.ones((8, E), BF16)
    colsum = jnp.zeros((8, E), F32)
    for j, d in enumerate(order):
        zc = zat(d)
        loads[j].wait()
        for p in range(Y):
            wide = mask_v[j, p * UB:(p + 1) * UB, :].astype(F32)
            block = wide.astype(BF16)
            msend[p, j] = block
            sums = lax.dot_general(ones_w, block, CONTRACT_LANES, preferred_element_type=F32)
            rs_send[p, pl.ds(zc, 1), :] = sums[0:1]
            colsum = colsum + jnp.sum(wide.reshape(UB // 8, 8, E), axis=0)
    cs_send[...] = jnp.sum(colsum, axis=0, keepdims=True)
    cs_row[row] = cs_send[...]
    ei_pan[0, c, spot] = item_ref[...]

    pl.semaphore_wait(barrier, R - 1 + Y - 1 + Z - 1)

    def send_mask(j):
        for d in range(1, Y):
            py = yat(d)
            remote(msend.at[py, j], mrecv.at[j, d - 1], mask_ssem, mask_rsem.at[j], z * Y + py, row).start()

    def gather_user(k):
        def send(way, step, h):
            src = eu_pan.at[k, zat(-step if way == 0 else step), pl.ds(h * H, H)]
            remote(src, src, ag_ssem.at[k], ag_rsem.at[way, step, h], right if way == 0 else left, row).start()

        def got(way, step, h):
            dst = eu_pan.at[k, zat(-step - 1 if way == 0 else step + 1), pl.ds(h * H, H)]
            wait_bytes(dst, ag_rsem.at[way, step, h])

        def begin(new_user):
            eu_pan[k, z] = new_user
            for h in range(NH):
                for way in range(2):
                    send(way, 0, (early[way] + late[way])[h])

        def hop(step):
            for h in range(NH):
                for way in range(2):
                    hh = (early[way] + late[way])[h]
                    got(way, step, hh)
                    if step < 2 or h < NH // 2:
                        send(way, step + 1, hh)

        def last():
            for h in range(NH // 2):
                for way in range(2):
                    got(way, 3, early[way][h])

        return begin, hop, last

    for d in range(1, Y):
        remote(rs_send.at[yat(d)], rs_y.at[d - 1], rs_ssem.at[0], rs_rsem, z * Y + yat(d), row).start()
    for d in range(1, R):
        remote(cs_send, cs_row.at[row], cs_ssem.at[0], cs_rsem.at[0], col, lax.rem(row + d, R)).start()
    for d in range(1, Y):
        remote(item_ref, ei_pan.at[0, c, spot], ei_ssem.at[0], ei_rsem.at[0, 0], z * Y + yat(d), row).start()
    send_mask(0)
    begin0, hop0, last0 = gather_user(0)
    begin0(user_ref[...])
    send_mask(1)

    usum[...] = user_ref[...].astype(F32)
    isum[...] = item_ref[...].astype(F32)
    wait_bytes(rs_y, rs_rsem)
    rs_z[z] = rs_send[y] + rs_y[0] + rs_y[1] + rs_y[2]
    for d in (4, 3, 5, 2, 6, 1, 7):
        remote(rs_z.at[z], rs_z.at[z], rs_ssem.at[1], rz_rsem, zat(d) * Y + y, row).start()

    wait_bytes(ei_pan.at[0, c, pl.ds(0, Y - 1)], ei_rsem.at[0, 0])
    own = ei_pan.at[0, c, pl.ds(x * Y, Y)]
    for d in range(1, X):
        remote(own, own, ei_ssem.at[0], ei_rsem.at[0, d], col, xat(d) * 2 + c).start()
    remote(own, own, fw_ssem.at[0], fw_rsem.at[0, 0], col, partner).start()

    wait_bytes(cs_row.at[pl.ds(0, R - 1)], cs_rsem.at[0])
    deg = cs_row[0]
    for r in range(1, R):
        deg = deg + cs_row[r]
    cs_y[y] = deg
    for d in range(1, Y):
        remote(cs_y.at[y], cs_y.at[y], cs_ssem.at[1], cs_rsem.at[1], z * Y + yat(d), row).start()
    for j in range(2, Z):
        send_mask(j)

    base = (row * (Z * Y) + col) * UB
    ids = lax.broadcasted_iota(jnp.int32, (UB, NQ), 0) + base
    hot[...] = jnp.where(ids == query_ref[...], 1.0, 0.0).T.astype(BF16)

    hop0(0)
    for d in (1, 3, 2):
        rows = pl.ds(xat(-d) * Y, Y)
        wait_bytes(ei_pan.at[0, c, rows], ei_rsem.at[0, d])
        remote(ei_pan.at[0, c, rows], ei_pan.at[0, c, rows], fw_ssem.at[0], fw_rsem.at[0, d], col, partner).start()
    wait_bytes(cs_y.at[pl.ds(0, Y - 1)], cs_rsem.at[1])
    for s in range(Y):
        invi[s] = lax.rsqrt(jnp.maximum(cs_y[s], 1.0))
    wait_bytes(rs_z.at[pl.ds(0, Z - 1)], rz_rsem)
    deg = rs_z[0]
    for d in range(1, Z):
        deg = deg + rs_z[d]
    invu[...] = lax.rsqrt(jnp.maximum(deg, 1.0))

    def make_adj(j, zc):
        wait_bytes(mrecv.at[j], mask_rsem.at[j])
        iu = jnp.broadcast_to(invu[pl.ds(zc, 1), :], (UB, UB)).T
        iu = jnp.concatenate([iu, iu], axis=1)
        for d in range(Y):
            s = yat(-d)
            m = (msend[y, j] if d == 0 else mrecv[j, d - 1]).astype(F32)
            a = (iu * m) * invi[s]
            adj[s, zc] = a.astype(BF16)
            adjt[s, :, pl.ds(pl.multiple_of(zc * UB, UB), UB)] = a.T.astype(BF16)

    def user_piece(k, j):
        zc = zat(order[j])
        if k == 0:
            make_adj(j, zc)
        acc = None
        for s in range(Y):
            panel = jnp.concatenate([ei_pan[k, cc, xx * Y + s] for xx in range(X) for cc in range(2)], axis=0)
            t = jnp.dot(adj[s, zc], panel, preferred_element_type=F32)
            acc = t if acc is None else acc + t
        up[j] = acc

    def item_share(k, product):
        for j, dy in enumerate((2, 1, 3, 0)):
            s = yat(dy)
            part = product(s).reshape(X, 2, IB, E)
            for xx in range(X):
                for cc in range(2):
                    ip[k, cc, s * X + xx] = part[xx, cc]
            remote(ip.at[k, other, pl.ds(s * X, X)], pr.at[k, j], pr_ssem.at[k], pr_rsem.at[k, j], col, partner).start()

    def item_parts(k):
        eu = eu_pan[k].reshape(Z * UB, E)
        item_share(k, lambda s: jnp.dot(adjt[s], eu, preferred_element_type=F32))

    def item_pair(n):
        near = [zat(d) for d in ((0, 1), (-1, 2), (-2, 3), (-3, 4))[n]]
        eu = jnp.concatenate([eu_pan[1, zc] for zc in near], axis=0)

        def add(s):
            lhs = jnp.concatenate([adjt[s, :, pl.ds(pl.multiple_of(zc * UB, UB), UB)] for zc in near], axis=1)
            part = jnp.dot(lhs, eu, preferred_element_type=F32)
            return part + macc[s] if n else part

        if n < 3:
            for s in range(Y):
                macc[s] = add(s)
        else:
            item_share(1, add)

    def item_send(k):
        for j, dy in enumerate((2, 1, 3, 0)):
            s = yat(dy)
            wait_bytes(pr.at[k, j], pr_rsem.at[k, j])
            iq[k, pl.ds(s * X, X)] = ip[k, c, pl.ds(s * X, X)] + pr[k, j]
            for dx in (2, 1, 3, 0):
                if dy or dx:
                    px = xat(dx)
                    remote(iq.at[k, s * X + px], ir.at[k, dy * X + dx - 1], ip_ssem.at[k], ip_rsem.at[k],
                           z * Y + s, px * 2 + c).start()

    def item_total(k):
        wait_bytes(ir.at[k], ip_rsem.at[k])
        total = iq[k, y * X + x]
        for slot in range(G // 2 - 1):
            total = total + ir[k, slot]
        return total

    def gather_plane(pan, ssem, rsem):
        for slot, dx, py, px in plane():
            remote(pan.at[c, spot], pan.at[c, spot], ssem, rsem.at[dx], z * Y + py, px * 2 + c).start()

    def forward_plane(pan, rsem, fssem, frsem):
        for dx in (0, 1, 3, 2):
            rows = pl.ds(xat(-dx) * Y, Y)
            wait_bytes(pan.at[c, pl.ds(0, Y if dx else Y - 1)], rsem.at[dx])
            remote(pan.at[c, rows], pan.at[c, rows], fssem, frsem.at[dx], col, partner).start()

    def wait_plane(pan, frsem):
        for dx in (0, 1, 3, 2):
            wait_bytes(pan.at[other, pl.ds(xat(-dx) * Y, Y)], frsem.at[dx])

    def user_total(k, hooks):
        def emit(way, step, h, first=False):
            rows = pl.ds(h * H, H)
            j = piece_of[4 - step] if way == 0 or step == 0 else piece_of[step - 4]
            value = up[j, h * H:(h + 1) * H]
            if not first:
                value = value + got(way, step - 1, h)
            us[k, way, step, h * H:(h + 1) * H] = value
            remote(us.at[k, way, step, rows], ur.at[k, way, step, rows], us_ssem.at[k], us_rsem.at[way, step, h],
                   right if way == 0 else left, row).start()

        def got(way, step, h):
            wait_bytes(ur.at[k, way, step, pl.ds(h * H, H)], us_rsem.at[way, step, h])
            return ur[k, way, step, h * H:(h + 1) * H]

        def hook(*at):
            if at in hooks:
                hooks[at]()

        user_piece(k, 0)
        for h in range(NH // 2):
            emit(0, 0, early[0][h], True)
            emit(1, 0, early[1][h], True)
        if k == 0:
            hook('piece', 0)
            for step in range(1, 4):
                for way in range(2):
                    user_piece(k, 2 * step - 1 + way)
                    for h in early[way] + late[way]:
                        emit(way, step, h, step == 1 and h in late[way])
                hook('piece', step)
            user_piece(k, 7)
            hook('own')
        else:
            for way in range(2):
                user_piece(k, 1 + way)
                for h in late[way]:
                    emit(way, 1, h, True)
            for step in range(1, 4):
                hook('before', step)
                if step < 3:
                    user_piece(k, 2 * step + 1)
                    user_piece(k, 2 * step + 2)
                else:
                    user_piece(k, 7)
                for h in range(NH // 2):
                    for way in range(2):
                        emit(way, step, early[way][h])
                if step < 3:
                    for h in range(NH // 2):
                        for way in range(2):
                            emit(way, step + 1, late[way][h])
                hook('after', step)
        parts = []
        for h in range(NH):
            parts.append(up[7, h * H:(h + 1) * H] + got(0, 3, h) + got(1, 3, h))
        new_user = jnp.concatenate(parts, axis=0).astype(BF16)
        usum[...] += new_user.astype(F32)
        return new_user

    def items_next(k):
        new_item = item_total(k).astype(BF16)
        isum[...] += new_item.astype(F32)
        ei_pan[k + 1, c, spot] = new_item
        gather_plane(ei_pan.at[k + 1], ei_ssem.at[k + 1], ei_rsem.at[k + 1])

    def items_forward(k):
        forward_plane(ei_pan.at[k], ei_rsem.at[k], fw_ssem.at[k], fw_rsem.at[k])

    def items_wait(k):
        wait_plane(ei_pan.at[k], fw_rsem.at[k])

    def items0():
        item_parts(0)
        item_send(0)

    hop0(1)
    items_wait(0)
    new_user = user_total(0, {('piece', 0): lambda: hop0(2), ('piece', 1): last0, ('own',): items0})
    begin1, hop1, last1 = gather_user(1)
    begin1(new_user)
    hop1(0)
    item_pair(0)
    hop1(1)
    item_pair(1)
    items_next(0)
    hop1(2)
    item_pair(2)
    last1()
    item_pair(3)
    items_forward(1)
    item_send(1)
    items_wait(1)
    new_user = user_total(1, {('after', 2): lambda: items_next(1)})
    begin2, hop2, last2 = gather_user(2)
    begin2(new_user)
    items_forward(2)
    items_wait(2)

    user_total(2, {('after', 1): lambda: hop2(0), ('after', 2): lambda: hop2(1), ('after', 3): lambda: hop2(2)})
    final_user = (usum[...] / (LAYERS + 1)).astype(BF16)
    fu_v[...] = final_user
    outs = [pltpu.make_async_copy(fu_v, fu_hbm, out_sem.at[0])]
    outs[0].start()

    qs[...] = jnp.dot(hot[...], final_user, preferred_element_type=F32).astype(BF16).reshape(2, G // 2, QB, E)
    to_partner = remote(qs.at[other], qp, q_ssem.at[0], q_rsem.at[0], col, partner)
    to_partner.start()
    to_partner.wait_recv()
    qt[...] = (qs[c].astype(F32) + qp[...].astype(F32)).astype(BF16)
    for slot, dx, py, px in plane():
        remote(qt.at[px * Y + py], qr.at[slot], q_ssem.at[1], q_rsem.at[1], z * Y + py, px * 2 + c).start()
    last2()
    item_parts(2)
    item_send(2)
    wait_bytes(qr, q_rsem.at[1])
    total = qt[spot].astype(F32)
    for slot in range(G // 2 - 1):
        total = total + qr[slot].astype(F32)
    qzs[...] = total.astype(BF16)
    for d in (4, 3, 5, 2, 6, 1, 7):
        remote(qzs, qz.at[d - 1], q_ssem.at[2], q_rsem.at[2], zat(d) * Y + y, row).start()
    wait_bytes(qz, q_rsem.at[2])
    for d in range(Z - 1):
        total = total + qz[d].astype(F32)
    qall[c, spot] = total.astype(BF16)
    gather_plane(qall, q_ssem.at[3], qg_rsem)
    new_item = item_total(2).astype(BF16)
    fi_v[...] = ((isum[...] + new_item.astype(F32)) / (LAYERS + 1)).astype(BF16)
    outs.append(pltpu.make_async_copy(fi_v, fi_hbm, out_sem.at[1]))
    outs[1].start()
    forward_plane(qall, qg_rsem, q_ssem.at[4], qf_rsem)
    outs.append(pltpu.make_async_copy(qall.at[c], q_hbm.at[c], out_sem.at[2]))
    outs[2].start()
    wait_plane(qall, qf_rsem)
    outs.append(pltpu.make_async_copy(qall.at[other], q_hbm.at[other], out_sem.at[3]))
    outs[3].start()

    wait_bytes(rs_y, rs_ssem.at[0])
    wait_bytes(rs_z.at[pl.ds(0, Z - 1)], rs_ssem.at[1])
    wait_bytes(cs_row.at[pl.ds(0, R - 1)], cs_ssem.at[0])
    wait_bytes(cs_y.at[pl.ds(0, Y - 1)], cs_ssem.at[1])
    wait_bytes(msend.at[pl.ds(0, Y - 1)], mask_ssem)
    for k in range(LAYERS):
        wait_bytes(ei_pan.at[k, 0, pl.ds(0, G // 2 - 1)], ei_ssem.at[k])
        wait_bytes(ei_pan.at[k, 0], fw_ssem.at[k])
        wait_bytes(pr.at[k], pr_ssem.at[k])
        wait_bytes(ir.at[k], ip_ssem.at[k])
        wait_bytes(up.at[pl.ds(0, 7)], us_ssem.at[k])
        wait_bytes(eu_pan.at[k, pl.ds(0, 7)], ag_ssem.at[k])
    to_partner.wait_send()
    wait_bytes(qr, q_ssem.at[1])
    wait_bytes(qz, q_ssem.at[2])
    wait_bytes(qr, q_ssem.at[3])
    wait_bytes(qt, q_ssem.at[4])
    for out in outs:
        out.wait()


def finish(user_ref, item_ref, picked_ref, fu_ref, fi_ref, sc_ref):
    fu_ref[...] = user_ref[...]
    fi_ref[...] = item_ref[...]
    sc_ref[...] = lax.dot_general(item_ref[...], picked_ref[...], CONTRACT_LANES, preferred_element_type=F32)


def propagate(mask, user, item, queries):
    dma = pltpu.SemaphoreType.DMA
    vmem, hbm = pl.BlockSpec(memory_space=pltpu.VMEM), pl.BlockSpec(memory_space=pl.ANY)
    L, N = LAYERS, G // 2
    final_user, final_item, picked = pl.pallas_call(
        kernel,
        out_shape=(jax.ShapeDtypeStruct((UB, E), BF16), jax.ShapeDtypeStruct((IB, E), BF16),
                   jax.ShapeDtypeStruct((2, N, QB, E), BF16)),
        in_specs=[hbm, vmem, vmem, vmem],
        out_specs=(hbm, hbm, hbm),
        scratch_shapes=[
            pltpu.VMEM((Z, Y * UB, E), jnp.int32),
            pltpu.VMEM((Y, Z, UB, E), BF16),
            pltpu.VMEM((Z, Y - 1, UB, E), BF16),
            pltpu.VMEM((Y, Z, UB, E), BF16),
            pltpu.VMEM((Y, E, Z * UB), BF16),
            pltpu.VMEM((Y, Z, UB), F32),
            pltpu.VMEM((Y - 1, Z, UB), F32),
            pltpu.VMEM((Z, Z, UB), F32),
            pltpu.VMEM((1, E), F32),
            pltpu.VMEM((R, 1, E), F32),
            pltpu.VMEM((Y, 1, E), F32),
            pltpu.VMEM((Z, UB), F32),
            pltpu.VMEM((Y, 1, E), F32),
            pltpu.VMEM((L, Z, UB, E), BF16),
            pltpu.VMEM((L, 2, N, IB, E), BF16),
            pltpu.VMEM((Z, UB, E), F32),
            pltpu.VMEM((Y, E, E), F32),
            pltpu.VMEM((L, 2, 4, UB, E), F32),
            pltpu.VMEM((L, 2, 4, UB, E), F32),
            pltpu.VMEM((L, 2, N, IB, E), F32),
            pltpu.VMEM((L, Y, X, IB, E), F32),
            pltpu.VMEM((L, N, IB, E), F32),
            pltpu.VMEM((L, N - 1, IB, E), F32),
            pltpu.VMEM((NQ, UB), BF16),
            pltpu.VMEM((2, N, QB, E), BF16),
            pltpu.VMEM((N, QB, E), BF16),
            pltpu.VMEM((N, QB, E), BF16),
            pltpu.VMEM((N - 1, QB, E), BF16),
            pltpu.VMEM((Z - 1, QB, E), BF16),
            pltpu.VMEM((QB, E), BF16),
            pltpu.VMEM((2, N, QB, E), BF16),
            pltpu.VMEM((UB, E), BF16),
            pltpu.VMEM((IB, E), BF16),
            pltpu.VMEM((UB, E), F32),
            pltpu.VMEM((IB, E), F32),
            dma((Z,)), dma, dma((Z,)),
            dma((2,)), dma, dma,
            dma((2,)), dma((2,)),
            dma((L,)), dma((L, X)), dma((L,)), dma((L, X)),
            dma((L,)), dma((2, 4, NH)),
            dma((L,)), dma((L, Y)), dma((L,)), dma((L,)),
            dma((L,)), dma((2, 4, NH)),
            dma((5,)), dma((3,)), dma((X,)), dma((X,)),
            dma((4,)),
        ],
        compiler_params=pltpu.CompilerParams(collective_id=0, has_side_effects=True, vmem_limit_bytes=60 * 2**20),
    )(mask, user, item, queries.reshape(1, NQ))
    final_user, final_item, scores = pl.pallas_call(
        finish,
        out_shape=(jax.ShapeDtypeStruct((UB, E), BF16), jax.ShapeDtypeStruct((IB, E), BF16),
                   jax.ShapeDtypeStruct((IB, NQ), F32)),
        in_specs=[vmem, vmem, vmem],
        out_specs=(vmem, vmem, vmem),
    )(final_user, final_item, picked.reshape(NQ, E))
    return final_user, final_item, scores.T


def solution(mesh):
    return jax.shard_map(propagate, mesh=mesh,
                         in_specs=(P('row', 'col'), P(('row', 'col'), None), P(('col', 'row'), None), P()),
                         out_specs=(P(('row', 'col'), None), P(('col', 'row'), None), P(None, ('col', 'row'))),
                         check_vma=False)
```

```python
import jax
import jax.numpy as jnp
from jax import lax
from jax.experimental import pallas as pl
from jax.experimental.pallas import tpu as pltpu
from jax.sharding import PartitionSpec as P

LAYERS = 3
Z, Y, X = 8, 4, 4
R = 2 * X
G = Y * R
UB, IB = 128, 32
E = 256
NQ = 1024
QB = NQ // G
NH = 4
H = UB // NH
F32, BF16 = jnp.float32, jnp.bfloat16
MESH = pl.DeviceIdType.MESH
CONTRACT_ROWS = (((0,), (0,)), ((), ()))
CONTRACT_LANES = (((1,), (1,)), ((), ()))


def remote(src, dst, send_sem, recv_sem, col, row):
    return pltpu.make_async_remote_copy(src_ref=src, dst_ref=dst, send_sem=send_sem, recv_sem=recv_sem,
                                        device_id=(col, row), device_id_type=MESH)


def wait_bytes(ref, sem):
    pltpu.make_async_copy(ref, ref, sem).wait()


def kernel(mask_ref, user_hbm, item_hbm, query_hbm, fu_out, fi_out, q_out,
           mask_v, user_ref, item_ref, query_ref, msend, mrecv, adj, adjt, rs_send, rs_y, rs_z, cs_send, cs_row, cs_y, invu, invi,
           eu_pan, ei_pan, up, macc, us, ur, ip, pr, iq, ir, hot, qs, qp, qt, qr, qz, qzs, qall, fu_v, fi_v, usum, isum,
           load_sem, mask_ssem, mask_rsem, rs_ssem, rs_rsem, rz_rsem, cs_ssem, cs_rsem, ei_ssem, ei_rsem, fw_ssem, fw_rsem, us_ssem, us_rsem,
           pr_ssem, pr_rsem, ip_ssem, ip_rsem, ag_ssem, ag_rsem, q_ssem, q_rsem, qg_rsem, qf_rsem, out_sem):
    col = lax.axis_index('col')
    row = lax.axis_index('row')
    z, y = lax.div(col, Y), lax.rem(col, Y)
    x, c = lax.div(row, 2), lax.rem(row, 2)
    other = 1 - c
    partner = x * 2 + other
    spot = x * Y + y

    def zat(d):
        return lax.rem(z + (d % Z), Z)

    def yat(d):
        return lax.rem(y + (d % Y), Y)

    def xat(d):
        return lax.rem(x + (d % X), X)

    def plane():
        for dx in (2, 1, 3, 0):
            for dy in (2, 1, 3, 0):
                if dy or dx:
                    yield dx * Y + dy - 1, dx, yat(dy), xat(dx)

    order = [4, 3, -3, 2, -2, 1, -1, 0]
    piece_of = {d: j for j, d in enumerate(order)}
    place = lax.rem(z, Z // 2)

    def ring_order(step, run):
        if step == 0:
            pl.when(place == 0)(lambda: run(((1,), (0,))))
            pl.when(place == Z // 2 - 1)(lambda: run(((0,), (1,))))
            pl.when((place > 0) & (place < Z // 2 - 1))(lambda: run(((0, 1),)))
        else:
            pl.when(place < Z // 4)(lambda: run(((1,), (0,))))
            pl.when(place >= Z // 4)(lambda: run(((0,), (1,))))

    early = (list(range(NH // 2)), list(range(NH // 2, NH)))
    late = (early[1], early[0])
    right, left = zat(1) * Y + y, zat(-1) * Y + y

    loads = []
    for j, d in enumerate(order):
        zc = zat(d)
        load = pltpu.make_async_copy(mask_ref.at[pl.ds(zc * (Y * UB), Y * UB)], mask_v.at[j], load_sem.at[j])
        load.start()
        loads.append(load)

    small = []
    for i, (src, dst) in enumerate(((user_hbm, user_ref), (item_hbm, item_ref), (query_hbm, query_ref))):
        small.append(pltpu.make_async_copy(src, dst, load_sem.at[Z + i]))
        small[i].start()

    barrier = pltpu.get_barrier_semaphore()
    for d in range(1, R):
        pl.semaphore_signal(barrier, inc=1, device_id=(col, lax.rem(row + d, R)), device_id_type=MESH)
    for d in range(1, Y):
        pl.semaphore_signal(barrier, inc=1, device_id=(z * Y + yat(d), row), device_id_type=MESH)
    for d in range(1, Z):
        pl.semaphore_signal(barrier, inc=1, device_id=(zat(d) * Y + y, row), device_id_type=MESH)

    ones_w = jnp.ones((8, E), BF16)
    colsum = jnp.zeros((8, E), F32)

    def send_mask(j):
        for d in range(1, Y):
            py = yat(d)
            remote(msend.at[py, j], mrecv.at[j, d - 1], mask_ssem, mask_rsem.at[j], z * Y + py, row).start()

    for j, d in enumerate(order):
        zc = zat(d)
        loads[j].wait()
        if j == 1:
            pl.semaphore_wait(barrier, R - 1 + Y - 1 + Z - 1)
            send_mask(0)
        for p in range(Y):
            wide = mask_v[j, p * UB:(p + 1) * UB, :].astype(F32)
            block = wide.astype(BF16)
            msend[p, j] = block
            sums = lax.dot_general(ones_w, block, CONTRACT_LANES, preferred_element_type=F32)
            rs_send[p, pl.ds(zc, 1), :] = sums[0:1]
            colsum = colsum + jnp.sum(wide.reshape(UB // 8, 8, E), axis=0)
    cs_send[...] = jnp.sum(colsum, axis=0, keepdims=True)
    cs_row[row] = cs_send[...]
    for load in small:
        load.wait()
    ei_pan[0, c, spot] = item_ref[...]

    def gather_user(k):
        def send(way, step, h):
            src = eu_pan.at[k, zat(-step if way == 0 else step), pl.ds(h * H, H)]
            remote(src, src, ag_ssem.at[k], ag_rsem.at[way, step, h], right if way == 0 else left, row).start()

        def got(way, step, h):
            dst = eu_pan.at[k, zat(-step - 1 if way == 0 else step + 1), pl.ds(h * H, H)]
            wait_bytes(dst, ag_rsem.at[way, step, h])

        def begin(new_user):
            eu_pan[k, z] = new_user
            for h in range(NH):
                for way in range(2):
                    send(way, 0, (early[way] + late[way])[h])

        def hop(step):
            def run(groups):
                for ways in groups:
                    for h in range(NH):
                        for way in ways:
                            hh = (early[way] + late[way])[h]
                            got(way, step, hh)
                            if step < 2 or h < NH // 2:
                                send(way, step + 1, hh)

            ring_order(step, run)

        def last():
            for h in range(NH // 2):
                for way in range(2):
                    got(way, 3, early[way][h])

        return begin, hop, last

    for d in range(1, Y):
        remote(rs_send.at[yat(d)], rs_y.at[d - 1], rs_ssem.at[0], rs_rsem, z * Y + yat(d), row).start()
    for d in range(1, R):
        remote(cs_send, cs_row.at[row], cs_ssem.at[0], cs_rsem.at[0], col, lax.rem(row + d, R)).start()
    for d in range(1, Y):
        remote(item_ref, ei_pan.at[0, c, spot], ei_ssem.at[0], ei_rsem.at[0, 0], z * Y + yat(d), row).start()
    begin0, hop0, last0 = gather_user(0)
    begin0(user_ref[...])
    send_mask(1)

    usum[...] = user_ref[...].astype(F32)
    isum[...] = item_ref[...].astype(F32)
    wait_bytes(rs_y, rs_rsem)
    rs_z[z] = rs_send[y] + rs_y[0] + rs_y[1] + rs_y[2]
    for d in (4, 3, 5, 2, 6, 1, 7):
        remote(rs_z.at[z], rs_z.at[z], rs_ssem.at[1], rz_rsem, zat(d) * Y + y, row).start()

    wait_bytes(ei_pan.at[0, c, pl.ds(0, Y - 1)], ei_rsem.at[0, 0])
    own = ei_pan.at[0, c, pl.ds(x * Y, Y)]
    for d in range(1, X):
        remote(own, own, ei_ssem.at[0], ei_rsem.at[0, d], col, xat(d) * 2 + c).start()
    remote(own, own, fw_ssem.at[0], fw_rsem.at[0, 0], col, partner).start()

    wait_bytes(cs_row.at[pl.ds(0, R - 1)], cs_rsem.at[0])
    deg = cs_row[0]
    for r in range(1, R):
        deg = deg + cs_row[r]
    cs_y[y] = deg
    for d in range(1, Y):
        remote(cs_y.at[y], cs_y.at[y], cs_ssem.at[1], cs_rsem.at[1], z * Y + yat(d), row).start()
    for j in range(2, Z):
        send_mask(j)

    base = (row * (Z * Y) + col) * UB
    ids = lax.broadcasted_iota(jnp.int32, (UB, NQ), 0) + base
    hot[...] = jnp.where(ids == query_ref[...], 1.0, 0.0).T.astype(BF16)

    hop0(0)
    for d in (1, 3, 2):
        rows = pl.ds(xat(-d) * Y, Y)
        wait_bytes(ei_pan.at[0, c, rows], ei_rsem.at[0, d])
        remote(ei_pan.at[0, c, rows], ei_pan.at[0, c, rows], fw_ssem.at[0], fw_rsem.at[0, d], col, partner).start()
    wait_bytes(cs_y.at[pl.ds(0, Y - 1)], cs_rsem.at[1])
    for s in range(Y):
        invi[s] = lax.rsqrt(jnp.maximum(cs_y[s], 1.0))
    wait_bytes(rs_z.at[pl.ds(0, Z - 1)], rz_rsem)
    deg = rs_z[0]
    for d in range(1, Z):
        deg = deg + rs_z[d]
    invu[...] = lax.rsqrt(jnp.maximum(deg, 1.0))

    def make_adj(j, zc):
        wait_bytes(mrecv.at[j], mask_rsem.at[j])
        iu = jnp.broadcast_to(invu[pl.ds(zc, 1), :], (UB, UB)).T
        iu = jnp.concatenate([iu, iu], axis=1)
        for d in range(Y):
            s = yat(-d)
            m = (msend[y, j] if d == 0 else mrecv[j, d - 1]).astype(F32)
            a = (iu * m) * invi[s]
            adj[s, zc] = a.astype(BF16)
            adjt[s, :, pl.ds(pl.multiple_of(zc * UB, UB), UB)] = a.T.astype(BF16)

    def user_piece(k, j):
        zc = zat(order[j])
        if k == 0:
            make_adj(j, zc)
        acc = None
        for s in range(Y):
            panel = jnp.concatenate([ei_pan[k, cc, xx * Y + s] for xx in range(X) for cc in range(2)], axis=0)
            t = jnp.dot(adj[s, zc], panel, preferred_element_type=F32)
            acc = t if acc is None else acc + t
        up[j] = acc

    def item_share(k, product, lag=Y):
        for j, dy in enumerate((2, 1, 3, 0)):
            s = yat(dy)
            part = product(s).reshape(X, 2, IB, E)
            for xx in range(X):
                for cc in range(2):
                    ip[k, cc, s * X + xx] = part[xx, cc]
            remote(ip.at[k, other, pl.ds(s * X, X)], pr.at[k, j], pr_ssem.at[k], pr_rsem.at[k, j], col, partner).start()
            if j >= lag:
                item_send(k, j - lag)

    def item_parts(k):
        eu = eu_pan[k].reshape(Z * UB, E)
        item_share(k, lambda s: jnp.dot(adjt[s], eu, preferred_element_type=F32), lag=3)

    def item_pair(n):
        near = [zat(d) for d in ((0, 1), (-1, 2), (-2, 3), (-3, 4))[n]]
        eu = jnp.concatenate([eu_pan[1, zc] for zc in near], axis=0)

        def add(s):
            lhs = jnp.concatenate([adjt[s, :, pl.ds(pl.multiple_of(zc * UB, UB), UB)] for zc in near], axis=1)
            part = jnp.dot(lhs, eu, preferred_element_type=F32)
            return part + macc[s] if n else part

        if n < 3:
            for s in range(Y):
                macc[s] = add(s)
        else:
            item_share(1, add)

    def item_send(k, j):
        dy = (2, 1, 3, 0)[j]
        s = yat(dy)
        wait_bytes(pr.at[k, j], pr_rsem.at[k, j])
        iq[k, pl.ds(s * X, X)] = ip[k, c, pl.ds(s * X, X)] + pr[k, j]
        for dx in (2, 1, 3, 0):
            if dy or dx:
                px = xat(dx)
                remote(iq.at[k, s * X + px], ir.at[k, dy * X + dx - 1], ip_ssem.at[k], ip_rsem.at[k],
                       z * Y + s, px * 2 + c).start()

    def items_send(k, first=0):
        for j in range(first, Y):
            item_send(k, j)

    def item_total(k):
        wait_bytes(ir.at[k], ip_rsem.at[k])
        total = iq[k, y * X + x]
        for slot in range(G // 2 - 1):
            total = total + ir[k, slot]
        return total

    def gather_plane(pan, ssem, rsem):
        for slot, dx, py, px in plane():
            remote(pan.at[c, spot], pan.at[c, spot], ssem, rsem.at[dx], z * Y + py, px * 2 + c).start()

    def forward_plane(pan, rsem, fssem, frsem):
        for dx in (0, 1, 3, 2):
            rows = pl.ds(xat(-dx) * Y, Y)
            wait_bytes(pan.at[c, pl.ds(0, Y if dx else Y - 1)], rsem.at[dx])
            remote(pan.at[c, rows], pan.at[c, rows], fssem, frsem.at[dx], col, partner).start()

    def wait_plane(pan, frsem):
        for dx in (0, 1, 3, 2):
            wait_bytes(pan.at[other, pl.ds(xat(-dx) * Y, Y)], frsem.at[dx])

    def user_total(k, hooks):
        def emit(way, step, h, first=False):
            rows = pl.ds(h * H, H)
            j = piece_of[4 - step] if way == 0 or step == 0 else piece_of[step - 4]
            value = up[j, h * H:(h + 1) * H]
            if not first:
                value = value + got(way, step - 1, h)
            us[k, way, step, h * H:(h + 1) * H] = value
            remote(us.at[k, way, step, rows], ur.at[k, way, step, rows], us_ssem.at[k], us_rsem.at[way, step, h],
                   right if way == 0 else left, row).start()

        def got(way, step, h):
            wait_bytes(ur.at[k, way, step, pl.ds(h * H, H)], us_rsem.at[way, step, h])
            return ur[k, way, step, h * H:(h + 1) * H]

        def hook(*at):
            if at in hooks:
                hooks[at]()

        user_piece(k, 0)
        for h in range(NH // 2):
            emit(0, 0, early[0][h], True)
            emit(1, 0, early[1][h], True)
        if k == 0:
            hook('piece', 0)
            for step in range(1, 4):
                for way in range(2):
                    user_piece(k, 2 * step - 1 + way)
                    for h in early[way] + late[way]:
                        emit(way, step, h, step == 1 and h in late[way])
                hook('piece', step)
            user_piece(k, 7)
            hook('own')
        else:
            for way in range(2):
                user_piece(k, 1 + way)
                for h in late[way]:
                    emit(way, 1, h, True)
            for step in range(1, 4):
                hook('before', step)
                if step < 3:
                    user_piece(k, 2 * step + 1)
                    user_piece(k, 2 * step + 2)
                else:
                    user_piece(k, 7)
                def run(groups):
                    for ways in groups:
                        for h in range(NH // 2):
                            for way in ways:
                                emit(way, step, early[way][h])
                        for h in range(NH // 2):
                            for way in ways:
                                if step < 3:
                                    emit(way, step + 1, late[way][h])

                ring_order(step - 1, run)
                hook('after', step)
        parts = []
        for h in range(NH):
            parts.append(up[7, h * H:(h + 1) * H] + got(0, 3, h) + got(1, 3, h))
        new_user = jnp.concatenate(parts, axis=0).astype(BF16)
        usum[...] += new_user.astype(F32)
        return new_user

    def items_next(k):
        new_item = item_total(k).astype(BF16)
        isum[...] += new_item.astype(F32)
        ei_pan[k + 1, c, spot] = new_item
        gather_plane(ei_pan.at[k + 1], ei_ssem.at[k + 1], ei_rsem.at[k + 1])

    def items_forward(k):
        forward_plane(ei_pan.at[k], ei_rsem.at[k], fw_ssem.at[k], fw_rsem.at[k])

    def items_wait(k):
        wait_plane(ei_pan.at[k], fw_rsem.at[k])

    hop0(1)
    items_wait(0)
    new_user = user_total(0, {('piece', 0): lambda: hop0(2), ('piece', 1): last0, ('own',): lambda: item_parts(0)})
    begin1, hop1, last1 = gather_user(1)
    begin1(new_user)
    items_send(0, 1)
    hop1(0)
    item_pair(0)
    hop1(1)
    item_pair(1)
    items_next(0)
    hop1(2)
    item_pair(2)
    last1()
    item_pair(3)
    items_forward(1)
    items_send(1)
    items_wait(1)
    new_user = user_total(1, {('after', 2): lambda: items_next(1)})
    begin2, hop2, last2 = gather_user(2)
    begin2(new_user)
    items_forward(2)
    items_wait(2)

    user_total(2, {('after', 1): lambda: hop2(0), ('after', 2): lambda: hop2(1)})
    final_user = (usum[...] / (LAYERS + 1)).astype(BF16)
    fu_v[...] = final_user
    outs = [pltpu.make_async_copy(fu_v, fu_out, out_sem.at[0])]
    outs[0].start()

    qs[...] = jnp.dot(hot[...], final_user, preferred_element_type=F32).astype(BF16).reshape(2, G // 2, QB, E)
    to_partner = remote(qs.at[other], qp, q_ssem.at[0], q_rsem.at[0], col, partner)
    to_partner.start()
    hop2(2)
    to_partner.wait_recv()
    qt[...] = (qs[c].astype(F32) + qp[...].astype(F32)).astype(BF16)
    for slot, dx, py, px in plane():
        remote(qt.at[px * Y + py], qr.at[slot], q_ssem.at[1], q_rsem.at[1], z * Y + py, px * 2 + c).start()
    last2()
    item_parts(2)
    items_send(2, 1)
    wait_bytes(qr, q_rsem.at[1])
    total = qt[spot].astype(F32)
    for slot in range(G // 2 - 1):
        total = total + qr[slot].astype(F32)
    qzs[...] = total.astype(BF16)
    for d in (4, 3, 5, 2, 6, 1, 7):
        remote(qzs, qz.at[d - 1], q_ssem.at[2], q_rsem.at[2], zat(d) * Y + y, row).start()
    wait_bytes(qz, q_rsem.at[2])
    for d in range(Z - 1):
        total = total + qz[d].astype(F32)
    qall[c, spot] = total.astype(BF16)
    gather_plane(qall, q_ssem.at[3], qg_rsem)
    new_item = item_total(2).astype(BF16)
    fi_v[...] = ((isum[...] + new_item.astype(F32)) / (LAYERS + 1)).astype(BF16)
    outs.append(pltpu.make_async_copy(fi_v, fi_out, out_sem.at[1]))
    outs[1].start()
    forward_plane(qall, qg_rsem, q_ssem.at[4], qf_rsem)
    outs.append(pltpu.make_async_copy(qall.at[c], q_out.at[c], out_sem.at[2]))
    outs[2].start()
    wait_plane(qall, qf_rsem)
    outs.append(pltpu.make_async_copy(qall.at[other], q_out.at[other], out_sem.at[3]))
    outs[3].start()

    wait_bytes(rs_y, rs_ssem.at[0])
    wait_bytes(rs_z.at[pl.ds(0, Z - 1)], rs_ssem.at[1])
    wait_bytes(cs_row.at[pl.ds(0, R - 1)], cs_ssem.at[0])
    wait_bytes(cs_y.at[pl.ds(0, Y - 1)], cs_ssem.at[1])
    wait_bytes(msend.at[pl.ds(0, Y - 1)], mask_ssem)
    for k in range(LAYERS):
        wait_bytes(ei_pan.at[k, 0, pl.ds(0, G // 2 - 1)], ei_ssem.at[k])
        wait_bytes(ei_pan.at[k, 0], fw_ssem.at[k])
        wait_bytes(pr.at[k], pr_ssem.at[k])
        wait_bytes(ir.at[k], ip_ssem.at[k])
        wait_bytes(up.at[pl.ds(0, 7)], us_ssem.at[k])
        wait_bytes(eu_pan.at[k, pl.ds(0, 7)], ag_ssem.at[k])
    to_partner.wait_send()
    wait_bytes(qr, q_ssem.at[1])
    wait_bytes(qz, q_ssem.at[2])
    wait_bytes(qr, q_ssem.at[3])
    wait_bytes(qt, q_ssem.at[4])
    for out in outs:
        out.wait()


def finish(user_ref, item_ref, picked_ref, fu_ref, fi_ref, sc_ref):
    fu_ref[...] = user_ref[...]
    fi_ref[...] = item_ref[...]
    sc_ref[...] = lax.dot_general(item_ref[...], picked_ref[...], CONTRACT_LANES, preferred_element_type=F32)


def propagate(mask, user, item, queries):
    dma = pltpu.SemaphoreType.DMA
    vmem, free = pl.BlockSpec(memory_space=pltpu.VMEM), pl.BlockSpec(memory_space=pl.ANY)
    L, N = LAYERS, G // 2
    final_user, final_item, picked = pl.pallas_call(
        kernel,
        out_shape=(jax.ShapeDtypeStruct((UB, E), BF16), jax.ShapeDtypeStruct((IB, E), BF16),
                   jax.ShapeDtypeStruct((2, N, QB, E), BF16)),
        in_specs=[pl.BlockSpec(memory_space=pltpu.HBM)] * 4,
        out_specs=(free, free, free),
        scratch_shapes=[
            pltpu.VMEM((Z, Y * UB, E), jnp.int32),
            pltpu.VMEM((UB, E), BF16),
            pltpu.VMEM((IB, E), BF16),
            pltpu.VMEM((1, NQ), jnp.int32),
            pltpu.VMEM((Y, Z, UB, E), BF16),
            pltpu.VMEM((Z, Y - 1, UB, E), BF16),
            pltpu.VMEM((Y, Z, UB, E), BF16),
            pltpu.VMEM((Y, E, Z * UB), BF16),
            pltpu.VMEM((Y, Z, UB), F32),
            pltpu.VMEM((Y - 1, Z, UB), F32),
            pltpu.VMEM((Z, Z, UB), F32),
            pltpu.VMEM((1, E), F32),
            pltpu.VMEM((R, 1, E), F32),
            pltpu.VMEM((Y, 1, E), F32),
            pltpu.VMEM((Z, UB), F32),
            pltpu.VMEM((Y, 1, E), F32),
            pltpu.VMEM((L, Z, UB, E), BF16),
            pltpu.VMEM((L, 2, N, IB, E), BF16),
            pltpu.VMEM((Z, UB, E), F32),
            pltpu.VMEM((Y, E, E), F32),
            pltpu.VMEM((L, 2, 4, UB, E), F32),
            pltpu.VMEM((L, 2, 4, UB, E), F32),
            pltpu.VMEM((L, 2, N, IB, E), F32),
            pltpu.VMEM((L, Y, X, IB, E), F32),
            pltpu.VMEM((L, N, IB, E), F32),
            pltpu.VMEM((L, N - 1, IB, E), F32),
            pltpu.VMEM((NQ, UB), BF16),
            pltpu.VMEM((2, N, QB, E), BF16),
            pltpu.VMEM((N, QB, E), BF16),
            pltpu.VMEM((N, QB, E), BF16),
            pltpu.VMEM((N - 1, QB, E), BF16),
            pltpu.VMEM((Z - 1, QB, E), BF16),
            pltpu.VMEM((QB, E), BF16),
            pltpu.VMEM((2, N, QB, E), BF16),
            pltpu.VMEM((UB, E), BF16),
            pltpu.VMEM((IB, E), BF16),
            pltpu.VMEM((UB, E), F32),
            pltpu.VMEM((IB, E), F32),
            dma((Z + 3,)), dma, dma((Z,)),
            dma((2,)), dma, dma,
            dma((2,)), dma((2,)),
            dma((L,)), dma((L, X)), dma((L,)), dma((L, X)),
            dma((L,)), dma((2, 4, NH)),
            dma((L,)), dma((L, Y)), dma((L,)), dma((L,)),
            dma((L,)), dma((2, 4, NH)),
            dma((5,)), dma((3,)), dma((X,)), dma((X,)),
            dma((4,)),
        ],
        compiler_params=pltpu.CompilerParams(collective_id=0, has_side_effects=True, vmem_limit_bytes=50 * 2**20),
    )(*(pltpu.with_memory_space_constraint(a, pltpu.HBM) for a in (mask, user, item, queries.reshape(1, NQ))))
    final_user, final_item, scores = pl.pallas_call(
        finish,
        out_shape=(jax.ShapeDtypeStruct((UB, E), BF16), jax.ShapeDtypeStruct((IB, E), BF16),
                   jax.ShapeDtypeStruct((IB, NQ), F32)),
        in_specs=[vmem, vmem, vmem],
        out_specs=(vmem, vmem, vmem),
        compiler_params=pltpu.CompilerParams(vmem_limit_bytes=8 * 2**20),
    )(final_user, final_item, picked.reshape(NQ, E))
    return final_user, final_item, scores.T


def solution(mesh):
    return jax.shard_map(propagate, mesh=mesh,
                         in_specs=(P('row', 'col'), P(('row', 'col'), None), P(('col', 'row'), None), P()),
                         out_specs=(P(('row', 'col'), None), P(('col', 'row'), None), P(None, ('col', 'row'))),
                         check_vma=False)
```

```python
import jax
import jax.numpy as jnp
from jax import lax
from jax.experimental import pallas as pl
from jax.experimental.pallas import tpu as pltpu
from jax.sharding import PartitionSpec as P

LAYERS = 3
Z, Y, X = 8, 4, 4
R = 2 * X
G = Y * R
UB, IB = 128, 32
E = 256
NQ = 1024
QB = NQ // G
NH = 4
H = UB // NH
F32, BF16 = jnp.float32, jnp.bfloat16
MESH = pl.DeviceIdType.MESH
CONTRACT_ROWS = (((0,), (0,)), ((), ()))
CONTRACT_LANES = (((1,), (1,)), ((), ()))


def remote(src, dst, send_sem, recv_sem, col, row):
    return pltpu.make_async_remote_copy(src_ref=src, dst_ref=dst, send_sem=send_sem, recv_sem=recv_sem,
                                        device_id=(col, row), device_id_type=MESH)


def wait_bytes(ref, sem):
    pltpu.make_async_copy(ref, ref, sem).wait()


def kernel(mask_ref, user_hbm, item_hbm, query_hbm, fu_out, fi_out, q_out,
           mask_v, user_ref, item_ref, query_ref, msend, mrecv, adj, adjt, rs_send, rs_y, rs_z, cs_send, cs_row, cs_y, invu, invi,
           eu_pan, ei_pan, up, macc, us, ur, ip, pr, iq, ir, hot, qs, qp, qt, qr, qz, qzs, qall, fu_v, fi_v, usum, isum,
           load_sem, mask_ssem, mask_rsem, rs_ssem, rs_rsem, rz_rsem, cs_ssem, cs_rsem, ei_ssem, ei_rsem, fw_ssem, fw_rsem, us_ssem, us_rsem,
           pr_ssem, pr_rsem, ip_ssem, ip_rsem, ag_ssem, ag_rsem, q_ssem, q_rsem, qg_rsem, qf_rsem, out_sem):
    col = lax.axis_index('col')
    row = lax.axis_index('row')
    z, y = lax.div(col, Y), lax.rem(col, Y)
    x, c = lax.div(row, 2), lax.rem(row, 2)
    other = 1 - c
    partner = x * 2 + other
    spot = x * Y + y

    def zat(d):
        return lax.rem(z + (d % Z), Z)

    def yat(d):
        return lax.rem(y + (d % Y), Y)

    def xat(d):
        return lax.rem(x + (d % X), X)

    def plane():
        for dx in (2, 1, 3, 0):
            for dy in (2, 1, 3, 0):
                if dy or dx:
                    yield dx * Y + dy - 1, dx, yat(dy), xat(dx)

    order = [4, 3, -3, 2, -2, 1, -1, 0]
    piece_of = {d: j for j, d in enumerate(order)}
    place = lax.rem(z, Z // 2)

    def ring_order(step, run):
        if step == 0:
            pl.when(place == 0)(lambda: run(((1,), (0,))))
            pl.when(place == Z // 2 - 1)(lambda: run(((0,), (1,))))
            pl.when((place > 0) & (place < Z // 2 - 1))(lambda: run(((0, 1),)))
        else:
            pl.when(place < Z // 4)(lambda: run(((1,), (0,))))
            pl.when(place >= Z // 4)(lambda: run(((0,), (1,))))

    early = (list(range(NH // 2)), list(range(NH // 2, NH)))
    late = (early[1], early[0])
    right, left = zat(1) * Y + y, zat(-1) * Y + y

    loads = []
    for j, d in enumerate(order):
        zc = zat(d)
        load = pltpu.make_async_copy(mask_ref.at[pl.ds(zc * (Y * UB), Y * UB)], mask_v.at[j], load_sem.at[j])
        load.start()
        loads.append(load)

    small = []
    for i, (src, dst) in enumerate(((user_hbm, user_ref), (item_hbm, item_ref), (query_hbm, query_ref))):
        small.append(pltpu.make_async_copy(src, dst, load_sem.at[Z + i]))
        small[i].start()

    barrier = pltpu.get_barrier_semaphore()
    for d in range(1, R):
        pl.semaphore_signal(barrier, inc=1, device_id=(col, lax.rem(row + d, R)), device_id_type=MESH)
    for d in range(1, Y):
        pl.semaphore_signal(barrier, inc=1, device_id=(z * Y + yat(d), row), device_id_type=MESH)
    for d in range(1, Z):
        pl.semaphore_signal(barrier, inc=1, device_id=(zat(d) * Y + y, row), device_id_type=MESH)

    ones_w = jnp.ones((8, E), BF16)
    colsum = jnp.zeros((8, E), F32)

    def send_mask(j):
        for d in range(1, Y):
            py = yat(d)
            remote(msend.at[py, j], mrecv.at[j, d - 1], mask_ssem, mask_rsem.at[j], z * Y + py, row).start()

    for j, d in enumerate(order):
        zc = zat(d)
        loads[j].wait()
        for p in range(Y):
            wide = mask_v[j, p * UB:(p + 1) * UB, :].astype(F32)
            block = wide.astype(BF16)
            msend[p, j] = block
            sums = lax.dot_general(ones_w, block, CONTRACT_LANES, preferred_element_type=F32)
            rs_send[p, pl.ds(zc, 1), :] = sums[0:1]
            colsum = colsum + jnp.sum(wide.reshape(UB // 8, 8, E), axis=0)
    cs_send[...] = jnp.sum(colsum, axis=0, keepdims=True)
    cs_row[row] = cs_send[...]
    for load in small:
        load.wait()
    ei_pan[0, c, spot] = item_ref[...]

    def gather_user(k):
        def send(way, step, h):
            src = eu_pan.at[k, zat(-step if way == 0 else step), pl.ds(h * H, H)]
            remote(src, src, ag_ssem.at[k], ag_rsem.at[way, step, h], right if way == 0 else left, row).start()

        def got(way, step, h):
            dst = eu_pan.at[k, zat(-step - 1 if way == 0 else step + 1), pl.ds(h * H, H)]
            wait_bytes(dst, ag_rsem.at[way, step, h])

        def begin(new_user):
            eu_pan[k, z] = new_user
            for h in range(NH):
                for way in range(2):
                    send(way, 0, (early[way] + late[way])[h])

        def hop(step):
            def run(groups):
                for ways in groups:
                    for h in range(NH):
                        for way in ways:
                            hh = (early[way] + late[way])[h]
                            got(way, step, hh)
                            if step < 2 or h < NH // 2:
                                send(way, step + 1, hh)

            ring_order(step, run)

        def last():
            for h in range(NH // 2):
                for way in range(2):
                    got(way, 3, early[way][h])

        return begin, hop, last

    pl.semaphore_wait(barrier, R - 1 + Y - 1 + Z - 1)
    for d in range(1, Y):
        remote(rs_send.at[yat(d)], rs_y.at[d - 1], rs_ssem.at[0], rs_rsem, z * Y + yat(d), row).start()
    for d in range(1, R):
        remote(cs_send, cs_row.at[row], cs_ssem.at[0], cs_rsem.at[0], col, lax.rem(row + d, R)).start()
    for d in range(1, Y):
        remote(item_ref, ei_pan.at[0, c, spot], ei_ssem.at[0], ei_rsem.at[0, 0], z * Y + yat(d), row).start()
    send_mask(0)
    begin0, hop0, last0 = gather_user(0)
    begin0(user_ref[...])
    send_mask(1)

    usum[...] = user_ref[...].astype(F32)
    isum[...] = item_ref[...].astype(F32)
    wait_bytes(rs_y, rs_rsem)
    rs_z[z] = rs_send[y] + rs_y[0] + rs_y[1] + rs_y[2]
    for d in (4, 3, 5, 2, 6, 1, 7):
        remote(rs_z.at[z], rs_z.at[z], rs_ssem.at[1], rz_rsem, zat(d) * Y + y, row).start()

    wait_bytes(ei_pan.at[0, c, pl.ds(0, Y - 1)], ei_rsem.at[0, 0])
    own = ei_pan.at[0, c, pl.ds(x * Y, Y)]
    for d in range(1, X):
        remote(own, own, ei_ssem.at[0], ei_rsem.at[0, d], col, xat(d) * 2 + c).start()
    remote(own, own, fw_ssem.at[0], fw_rsem.at[0, 0], col, partner).start()

    wait_bytes(cs_row.at[pl.ds(0, R - 1)], cs_rsem.at[0])
    deg = cs_row[0]
    for r in range(1, R):
        deg = deg + cs_row[r]
    cs_y[y] = deg
    for d in range(1, Y):
        remote(cs_y.at[y], cs_y.at[y], cs_ssem.at[1], cs_rsem.at[1], z * Y + yat(d), row).start()
    for j in range(2, Z):
        send_mask(j)

    base = (row * (Z * Y) + col) * UB
    ids = lax.broadcasted_iota(jnp.int32, (UB, NQ), 0) + base
    hot[...] = jnp.where(ids == query_ref[...], 1.0, 0.0).T.astype(BF16)

    hop0(0)
    for d in (1, 3, 2):
        rows = pl.ds(xat(-d) * Y, Y)
        wait_bytes(ei_pan.at[0, c, rows], ei_rsem.at[0, d])
        remote(ei_pan.at[0, c, rows], ei_pan.at[0, c, rows], fw_ssem.at[0], fw_rsem.at[0, d], col, partner).start()
    wait_bytes(cs_y.at[pl.ds(0, Y - 1)], cs_rsem.at[1])
    for s in range(Y):
        invi[s] = lax.rsqrt(jnp.maximum(cs_y[s], 1.0))
    wait_bytes(rs_z.at[pl.ds(0, Z - 1)], rz_rsem)
    deg = rs_z[0]
    for d in range(1, Z):
        deg = deg + rs_z[d]
    invu[...] = lax.rsqrt(jnp.maximum(deg, 1.0))

    def make_adj(j, zc):
        wait_bytes(mrecv.at[j], mask_rsem.at[j])
        iu = jnp.broadcast_to(invu[pl.ds(zc, 1), :], (UB, UB)).T
        iu = jnp.concatenate([iu, iu], axis=1)
        for d in range(Y):
            s = yat(-d)
            m = (msend[y, j] if d == 0 else mrecv[j, d - 1]).astype(F32)
            a = (iu * m) * invi[s]
            adj[s, zc] = a.astype(BF16)
            adjt[s, :, pl.ds(pl.multiple_of(zc * UB, UB), UB)] = a.T.astype(BF16)

    def user_piece(k, j):
        zc = zat(order[j])
        if k == 0:
            make_adj(j, zc)
        acc = None
        for s in range(Y):
            panel = jnp.concatenate([ei_pan[k, cc, xx * Y + s] for xx in range(X) for cc in range(2)], axis=0)
            t = jnp.dot(adj[s, zc], panel, preferred_element_type=F32)
            acc = t if acc is None else acc + t
        up[j] = acc

    def item_share(k, product, lag=Y):
        for j, dy in enumerate((2, 1, 3, 0)):
            s = yat(dy)
            part = product(s).reshape(X, 2, IB, E)
            for xx in range(X):
                for cc in range(2):
                    ip[k, cc, s * X + xx] = part[xx, cc]
            remote(ip.at[k, other, pl.ds(s * X, X)], pr.at[k, j], pr_ssem.at[k], pr_rsem.at[k, j], col, partner).start()
            if j >= lag:
                item_send(k, j - lag)

    def item_parts(k):
        eu = eu_pan[k].reshape(Z * UB, E)
        item_share(k, lambda s: jnp.dot(adjt[s], eu, preferred_element_type=F32), lag=3)

    def item_pair(n):
        near = [zat(d) for d in ((0, 1), (-1, 2), (-2, 3), (-3, 4))[n]]
        eu = jnp.concatenate([eu_pan[1, zc] for zc in near], axis=0)

        def add(s):
            lhs = jnp.concatenate([adjt[s, :, pl.ds(pl.multiple_of(zc * UB, UB), UB)] for zc in near], axis=1)
            part = jnp.dot(lhs, eu, preferred_element_type=F32)
            return part + macc[s] if n else part

        if n < 3:
            for s in range(Y):
                macc[s] = add(s)
        else:
            item_share(1, add)

    def item_send(k, j):
        dy = (2, 1, 3, 0)[j]
        s = yat(dy)
        wait_bytes(pr.at[k, j], pr_rsem.at[k, j])
        iq[k, pl.ds(s * X, X)] = ip[k, c, pl.ds(s * X, X)] + pr[k, j]
        for dx in (2, 1, 3, 0):
            if dy or dx:
                px = xat(dx)
                remote(iq.at[k, s * X + px], ir.at[k, dy * X + dx - 1], ip_ssem.at[k], ip_rsem.at[k],
                       z * Y + s, px * 2 + c).start()

    def items_send(k, first=0):
        for j in range(first, Y):
            item_send(k, j)

    def item_total(k):
        wait_bytes(ir.at[k], ip_rsem.at[k])
        total = iq[k, y * X + x]
        for slot in range(G // 2 - 1):
            total = total + ir[k, slot]
        return total

    def gather_plane(pan, ssem, rsem):
        for slot, dx, py, px in plane():
            remote(pan.at[c, spot], pan.at[c, spot], ssem, rsem.at[dx], z * Y + py, px * 2 + c).start()

    def forward_plane(pan, rsem, fssem, frsem):
        for dx in (0, 1, 3, 2):
            rows = pl.ds(xat(-dx) * Y, Y)
            wait_bytes(pan.at[c, pl.ds(0, Y if dx else Y - 1)], rsem.at[dx])
            remote(pan.at[c, rows], pan.at[c, rows], fssem, frsem.at[dx], col, partner).start()

    def wait_plane(pan, frsem):
        for dx in (0, 1, 3, 2):
            wait_bytes(pan.at[other, pl.ds(xat(-dx) * Y, Y)], frsem.at[dx])

    def user_total(k, hooks):
        def emit(way, step, h, first=False):
            rows = pl.ds(h * H, H)
            j = piece_of[4 - step] if way == 0 or step == 0 else piece_of[step - 4]
            value = up[j, h * H:(h + 1) * H]
            if not first:
                value = value + got(way, step - 1, h)
            us[k, way, step, h * H:(h + 1) * H] = value
            remote(us.at[k, way, step, rows], ur.at[k, way, step, rows], us_ssem.at[k], us_rsem.at[way, step, h],
                   right if way == 0 else left, row).start()

        def got(way, step, h):
            wait_bytes(ur.at[k, way, step, pl.ds(h * H, H)], us_rsem.at[way, step, h])
            return ur[k, way, step, h * H:(h + 1) * H]

        def hook(*at):
            if at in hooks:
                hooks[at]()

        user_piece(k, 0)
        for h in range(NH // 2):
            emit(0, 0, early[0][h], True)
            emit(1, 0, early[1][h], True)
        if k == 0:
            hook('piece', 0)
            for step in range(1, 4):
                for way in range(2):
                    user_piece(k, 2 * step - 1 + way)
                    for h in early[way] + late[way]:
                        emit(way, step, h, step == 1 and h in late[way])
                hook('piece', step)
            user_piece(k, 7)
            hook('own')
        else:
            for way in range(2):
                user_piece(k, 1 + way)
                for h in late[way]:
                    emit(way, 1, h, True)
            for step in range(1, 4):
                hook('before', step)
                if step < 3:
                    user_piece(k, 2 * step + 1)
                    user_piece(k, 2 * step + 2)
                else:
                    user_piece(k, 7)
                def run(groups):
                    for ways in groups:
                        for h in range(NH // 2):
                            for way in ways:
                                emit(way, step, early[way][h])
                        for h in range(NH // 2):
                            for way in ways:
                                if step < 3:
                                    emit(way, step + 1, late[way][h])

                ring_order(step - 1, run)
                hook('after', step)
        parts = []
        for h in range(NH):
            parts.append(up[7, h * H:(h + 1) * H] + got(0, 3, h) + got(1, 3, h))
        new_user = jnp.concatenate(parts, axis=0).astype(BF16)
        usum[...] += new_user.astype(F32)
        return new_user

    def items_next(k):
        new_item = item_total(k).astype(BF16)
        isum[...] += new_item.astype(F32)
        ei_pan[k + 1, c, spot] = new_item
        gather_plane(ei_pan.at[k + 1], ei_ssem.at[k + 1], ei_rsem.at[k + 1])

    def items_forward(k):
        forward_plane(ei_pan.at[k], ei_rsem.at[k], fw_ssem.at[k], fw_rsem.at[k])

    def items_wait(k):
        wait_plane(ei_pan.at[k], fw_rsem.at[k])

    hop0(1)
    items_wait(0)
    new_user = user_total(0, {('piece', 0): lambda: hop0(2), ('piece', 1): last0, ('own',): lambda: item_parts(0)})
    begin1, hop1, last1 = gather_user(1)
    begin1(new_user)
    items_send(0, 1)
    hop1(0)
    item_pair(0)
    hop1(1)
    item_pair(1)
    items_next(0)
    hop1(2)
    item_pair(2)
    last1()
    item_pair(3)
    items_forward(1)
    items_send(1)
    items_wait(1)
    new_user = user_total(1, {('after', 2): lambda: items_next(1)})
    begin2, hop2, last2 = gather_user(2)
    begin2(new_user)
    items_forward(2)
    items_wait(2)

    user_total(2, {('after', 1): lambda: hop2(0), ('after', 2): lambda: hop2(1)})
    final_user = (usum[...] / (LAYERS + 1)).astype(BF16)
    fu_v[...] = final_user
    outs = [pltpu.make_async_copy(fu_v, fu_out, out_sem.at[0])]
    outs[0].start()

    qs[...] = jnp.dot(hot[...], final_user, preferred_element_type=F32).astype(BF16).reshape(2, G // 2, QB, E)
    to_partner = remote(qs.at[other], qp, q_ssem.at[0], q_rsem.at[0], col, partner)
    to_partner.start()
    hop2(2)
    to_partner.wait_recv()
    qt[...] = (qs[c].astype(F32) + qp[...].astype(F32)).astype(BF16)
    for slot, dx, py, px in plane():
        remote(qt.at[px * Y + py], qr.at[slot], q_ssem.at[1], q_rsem.at[1], z * Y + py, px * 2 + c).start()
    last2()
    item_parts(2)
    items_send(2, 1)
    wait_bytes(qr, q_rsem.at[1])
    total = qt[spot].astype(F32)
    for slot in range(G // 2 - 1):
        total = total + qr[slot].astype(F32)
    qzs[...] = total.astype(BF16)
    for d in (4, 3, 5, 2, 6, 1, 7):
        remote(qzs, qz.at[d - 1], q_ssem.at[2], q_rsem.at[2], zat(d) * Y + y, row).start()
    wait_bytes(qz, q_rsem.at[2])
    for d in range(Z - 1):
        total = total + qz[d].astype(F32)
    qall[c, spot] = total.astype(BF16)
    gather_plane(qall, q_ssem.at[3], qg_rsem)
    new_item = item_total(2).astype(BF16)
    fi_v[...] = ((isum[...] + new_item.astype(F32)) / (LAYERS + 1)).astype(BF16)
    outs.append(pltpu.make_async_copy(fi_v, fi_out, out_sem.at[1]))
    outs[1].start()
    forward_plane(qall, qg_rsem, q_ssem.at[4], qf_rsem)
    outs.append(pltpu.make_async_copy(qall.at[c], q_out.at[c], out_sem.at[2]))
    outs[2].start()
    wait_plane(qall, qf_rsem)
    outs.append(pltpu.make_async_copy(qall.at[other], q_out.at[other], out_sem.at[3]))
    outs[3].start()

    wait_bytes(rs_y, rs_ssem.at[0])
    wait_bytes(rs_z.at[pl.ds(0, Z - 1)], rs_ssem.at[1])
    wait_bytes(cs_row.at[pl.ds(0, R - 1)], cs_ssem.at[0])
    wait_bytes(cs_y.at[pl.ds(0, Y - 1)], cs_ssem.at[1])
    wait_bytes(msend.at[pl.ds(0, Y - 1)], mask_ssem)
    for k in range(LAYERS):
        wait_bytes(ei_pan.at[k, 0, pl.ds(0, G // 2 - 1)], ei_ssem.at[k])
        wait_bytes(ei_pan.at[k, 0], fw_ssem.at[k])
        wait_bytes(pr.at[k], pr_ssem.at[k])
        wait_bytes(ir.at[k], ip_ssem.at[k])
        wait_bytes(up.at[pl.ds(0, 7)], us_ssem.at[k])
        wait_bytes(eu_pan.at[k, pl.ds(0, 7)], ag_ssem.at[k])
    to_partner.wait_send()
    wait_bytes(qr, q_ssem.at[1])
    wait_bytes(qz, q_ssem.at[2])
    wait_bytes(qr, q_ssem.at[3])
    wait_bytes(qt, q_ssem.at[4])
    for out in outs:
        out.wait()


def finish(user_ref, item_ref, picked_ref, fu_ref, fi_ref, sc_ref):
    fu_ref[...] = user_ref[...]
    fi_ref[...] = item_ref[...]
    sc_ref[...] = lax.dot_general(item_ref[...], picked_ref[...], CONTRACT_LANES, preferred_element_type=F32)


def propagate(mask, user, item, queries):
    dma = pltpu.SemaphoreType.DMA
    vmem, free = pl.BlockSpec(memory_space=pltpu.VMEM), pl.BlockSpec(memory_space=pl.ANY)
    L, N = LAYERS, G // 2
    final_user, final_item, picked = pl.pallas_call(
        kernel,
        out_shape=(jax.ShapeDtypeStruct((UB, E), BF16), jax.ShapeDtypeStruct((IB, E), BF16),
                   jax.ShapeDtypeStruct((2, N, QB, E), BF16)),
        in_specs=[pl.BlockSpec(memory_space=pltpu.HBM)] * 4,
        out_specs=(free, free, free),
        scratch_shapes=[
            pltpu.VMEM((Z, Y * UB, E), jnp.int32),
            pltpu.VMEM((UB, E), BF16),
            pltpu.VMEM((IB, E), BF16),
            pltpu.VMEM((1, NQ), jnp.int32),
            pltpu.VMEM((Y, Z, UB, E), BF16),
            pltpu.VMEM((Z, Y - 1, UB, E), BF16),
            pltpu.VMEM((Y, Z, UB, E), BF16),
            pltpu.VMEM((Y, E, Z * UB), BF16),
            pltpu.VMEM((Y, Z, UB), F32),
            pltpu.VMEM((Y - 1, Z, UB), F32),
            pltpu.VMEM((Z, Z, UB), F32),
            pltpu.VMEM((1, E), F32),
            pltpu.VMEM((R, 1, E), F32),
            pltpu.VMEM((Y, 1, E), F32),
            pltpu.VMEM((Z, UB), F32),
            pltpu.VMEM((Y, 1, E), F32),
            pltpu.VMEM((L, Z, UB, E), BF16),
            pltpu.VMEM((L, 2, N, IB, E), BF16),
            pltpu.VMEM((Z, UB, E), F32),
            pltpu.VMEM((Y, E, E), F32),
            pltpu.VMEM((L, 2, 4, UB, E), F32),
            pltpu.VMEM((L, 2, 4, UB, E), F32),
            pltpu.VMEM((L, 2, N, IB, E), F32),
            pltpu.VMEM((L, Y, X, IB, E), F32),
            pltpu.VMEM((L, N, IB, E), F32),
            pltpu.VMEM((L, N - 1, IB, E), F32),
            pltpu.VMEM((NQ, UB), BF16),
            pltpu.VMEM((2, N, QB, E), BF16),
            pltpu.VMEM((N, QB, E), BF16),
            pltpu.VMEM((N, QB, E), BF16),
            pltpu.VMEM((N - 1, QB, E), BF16),
            pltpu.VMEM((Z - 1, QB, E), BF16),
            pltpu.VMEM((QB, E), BF16),
            pltpu.VMEM((2, N, QB, E), BF16),
            pltpu.VMEM((UB, E), BF16),
            pltpu.VMEM((IB, E), BF16),
            pltpu.VMEM((UB, E), F32),
            pltpu.VMEM((IB, E), F32),
            dma((Z + 3,)), dma, dma((Z,)),
            dma((2,)), dma, dma,
            dma((2,)), dma((2,)),
            dma((L,)), dma((L, X)), dma((L,)), dma((L, X)),
            dma((L,)), dma((2, 4, NH)),
            dma((L,)), dma((L, Y)), dma((L,)), dma((L,)),
            dma((L,)), dma((2, 4, NH)),
            dma((5,)), dma((3,)), dma((X,)), dma((X,)),
            dma((4,)),
        ],
        compiler_params=pltpu.CompilerParams(collective_id=0, has_side_effects=True, vmem_limit_bytes=50 * 2**20),
    )(*(pltpu.with_memory_space_constraint(a, pltpu.HBM) for a in (mask, user, item, queries.reshape(1, NQ))))
    final_user, final_item, scores = pl.pallas_call(
        finish,
        out_shape=(jax.ShapeDtypeStruct((UB, E), BF16), jax.ShapeDtypeStruct((IB, E), BF16),
                   jax.ShapeDtypeStruct((IB, NQ), F32)),
        in_specs=[vmem, vmem, vmem],
        out_specs=(vmem, vmem, vmem),
        compiler_params=pltpu.CompilerParams(vmem_limit_bytes=8 * 2**20),
    )(final_user, final_item, picked.reshape(NQ, E))
    return final_user, final_item, scores.T


def solution(mesh):
    return jax.shard_map(propagate, mesh=mesh,
                         in_specs=(P('row', 'col'), P(('row', 'col'), None), P(('col', 'row'), None), P()),
                         out_specs=(P(('row', 'col'), None), P(('col', 'row'), None), P(None, ('col', 'row'))),
                         check_vma=False)
```

```python
import jax
import jax.numpy as jnp
from jax import lax
from jax.experimental import pallas as pl
from jax.experimental.pallas import tpu as pltpu
from jax.sharding import PartitionSpec as P

LAYERS = 3
Z, Y, X = 8, 4, 4
R = 2 * X
G = Y * R
UB, IB = 128, 32
E = 256
NQ = 1024
QB = NQ // G
NH = 4
H = UB // NH
F32, BF16 = jnp.float32, jnp.bfloat16
MESH = pl.DeviceIdType.MESH
CONTRACT_ROWS = (((0,), (0,)), ((), ()))
CONTRACT_LANES = (((1,), (1,)), ((), ()))


def remote(src, dst, send_sem, recv_sem, col, row):
    return pltpu.make_async_remote_copy(src_ref=src, dst_ref=dst, send_sem=send_sem, recv_sem=recv_sem,
                                        device_id=(col, row), device_id_type=MESH)


def wait_bytes(ref, sem):
    pltpu.make_async_copy(ref, ref, sem).wait()


def kernel(mask_ref, user_hbm, item_hbm, query_hbm, fu_out, fi_out, q_out,
           mask_v, user_ref, item_ref, query_ref, msend, mrecv, adj, adjt, rs_send, rs_y, rs_z, cs_send, cs_row, cs_y, invu, invi,
           eu_pan, ei_pan, up, macc, us, ur, ip, pr, iq, ir, hot, qs, qp, qt, qr, qz, qzs, qall, fu_v, fi_v, usum, isum,
           load_sem, mask_ssem, mask_rsem, rs_ssem, rs_rsem, rz_rsem, cs_ssem, cs_rsem, ei_ssem, ei_rsem, fw_ssem, fw_rsem, us_ssem, us_rsem,
           pr_ssem, pr_rsem, ip_ssem, ip_rsem, ag_ssem, ag_rsem, q_ssem, q_rsem, qg_rsem, qf_rsem, out_sem):
    col = lax.axis_index('col')
    row = lax.axis_index('row')
    z, y = lax.div(col, Y), lax.rem(col, Y)
    x, c = lax.div(row, 2), lax.rem(row, 2)
    other = 1 - c
    partner = x * 2 + other
    spot = x * Y + y

    def zat(d):
        return lax.rem(z + (d % Z), Z)

    def yat(d):
        return lax.rem(y + (d % Y), Y)

    def xat(d):
        return lax.rem(x + (d % X), X)

    def plane():
        for dx in (2, 1, 3, 0):
            for dy in (2, 1, 3, 0):
                if dy or dx:
                    yield dx * Y + dy - 1, dx, yat(dy), xat(dx)

    order = [4, 3, -3, 2, -2, 1, -1, 0]
    piece_of = {d: j for j, d in enumerate(order)}
    place = lax.rem(z, Z // 2)

    def ring_order(step, run):
        if step == 0:
            pl.when(place == 0)(lambda: run(((1,), (0,))))
            pl.when(place == Z // 2 - 1)(lambda: run(((0,), (1,))))
            pl.when((place > 0) & (place < Z // 2 - 1))(lambda: run(((0, 1),)))
        else:
            pl.when(place < Z // 4)(lambda: run(((1,), (0,))))
            pl.when(place >= Z // 4)(lambda: run(((0,), (1,))))

    early = (list(range(NH // 2)), list(range(NH // 2, NH)))
    late = (early[1], early[0])
    right, left = zat(1) * Y + y, zat(-1) * Y + y

    loads = []
    for j, d in enumerate(order):
        zc = zat(d)
        load = pltpu.make_async_copy(mask_ref.at[pl.ds(zc * (Y * UB), Y * UB)], mask_v.at[j], load_sem.at[j])
        load.start()
        loads.append(load)

    small = []
    for i, (src, dst) in enumerate(((user_hbm, user_ref), (item_hbm, item_ref), (query_hbm, query_ref))):
        small.append(pltpu.make_async_copy(src, dst, load_sem.at[Z + i]))
        small[i].start()

    barrier = pltpu.get_barrier_semaphore()
    for d in range(1, R):
        pl.semaphore_signal(barrier, inc=1, device_id=(col, lax.rem(row + d, R)), device_id_type=MESH)
    for d in range(1, Y):
        pl.semaphore_signal(barrier, inc=1, device_id=(z * Y + yat(d), row), device_id_type=MESH)
    for d in range(1, Z):
        pl.semaphore_signal(barrier, inc=1, device_id=(zat(d) * Y + y, row), device_id_type=MESH)

    ones_w = jnp.ones((8, E), BF16)
    colsum = jnp.zeros((8, E), F32)

    def send_mask(j):
        for d in range(1, Y):
            py = yat(d)
            remote(msend.at[py, j], mrecv.at[j, d - 1], mask_ssem, mask_rsem.at[j], z * Y + py, row).start()

    for j, d in enumerate(order):
        zc = zat(d)
        loads[j].wait()
        for p in range(Y):
            wide = mask_v[j, p * UB:(p + 1) * UB, :].astype(F32)
            block = wide.astype(BF16)
            msend[p, j] = block
            sums = lax.dot_general(ones_w, block, CONTRACT_LANES, preferred_element_type=F32)
            rs_send[p, pl.ds(zc, 1), :] = sums[0:1]
            colsum = colsum + jnp.sum(wide.reshape(UB // 8, 8, E), axis=0)
    cs_send[...] = jnp.sum(colsum, axis=0, keepdims=True)
    cs_row[row] = cs_send[...]
    for load in small:
        load.wait()
    ei_pan[0, c, spot] = item_ref[...]

    def gather_user(k):
        def send(way, step, h):
            src = eu_pan.at[k, zat(-step if way == 0 else step), pl.ds(h * H, H)]
            remote(src, src, ag_ssem, ag_rsem.at[way, step, h], right if way == 0 else left, row).start()

        def got(way, step, h):
            dst = eu_pan.at[k, zat(-step - 1 if way == 0 else step + 1), pl.ds(h * H, H)]
            wait_bytes(dst, ag_rsem.at[way, step, h])

        def begin(new_user):
            eu_pan[k, z] = new_user
            for h in range(NH):
                for way in range(2):
                    send(way, 0, (early[way] + late[way])[h])

        def hop(step):
            def run(groups):
                for ways in groups:
                    for h in range(NH):
                        for way in ways:
                            hh = (early[way] + late[way])[h]
                            got(way, step, hh)
                            if step < 2 or h < NH // 2:
                                send(way, step + 1, hh)

            ring_order(step, run)

        def last():
            for h in range(NH // 2):
                for way in range(2):
                    got(way, 3, early[way][h])

        return begin, hop, last

    pl.semaphore_wait(barrier, R - 1 + Y - 1 + Z - 1)
    for d in range(1, Y):
        remote(rs_send.at[yat(d)], rs_y.at[d - 1], rs_ssem.at[0], rs_rsem, z * Y + yat(d), row).start()
    for d in range(1, R):
        remote(cs_send, cs_row.at[row], cs_ssem.at[0], cs_rsem.at[0], col, lax.rem(row + d, R)).start()
    for d in range(1, Y):
        remote(item_ref, ei_pan.at[0, c, spot], ei_ssem, ei_rsem.at[0, 0], z * Y + yat(d), row).start()
    send_mask(0)
    begin0, hop0, last0 = gather_user(0)
    begin0(user_ref[...])
    send_mask(1)

    usum[...] = user_ref[...].astype(F32)
    isum[...] = item_ref[...].astype(F32)
    wait_bytes(rs_y, rs_rsem)
    rs_z[z] = rs_send[y] + rs_y[0] + rs_y[1] + rs_y[2]
    for d in (4, 3, 5, 2, 6, 1, 7):
        remote(rs_z.at[z], rs_z.at[z], rs_ssem.at[1], rz_rsem, zat(d) * Y + y, row).start()

    wait_bytes(ei_pan.at[0, c, pl.ds(0, Y - 1)], ei_rsem.at[0, 0])
    own = ei_pan.at[0, c, pl.ds(x * Y, Y)]
    for d in range(1, X):
        remote(own, own, ei_ssem, ei_rsem.at[0, d], col, xat(d) * 2 + c).start()
    remote(own, own, fw_ssem, fw_rsem.at[0, 0], col, partner).start()

    wait_bytes(cs_row.at[pl.ds(0, R - 1)], cs_rsem.at[0])
    deg = cs_row[0]
    for r in range(1, R):
        deg = deg + cs_row[r]
    cs_y[y] = deg
    for d in range(1, Y):
        remote(cs_y.at[y], cs_y.at[y], cs_ssem.at[1], cs_rsem.at[1], z * Y + yat(d), row).start()
    for j in range(2, Z):
        send_mask(j)

    base = (row * (Z * Y) + col) * UB
    ids = lax.broadcasted_iota(jnp.int32, (UB, NQ), 0) + base
    hot[...] = jnp.where(ids == query_ref[...], 1.0, 0.0).T.astype(BF16)

    hop0(0)
    for d in (1, 3, 2):
        rows = pl.ds(xat(-d) * Y, Y)
        wait_bytes(ei_pan.at[0, c, rows], ei_rsem.at[0, d])
        remote(ei_pan.at[0, c, rows], ei_pan.at[0, c, rows], fw_ssem, fw_rsem.at[0, d], col, partner).start()
    wait_bytes(cs_y.at[pl.ds(0, Y - 1)], cs_rsem.at[1])
    for s in range(Y):
        invi[s] = lax.rsqrt(jnp.maximum(cs_y[s], 1.0))
    wait_bytes(rs_z.at[pl.ds(0, Z - 1)], rz_rsem)
    deg = rs_z[0]
    for d in range(1, Z):
        deg = deg + rs_z[d]
    invu[...] = lax.rsqrt(jnp.maximum(deg, 1.0))

    def make_adj(j, zc):
        wait_bytes(mrecv.at[j], mask_rsem.at[j])
        iu = jnp.broadcast_to(invu[pl.ds(zc, 1), :], (UB, UB)).T
        iu = jnp.concatenate([iu, iu], axis=1)
        for d in range(Y):
            s = yat(-d)
            m = (msend[y, j] if d == 0 else mrecv[j, d - 1]).astype(F32)
            a = (iu * m) * invi[s]
            adj[s, zc] = a.astype(BF16)
            adjt[s, :, pl.ds(pl.multiple_of(zc * UB, UB), UB)] = a.T.astype(BF16)

    def user_piece(k, j):
        zc = zat(order[j])
        if k == 0:
            make_adj(j, zc)
        acc = None
        for s in range(Y):
            panel = jnp.concatenate([ei_pan[k, cc, xx * Y + s] for xx in range(X) for cc in range(2)], axis=0)
            t = jnp.dot(adj[s, zc], panel, preferred_element_type=F32)
            acc = t if acc is None else acc + t
        up[j] = acc

    def item_share(k, product, lag=Y):
        for j, dy in enumerate((2, 1, 3, 0)):
            s = yat(dy)
            part = product(s).reshape(X, 2, IB, E)
            for xx in range(X):
                for cc in range(2):
                    ip[k, cc, s * X + xx] = part[xx, cc]
            remote(ip.at[k, other, pl.ds(s * X, X)], pr.at[k, j], pr_ssem, pr_rsem.at[k % 2, j], col, partner).start()
            if j >= lag:
                item_send(k, j - lag)

    def item_parts(k):
        eu = eu_pan[k].reshape(Z * UB, E)
        item_share(k, lambda s: jnp.dot(adjt[s], eu, preferred_element_type=F32), lag=3)

    pairs = (((4, 3), (-3, 2), (-2, 1), (-1, 0)), ((0, 1), (-1, 2), (-2, 3), (-3, 4)))

    def item_pair(k, n):
        near = [zat(d) for d in pairs[k][n]]
        eu = jnp.concatenate([eu_pan[k, zc] for zc in near], axis=0)

        def add(s):
            lhs = jnp.concatenate([adjt[s, :, pl.ds(pl.multiple_of(zc * UB, UB), UB)] for zc in near], axis=1)
            part = jnp.dot(lhs, eu, preferred_element_type=F32)
            return part + macc[s] if n else part

        if n < 3:
            for s in range(Y):
                macc[s] = add(s)
        else:
            item_share(k, add)

    def item_send(k, j):
        dy = (2, 1, 3, 0)[j]
        s = yat(dy)
        wait_bytes(pr.at[k, j], pr_rsem.at[k % 2, j])
        iq[k, pl.ds(s * X, X)] = ip[k, c, pl.ds(s * X, X)] + pr[k, j]
        for dx in (2, 1, 3, 0):
            if dy or dx:
                px = xat(dx)
                remote(iq.at[k, s * X + px], ir.at[k, dy * X + dx - 1], ip_ssem, ip_rsem.at[k],
                       z * Y + s, px * 2 + c).start()

    def items_send(k, first=0):
        for j in range(first, Y):
            item_send(k, j)

    def item_total(k):
        wait_bytes(ir.at[k], ip_rsem.at[k])
        total = iq[k, y * X + x]
        for slot in range(G // 2 - 1):
            total = total + ir[k, slot]
        return total

    def gather_plane(pan, ssem, rsem):
        for slot, dx, py, px in plane():
            remote(pan.at[c, spot], pan.at[c, spot], ssem, rsem.at[dx], z * Y + py, px * 2 + c).start()

    def forward_plane(pan, rsem, fssem, frsem, dst):
        for dx in (0, 1, 3, 2):
            rows = pl.ds(xat(-dx) * Y, Y)
            wait_bytes(pan.at[c, pl.ds(0, Y if dx else Y - 1)], rsem.at[dx])
            remote(pan.at[c, rows], dst.at[c, rows], fssem, frsem.at[dx], col, partner).start()

    def wait_plane(pan, frsem):
        for dx in (0, 1, 3, 2):
            wait_bytes(pan.at[other, pl.ds(xat(-dx) * Y, Y)], frsem.at[dx])

    def user_total(k, hooks):
        def emit(way, step, h, first=False):
            rows = pl.ds(h * H, H)
            j = piece_of[4 - step] if way == 0 or step == 0 else piece_of[step - 4]
            value = up[j, h * H:(h + 1) * H]
            if not first:
                value = value + got(way, step - 1, h)
            us[k, way, step, h * H:(h + 1) * H] = value
            remote(us.at[k, way, step, rows], ur.at[k, way, step, rows], us_ssem.at[k], us_rsem.at[way, step, h],
                   right if way == 0 else left, row).start()

        def got(way, step, h):
            wait_bytes(ur.at[k, way, step, pl.ds(h * H, H)], us_rsem.at[way, step, h])
            return ur[k, way, step, h * H:(h + 1) * H]

        def hook(*at):
            if at in hooks:
                hooks[at]()

        user_piece(k, 0)
        for h in range(NH // 2):
            emit(0, 0, early[0][h], True)
            emit(1, 0, early[1][h], True)
        if k == 0:
            hook('piece', 0)
            for step in range(1, 4):
                for way in range(2):
                    user_piece(k, 2 * step - 1 + way)
                    for h in early[way] + late[way]:
                        emit(way, step, h, step == 1 and h in late[way])
                hook('piece', step)
            user_piece(k, 7)
            hook('own')
        else:
            for way in range(2):
                user_piece(k, 1 + way)
                for h in late[way]:
                    emit(way, 1, h, True)
            for step in range(1, 4):
                hook('before', step)
                if step < 3:
                    user_piece(k, 2 * step + 1)
                    user_piece(k, 2 * step + 2)
                else:
                    user_piece(k, 7)
                def run(groups):
                    for ways in groups:
                        for h in range(NH // 2):
                            for way in ways:
                                emit(way, step, early[way][h])
                        for h in range(NH // 2):
                            for way in ways:
                                if step < 3:
                                    emit(way, step + 1, late[way][h])

                ring_order(step - 1, run)
                hook('after', step)
        parts = []
        for h in range(NH):
            parts.append(up[7, h * H:(h + 1) * H] + got(0, 3, h) + got(1, 3, h))
        new_user = jnp.concatenate(parts, axis=0).astype(BF16)
        usum[...] += new_user.astype(F32)
        return new_user

    def items_next(k):
        new_item = item_total(k).astype(BF16)
        isum[...] += new_item.astype(F32)
        ei_pan[k + 1, c, spot] = new_item
        gather_plane(ei_pan.at[k + 1], ei_ssem, ei_rsem.at[(k + 1) % 2])

    def items_forward(k):
        forward_plane(ei_pan.at[k], ei_rsem.at[k % 2], fw_ssem, fw_rsem.at[k % 2], ei_pan.at[k])

    def items_wait(k):
        wait_plane(ei_pan.at[k], fw_rsem.at[k % 2])

    hop0(1)
    items_wait(0)

    def first_pair():
        last0()
        item_pair(0, 0)

    def last_pair():
        item_pair(0, 3)
        items_send(0)

    new_user = user_total(0, {('piece', 0): lambda: hop0(2), ('piece', 1): first_pair, ('piece', 2): lambda: item_pair(0, 1),
                              ('piece', 3): lambda: item_pair(0, 2), ('own',): last_pair})
    begin1, hop1, last1 = gather_user(1)
    begin1(new_user)
    hop1(0)
    item_pair(1, 0)
    hop1(1)
    item_pair(1, 1)
    items_next(0)
    hop1(2)
    item_pair(1, 2)
    last1()
    item_pair(1, 3)
    items_forward(1)
    items_send(1)
    items_wait(1)
    new_user = user_total(1, {('after', 2): lambda: items_next(1)})
    begin2, hop2, last2 = gather_user(2)
    begin2(new_user)
    items_forward(2)
    items_wait(2)

    user_total(2, {('after', 1): lambda: hop2(0), ('after', 2): lambda: hop2(1)})
    final_user = (usum[...] / (LAYERS + 1)).astype(BF16)
    fu_v[...] = final_user
    outs = [pltpu.make_async_copy(fu_v, fu_out, out_sem.at[0])]
    outs[0].start()

    qs[...] = jnp.dot(hot[...], final_user, preferred_element_type=F32).astype(BF16).reshape(2, G // 2, QB, E)
    to_partner = remote(qs.at[other], qp, q_ssem.at[0], q_rsem.at[0], col, partner)
    to_partner.start()
    hop2(2)
    to_partner.wait_recv()
    qt[...] = (qs[c].astype(F32) + qp[...].astype(F32)).astype(BF16)
    for slot, dx, py, px in plane():
        remote(qt.at[px * Y + py], qr.at[slot], q_ssem.at[1], q_rsem.at[1], z * Y + py, px * 2 + c).start()
    last2()
    item_parts(2)
    items_send(2, 1)
    wait_bytes(qr, q_rsem.at[1])
    total = qt[spot].astype(F32)
    for slot in range(G // 2 - 1):
        total = total + qr[slot].astype(F32)
    qzs[...] = total.astype(BF16)
    for d in (4, 3, 5, 2, 6, 1, 7):
        remote(qzs, qz.at[d - 1], q_ssem.at[2], q_rsem.at[2], zat(d) * Y + y, row).start()
    wait_bytes(qz, q_rsem.at[2])
    for d in range(Z - 1):
        total = total + qz[d].astype(F32)
    qall[c, spot] = total.astype(BF16)
    gather_plane(qall, q_ssem.at[3], qg_rsem)
    new_item = item_total(2).astype(BF16)
    fi_v[...] = ((isum[...] + new_item.astype(F32)) / (LAYERS + 1)).astype(BF16)
    outs.append(pltpu.make_async_copy(fi_v, fi_out, out_sem.at[1]))
    outs[1].start()
    forward_plane(qall, qg_rsem, q_ssem.at[4], qf_rsem, q_out)
    outs.append(pltpu.make_async_copy(qall.at[c], q_out.at[c], out_sem.at[2]))
    outs[2].start()
    wait_plane(q_out, qf_rsem)

    wait_bytes(rs_y, rs_ssem.at[0])
    wait_bytes(rs_z.at[pl.ds(0, Z - 1)], rs_ssem.at[1])
    wait_bytes(cs_row.at[pl.ds(0, R - 1)], cs_ssem.at[0])
    wait_bytes(cs_y.at[pl.ds(0, Y - 1)], cs_ssem.at[1])
    wait_bytes(msend.at[pl.ds(0, Y - 1)], mask_ssem)
    wait_bytes(ei_pan.at[:, 0, pl.ds(0, G // 2 - 1)], ei_ssem)
    wait_bytes(ei_pan.at[:, 0], fw_ssem)
    wait_bytes(pr, pr_ssem)
    wait_bytes(ir, ip_ssem)
    wait_bytes(eu_pan.at[:, pl.ds(0, 7)], ag_ssem)
    for k in range(LAYERS):
        wait_bytes(up.at[pl.ds(0, 7)], us_ssem.at[k])
    to_partner.wait_send()
    wait_bytes(qr, q_ssem.at[1])
    wait_bytes(qz, q_ssem.at[2])
    wait_bytes(qr, q_ssem.at[3])
    wait_bytes(qt, q_ssem.at[4])
    for out in outs:
        out.wait()


def finish(user_ref, item_ref, picked_ref, fu_ref, fi_ref, sc_ref):
    fu_ref[...] = user_ref[...]
    fi_ref[...] = item_ref[...]
    sc_ref[...] = lax.dot_general(item_ref[...], picked_ref[...], CONTRACT_LANES, preferred_element_type=F32)


def propagate(mask, user, item, queries):
    dma = pltpu.SemaphoreType.DMA
    vmem, free = pl.BlockSpec(memory_space=pltpu.VMEM), pl.BlockSpec(memory_space=pl.ANY)
    L, N = LAYERS, G // 2
    final_user, final_item, picked = pl.pallas_call(
        kernel,
        out_shape=(jax.ShapeDtypeStruct((UB, E), BF16), jax.ShapeDtypeStruct((IB, E), BF16),
                   jax.ShapeDtypeStruct((2, N, QB, E), BF16)),
        in_specs=[pl.BlockSpec(memory_space=pltpu.HBM)] * 4,
        out_specs=(free, free, free),
        scratch_shapes=[
            pltpu.VMEM((Z, Y * UB, E), jnp.int32),
            pltpu.VMEM((UB, E), BF16),
            pltpu.VMEM((IB, E), BF16),
            pltpu.VMEM((1, NQ), jnp.int32),
            pltpu.VMEM((Y, Z, UB, E), BF16),
            pltpu.VMEM((Z, Y - 1, UB, E), BF16),
            pltpu.VMEM((Y, Z, UB, E), BF16),
            pltpu.VMEM((Y, E, Z * UB), BF16),
            pltpu.VMEM((Y, Z, UB), F32),
            pltpu.VMEM((Y - 1, Z, UB), F32),
            pltpu.VMEM((Z, Z, UB), F32),
            pltpu.VMEM((1, E), F32),
            pltpu.VMEM((R, 1, E), F32),
            pltpu.VMEM((Y, 1, E), F32),
            pltpu.VMEM((Z, UB), F32),
            pltpu.VMEM((Y, 1, E), F32),
            pltpu.VMEM((L, Z, UB, E), BF16),
            pltpu.VMEM((L, 2, N, IB, E), BF16),
            pltpu.VMEM((Z, UB, E), F32),
            pltpu.VMEM((Y, E, E), F32),
            pltpu.VMEM((L, 2, 4, UB, E), F32),
            pltpu.VMEM((L, 2, 4, UB, E), F32),
            pltpu.VMEM((L, 2, N, IB, E), F32),
            pltpu.VMEM((L, Y, X, IB, E), F32),
            pltpu.VMEM((L, N, IB, E), F32),
            pltpu.VMEM((L, N - 1, IB, E), F32),
            pltpu.VMEM((NQ, UB), BF16),
            pltpu.VMEM((2, N, QB, E), BF16),
            pltpu.VMEM((N, QB, E), BF16),
            pltpu.VMEM((N, QB, E), BF16),
            pltpu.VMEM((N - 1, QB, E), BF16),
            pltpu.VMEM((Z - 1, QB, E), BF16),
            pltpu.VMEM((QB, E), BF16),
            pltpu.VMEM((2, N, QB, E), BF16),
            pltpu.VMEM((UB, E), BF16),
            pltpu.VMEM((IB, E), BF16),
            pltpu.VMEM((UB, E), F32),
            pltpu.VMEM((IB, E), F32),
            dma((Z + 3,)), dma, dma((Z,)),
            dma((2,)), dma, dma,
            dma((2,)), dma((2,)),
            dma, dma((2, X)), dma, dma((2, X)),
            dma((L,)), dma((2, 4, NH)),
            dma, dma((2, Y)), dma, dma((L,)),
            dma, dma((2, 4, NH)),
            dma((5,)), dma((3,)), dma((X,)), dma((X,)),
            dma((3,)),
        ],
        compiler_params=pltpu.CompilerParams(collective_id=0, has_side_effects=True, vmem_limit_bytes=50 * 2**20),
    )(*(pltpu.with_memory_space_constraint(a, pltpu.HBM) for a in (mask, user, item, queries.reshape(1, NQ))))
    final_user, final_item, scores = pl.pallas_call(
        finish,
        out_shape=(jax.ShapeDtypeStruct((UB, E), BF16), jax.ShapeDtypeStruct((IB, E), BF16),
                   jax.ShapeDtypeStruct((IB, NQ), F32)),
        in_specs=[vmem, vmem, vmem],
        out_specs=(vmem, vmem, vmem),
        compiler_params=pltpu.CompilerParams(vmem_limit_bytes=8 * 2**20),
    )(final_user, final_item, picked.reshape(NQ, E))
    return final_user, final_item, scores.T


def solution(mesh):
    return jax.shard_map(propagate, mesh=mesh,
                         in_specs=(P('row', 'col'), P(('row', 'col'), None), P(('col', 'row'), None), P()),
                         out_specs=(P(('row', 'col'), None), P(('col', 'row'), None), P(None, ('col', 'row'))),
                         check_vma=False)
```

```python
import jax
import jax.numpy as jnp
from jax import lax
from jax.experimental import pallas as pl
from jax.experimental.pallas import tpu as pltpu
from jax.sharding import PartitionSpec as P

LAYERS = 3
Z, Y, X = 8, 4, 4
R = 2 * X
G = Y * R
UB, IB = 128, 32
E = 256
NQ = 1024
QB = NQ // G
NH = 4
H = UB // NH
F32, BF16 = jnp.float32, jnp.bfloat16
MESH = pl.DeviceIdType.MESH
CONTRACT_ROWS = (((0,), (0,)), ((), ()))
CONTRACT_LANES = (((1,), (1,)), ((), ()))


def remote(src, dst, send_sem, recv_sem, col, row):
    return pltpu.make_async_remote_copy(src_ref=src, dst_ref=dst, send_sem=send_sem, recv_sem=recv_sem,
                                        device_id=(col, row), device_id_type=MESH)


def wait_bytes(ref, sem):
    pltpu.make_async_copy(ref, ref, sem).wait()


def kernel(mask_ref, user_hbm, item_hbm, query_hbm, fu_out, fi_out, q_out,
           mask_v, user_ref, item_ref, query_ref, msend, mrecv, adj, adjt, rs_send, rs_y, rs_z, cs_send, cs_row, cs_y, invu, invi,
           eu_pan, ei_pan, up, macc, us, ur, ip, pr, iq, ir, hot, qs, qp, qt, qr, qz, qzs, qall, fu_v, fi_v, usum, isum,
           load_sem, mask_ssem, mask_rsem, rs_ssem, rs_rsem, rz_rsem, cs_ssem, cs_rsem, ei_ssem, ei_rsem, fw_ssem, fw_rsem, us_ssem, us_rsem,
           pr_ssem, pr_rsem, ip_ssem, ip_rsem, ag_ssem, ag_rsem, q_ssem, q_rsem, qg_rsem, qf_rsem, out_sem):
    col = lax.axis_index('col')
    row = lax.axis_index('row')
    z, y = lax.div(col, Y), lax.rem(col, Y)
    x, c = lax.div(row, 2), lax.rem(row, 2)
    other = 1 - c
    partner = x * 2 + other
    spot = x * Y + y

    def zat(d):
        return lax.rem(z + (d % Z), Z)

    def yat(d):
        return lax.rem(y + (d % Y), Y)

    def xat(d):
        return lax.rem(x + (d % X), X)

    def plane():
        for dx in (2, 1, 3, 0):
            for dy in (2, 1, 3, 0):
                if dy or dx:
                    yield dx * Y + dy - 1, dx, yat(dy), xat(dx)

    order = [4, 3, -3, 2, -2, 1, -1, 0]
    piece_of = {d: j for j, d in enumerate(order)}
    place = lax.rem(z, Z // 2)

    def ring_order(step, run):
        if step == 0:
            pl.when(place == 0)(lambda: run(((1,), (0,))))
            pl.when(place == Z // 2 - 1)(lambda: run(((0,), (1,))))
            pl.when((place > 0) & (place < Z // 2 - 1))(lambda: run(((0, 1),)))
        else:
            pl.when(place < Z // 4)(lambda: run(((1,), (0,))))
            pl.when(place >= Z // 4)(lambda: run(((0,), (1,))))

    early = (list(range(NH // 2)), list(range(NH // 2, NH)))
    late = (early[1], early[0])
    right, left = zat(1) * Y + y, zat(-1) * Y + y

    loads = []
    for j, d in enumerate(order):
        zc = zat(d)
        load = pltpu.make_async_copy(mask_ref.at[pl.ds(zc * (Y * UB), Y * UB)], mask_v.at[j], load_sem.at[j])
        load.start()
        loads.append(load)

    small = []
    for i, (src, dst) in enumerate(((user_hbm, user_ref), (item_hbm, item_ref), (query_hbm, query_ref))):
        small.append(pltpu.make_async_copy(src, dst, load_sem.at[Z + i]))
        small[i].start()

    barrier = pltpu.get_barrier_semaphore()
    for d in range(1, R):
        pl.semaphore_signal(barrier, inc=1, device_id=(col, lax.rem(row + d, R)), device_id_type=MESH)
    for d in range(1, Y):
        pl.semaphore_signal(barrier, inc=1, device_id=(z * Y + yat(d), row), device_id_type=MESH)
    for d in range(1, Z):
        pl.semaphore_signal(barrier, inc=1, device_id=(zat(d) * Y + y, row), device_id_type=MESH)

    ones_w = jnp.ones((8, E), BF16)
    colsum = jnp.zeros((8, E), F32)

    def send_mask(j):
        for d in range(1, Y):
            py = yat(d)
            remote(msend.at[py, j], mrecv.at[j, d - 1], mask_ssem, mask_rsem.at[j], z * Y + py, row).start()

    for j, d in enumerate(order):
        zc = zat(d)
        loads[j].wait()
        for p in range(Y):
            wide = mask_v[j, p * UB:(p + 1) * UB, :].astype(F32)
            block = wide.astype(BF16)
            msend[p, j] = block
            sums = lax.dot_general(ones_w, block, CONTRACT_LANES, preferred_element_type=F32)
            rs_send[p, pl.ds(zc, 1), :] = sums[0:1]
            colsum = colsum + jnp.sum(wide.reshape(UB // 8, 8, E), axis=0)
    cs_send[...] = jnp.sum(colsum, axis=0, keepdims=True)
    cs_row[row] = cs_send[...]
    for load in small:
        load.wait()
    ei_pan[0, c, spot] = item_ref[...]

    def gather_user(k):
        def send(way, step, h):
            src = eu_pan.at[k, zat(-step if way == 0 else step), pl.ds(h * H, H)]
            remote(src, src, ag_ssem, ag_rsem.at[way, step, h], right if way == 0 else left, row).start()

        def got(way, step, h):
            dst = eu_pan.at[k, zat(-step - 1 if way == 0 else step + 1), pl.ds(h * H, H)]
            wait_bytes(dst, ag_rsem.at[way, step, h])

        def begin(new_user):
            eu_pan[k, z] = new_user
            for h in range(NH):
                for way in range(2):
                    send(way, 0, (early[way] + late[way])[h])

        def hop(step):
            def run(groups):
                for ways in groups:
                    for h in range(NH):
                        for way in ways:
                            hh = (early[way] + late[way])[h]
                            got(way, step, hh)
                            if step < 2 or h < NH // 2:
                                send(way, step + 1, hh)

            ring_order(step, run)

        def last():
            for h in range(NH // 2):
                for way in range(2):
                    got(way, 3, early[way][h])

        return begin, hop, last

    pl.semaphore_wait(barrier, R - 1 + Y - 1 + Z - 1)
    for d in range(1, Y):
        remote(rs_send.at[yat(d)], rs_y.at[d - 1], rs_ssem.at[0], rs_rsem, z * Y + yat(d), row).start()
    for d in range(1, R):
        remote(cs_send, cs_row.at[row], cs_ssem.at[0], cs_rsem.at[0], col, lax.rem(row + d, R)).start()
    for d in range(1, Y):
        remote(item_ref, ei_pan.at[0, c, spot], ei_ssem, ei_rsem.at[0, 0], z * Y + yat(d), row).start()
    send_mask(0)
    begin0, hop0, last0 = gather_user(0)
    begin0(user_ref[...])
    send_mask(1)

    usum[...] = user_ref[...].astype(F32)
    isum[...] = item_ref[...].astype(F32)
    wait_bytes(rs_y, rs_rsem)
    rs_z[z] = rs_send[y] + rs_y[0] + rs_y[1] + rs_y[2]
    for d in (4, 3, 5, 2, 6, 1, 7):
        remote(rs_z.at[z], rs_z.at[z], rs_ssem.at[1], rz_rsem, zat(d) * Y + y, row).start()

    wait_bytes(ei_pan.at[0, c, pl.ds(0, Y - 1)], ei_rsem.at[0, 0])
    own = ei_pan.at[0, c, pl.ds(x * Y, Y)]
    for d in range(1, X):
        remote(own, own, ei_ssem, ei_rsem.at[0, d], col, xat(d) * 2 + c).start()
    remote(own, own, fw_ssem, fw_rsem.at[0, 0], col, partner).start()

    wait_bytes(cs_row.at[pl.ds(0, R - 1)], cs_rsem.at[0])
    deg = cs_row[0]
    for r in range(1, R):
        deg = deg + cs_row[r]
    cs_y[y] = deg
    for d in range(1, Y):
        remote(cs_y.at[y], cs_y.at[y], cs_ssem.at[1], cs_rsem.at[1], z * Y + yat(d), row).start()
    for j in range(2, Z):
        send_mask(j)

    base = (row * (Z * Y) + col) * UB
    ids = lax.broadcasted_iota(jnp.int32, (UB, NQ), 0) + base
    hot[...] = jnp.where(ids == query_ref[...], 1.0, 0.0).T.astype(BF16)

    hop0(0)
    for d in (1, 3, 2):
        rows = pl.ds(xat(-d) * Y, Y)
        wait_bytes(ei_pan.at[0, c, rows], ei_rsem.at[0, d])
        remote(ei_pan.at[0, c, rows], ei_pan.at[0, c, rows], fw_ssem, fw_rsem.at[0, d], col, partner).start()
    wait_bytes(cs_y.at[pl.ds(0, Y - 1)], cs_rsem.at[1])
    for s in range(Y):
        invi[s] = lax.rsqrt(jnp.maximum(cs_y[s], 1.0))
    wait_bytes(rs_z.at[pl.ds(0, Z - 1)], rz_rsem)
    deg = rs_z[0]
    for d in range(1, Z):
        deg = deg + rs_z[d]
    invu[...] = lax.rsqrt(jnp.maximum(deg, 1.0))

    def make_adj(j, zc):
        wait_bytes(mrecv.at[j], mask_rsem.at[j])
        iu = jnp.broadcast_to(invu[pl.ds(zc, 1), :], (UB, UB)).T
        iu = jnp.concatenate([iu, iu], axis=1)
        for d in range(Y):
            s = yat(-d)
            m = (msend[y, j] if d == 0 else mrecv[j, d - 1]).astype(F32)
            a = (iu * m) * invi[s]
            adj[s, zc] = a.astype(BF16)
            adjt[s, :, pl.ds(pl.multiple_of(zc * UB, UB), UB)] = a.T.astype(BF16)

    def user_piece(k, j):
        zc = zat(order[j])
        if k == 0:
            make_adj(j, zc)
        acc = None
        for s in range(Y):
            panel = jnp.concatenate([ei_pan[k, cc, xx * Y + s] for xx in range(X) for cc in range(2)], axis=0)
            t = jnp.dot(adj[s, zc], panel, preferred_element_type=F32)
            acc = t if acc is None else acc + t
        up[j] = acc

    def item_share(k, product, lag=Y):
        for j, dy in enumerate((2, 1, 3, 0)):
            s = yat(dy)
            part = product(s).reshape(X, 2, IB, E)
            for xx in range(X):
                for cc in range(2):
                    ip[k, cc, s * X + xx] = part[xx, cc]
            remote(ip.at[k, other, pl.ds(s * X, X)], pr.at[k, j], pr_ssem, pr_rsem.at[k % 2, j], col, partner).start()
            if j >= lag:
                item_send(k, j - lag)

    def item_parts(k):
        eu = eu_pan[k].reshape(Z * UB, E)
        item_share(k, lambda s: jnp.dot(adjt[s], eu, preferred_element_type=F32), lag=3)

    pairs = (((4, 3), (-3, 2), (-2, 1), (-1, 0)), ((0, 1), (-1, 2), (-2, 3), (-3, 4)))

    def item_pair(k, n):
        near = [zat(d) for d in pairs[k][n]]
        eu = jnp.concatenate([eu_pan[k, zc] for zc in near], axis=0)

        def add(s):
            lhs = jnp.concatenate([adjt[s, :, pl.ds(pl.multiple_of(zc * UB, UB), UB)] for zc in near], axis=1)
            part = jnp.dot(lhs, eu, preferred_element_type=F32)
            return part + macc[s] if n else part

        if n < 3:
            for s in range(Y):
                macc[s] = add(s)
        else:
            item_share(k, add)

    def item_send(k, j):
        dy = (2, 1, 3, 0)[j]
        s = yat(dy)
        wait_bytes(pr.at[k, j], pr_rsem.at[k % 2, j])
        iq[k, pl.ds(s * X, X)] = ip[k, c, pl.ds(s * X, X)] + pr[k, j]
        for dx in (2, 1, 3, 0):
            if dy or dx:
                px = xat(dx)
                remote(iq.at[k, s * X + px], ir.at[k, dy * X + dx - 1], ip_ssem, ip_rsem.at[k],
                       z * Y + s, px * 2 + c).start()

    def items_send(k, first=0):
        for j in range(first, Y):
            item_send(k, j)

    def item_total(k):
        wait_bytes(ir.at[k], ip_rsem.at[k])
        total = iq[k, y * X + x]
        for slot in range(G // 2 - 1):
            total = total + ir[k, slot]
        return total

    def gather_plane(pan, ssem, rsem):
        for slot, dx, py, px in plane():
            remote(pan.at[c, spot], pan.at[c, spot], ssem, rsem.at[dx], z * Y + py, px * 2 + c).start()

    def forward_plane(pan, rsem, fssem, frsem, dst):
        for dx in (0, 1, 3, 2):
            rows = pl.ds(xat(-dx) * Y, Y)
            wait_bytes(pan.at[c, pl.ds(0, Y if dx else Y - 1)], rsem.at[dx])
            remote(pan.at[c, rows], dst.at[c, rows], fssem, frsem.at[dx], col, partner).start()

    def wait_plane(pan, frsem):
        for dx in (0, 1, 3, 2):
            wait_bytes(pan.at[other, pl.ds(xat(-dx) * Y, Y)], frsem.at[dx])

    def user_total(k, hooks):
        def emit(way, step, h, first=False):
            rows = pl.ds(h * H, H)
            j = piece_of[4 - step] if way == 0 or step == 0 else piece_of[step - 4]
            value = up[j, h * H:(h + 1) * H]
            if not first:
                value = value + got(way, step - 1, h)
            us[k, way, step, h * H:(h + 1) * H] = value
            remote(us.at[k, way, step, rows], ur.at[k, way, step, rows], us_ssem.at[k], us_rsem.at[way, step, h],
                   right if way == 0 else left, row).start()

        def got(way, step, h):
            wait_bytes(ur.at[k, way, step, pl.ds(h * H, H)], us_rsem.at[way, step, h])
            return ur[k, way, step, h * H:(h + 1) * H]

        def hook(*at):
            if at in hooks:
                hooks[at]()

        user_piece(k, 0)
        for h in range(NH // 2):
            emit(0, 0, early[0][h], True)
            emit(1, 0, early[1][h], True)
        if k == 0:
            hook('piece', 0)
            for step in range(1, 4):
                for way in range(2):
                    user_piece(k, 2 * step - 1 + way)
                    for h in early[way] + late[way]:
                        emit(way, step, h, step == 1 and h in late[way])
                hook('piece', step)
            user_piece(k, 7)
            hook('own')
        else:
            for way in range(2):
                user_piece(k, 1 + way)
                for h in late[way]:
                    emit(way, 1, h, True)
            for step in range(1, 4):
                hook('before', step)
                if step < 3:
                    user_piece(k, 2 * step + 1)
                    user_piece(k, 2 * step + 2)
                else:
                    user_piece(k, 7)
                def run(groups):
                    for ways in groups:
                        for h in range(NH // 2):
                            for way in ways:
                                emit(way, step, early[way][h])
                        for h in range(NH // 2):
                            for way in ways:
                                if step < 3:
                                    emit(way, step + 1, late[way][h])

                ring_order(step - 1, run)
                hook('after', step)
        parts = []
        for h in range(NH):
            parts.append(up[7, h * H:(h + 1) * H] + got(0, 3, h) + got(1, 3, h))
        new_user = jnp.concatenate(parts, axis=0).astype(BF16)
        usum[...] += new_user.astype(F32)
        return new_user

    def items_next(k):
        new_item = item_total(k).astype(BF16)
        isum[...] += new_item.astype(F32)
        ei_pan[k + 1, c, spot] = new_item
        gather_plane(ei_pan.at[k + 1], ei_ssem, ei_rsem.at[(k + 1) % 2])

    def items_forward(k):
        forward_plane(ei_pan.at[k], ei_rsem.at[k % 2], fw_ssem, fw_rsem.at[k % 2], ei_pan.at[k])

    def items_wait(k):
        wait_plane(ei_pan.at[k], fw_rsem.at[k % 2])

    hop0(1)
    items_wait(0)

    new_user = user_total(0, {('piece', 0): lambda: hop0(2), ('piece', 1): last0, ('own',): lambda: item_parts(0)})
    begin1, hop1, last1 = gather_user(1)
    begin1(new_user)
    items_send(0, 1)
    hop1(0)
    item_pair(1, 0)
    hop1(1)
    item_pair(1, 1)
    items_next(0)
    hop1(2)
    item_pair(1, 2)
    last1()
    item_pair(1, 3)
    items_forward(1)
    items_send(1)
    items_wait(1)
    new_user = user_total(1, {('after', 2): lambda: items_next(1)})
    begin2, hop2, last2 = gather_user(2)
    begin2(new_user)
    items_forward(2)
    items_wait(2)

    user_total(2, {('after', 2): lambda: hop2(0), ('after', 3): lambda: hop2(1)})
    final_user = (usum[...] / (LAYERS + 1)).astype(BF16)
    fu_v[...] = final_user
    outs = [pltpu.make_async_copy(fu_v, fu_out, out_sem.at[0])]
    outs[0].start()

    qs[...] = jnp.dot(hot[...], final_user, preferred_element_type=F32).astype(BF16).reshape(2, G // 2, QB, E)
    to_partner = remote(qs.at[other], qp, q_ssem.at[0], q_rsem.at[0], col, partner)
    to_partner.start()
    hop2(2)
    to_partner.wait_recv()
    qt[...] = (qs[c].astype(F32) + qp[...].astype(F32)).astype(BF16)
    for slot, dx, py, px in plane():
        remote(qt.at[px * Y + py], qr.at[slot], q_ssem.at[1], q_rsem.at[1], z * Y + py, px * 2 + c).start()
    last2()
    item_parts(2)
    items_send(2, 1)
    wait_bytes(qr, q_rsem.at[1])
    total = qt[spot].astype(F32)
    for slot in range(G // 2 - 1):
        total = total + qr[slot].astype(F32)
    qzs[...] = total.astype(BF16)
    for d in (4, 3, 5, 2, 6, 1, 7):
        remote(qzs, qz.at[d - 1], q_ssem.at[2], q_rsem.at[2], zat(d) * Y + y, row).start()
    wait_bytes(qz, q_rsem.at[2])
    for d in range(Z - 1):
        total = total + qz[d].astype(F32)
    qall[c, spot] = total.astype(BF16)
    gather_plane(qall, q_ssem.at[3], qg_rsem)
    new_item = item_total(2).astype(BF16)
    fi_v[...] = ((isum[...] + new_item.astype(F32)) / (LAYERS + 1)).astype(BF16)
    outs.append(pltpu.make_async_copy(fi_v, fi_out, out_sem.at[1]))
    outs[1].start()
    forward_plane(qall, qg_rsem, q_ssem.at[4], qf_rsem, q_out)
    outs.append(pltpu.make_async_copy(qall.at[c], q_out.at[c], out_sem.at[2]))
    outs[2].start()
    wait_plane(q_out, qf_rsem)

    wait_bytes(rs_y, rs_ssem.at[0])
    wait_bytes(rs_z.at[pl.ds(0, Z - 1)], rs_ssem.at[1])
    wait_bytes(cs_row.at[pl.ds(0, R - 1)], cs_ssem.at[0])
    wait_bytes(cs_y.at[pl.ds(0, Y - 1)], cs_ssem.at[1])
    wait_bytes(msend.at[pl.ds(0, Y - 1)], mask_ssem)
    wait_bytes(ei_pan.at[:, 0, pl.ds(0, G // 2 - 1)], ei_ssem)
    wait_bytes(ei_pan.at[:, 0], fw_ssem)
    wait_bytes(pr, pr_ssem)
    wait_bytes(ir, ip_ssem)
    wait_bytes(eu_pan.at[:, pl.ds(0, 7)], ag_ssem)
    for k in range(LAYERS):
        wait_bytes(up.at[pl.ds(0, 7)], us_ssem.at[k])
    to_partner.wait_send()
    wait_bytes(qr, q_ssem.at[1])
    wait_bytes(qz, q_ssem.at[2])
    wait_bytes(qr, q_ssem.at[3])
    wait_bytes(qt, q_ssem.at[4])
    for out in outs:
        out.wait()


def finish(user_ref, item_ref, picked_ref, fu_ref, fi_ref, sc_ref):
    fu_ref[...] = user_ref[...]
    fi_ref[...] = item_ref[...]
    sc_ref[...] = lax.dot_general(item_ref[...], picked_ref[...], CONTRACT_LANES, preferred_element_type=F32)


def propagate(mask, user, item, queries):
    dma = pltpu.SemaphoreType.DMA
    vmem, free = pl.BlockSpec(memory_space=pltpu.VMEM), pl.BlockSpec(memory_space=pl.ANY)
    L, N = LAYERS, G // 2
    final_user, final_item, picked = pl.pallas_call(
        kernel,
        out_shape=(jax.ShapeDtypeStruct((UB, E), BF16), jax.ShapeDtypeStruct((IB, E), BF16),
                   jax.ShapeDtypeStruct((2, N, QB, E), BF16)),
        in_specs=[pl.BlockSpec(memory_space=pltpu.HBM)] * 4,
        out_specs=(free, free, free),
        scratch_shapes=[
            pltpu.VMEM((Z, Y * UB, E), jnp.int32),
            pltpu.VMEM((UB, E), BF16),
            pltpu.VMEM((IB, E), BF16),
            pltpu.VMEM((1, NQ), jnp.int32),
            pltpu.VMEM((Y, Z, UB, E), BF16),
            pltpu.VMEM((Z, Y - 1, UB, E), BF16),
            pltpu.VMEM((Y, Z, UB, E), BF16),
            pltpu.VMEM((Y, E, Z * UB), BF16),
            pltpu.VMEM((Y, Z, UB), F32),
            pltpu.VMEM((Y - 1, Z, UB), F32),
            pltpu.VMEM((Z, Z, UB), F32),
            pltpu.VMEM((1, E), F32),
            pltpu.VMEM((R, 1, E), F32),
            pltpu.VMEM((Y, 1, E), F32),
            pltpu.VMEM((Z, UB), F32),
            pltpu.VMEM((Y, 1, E), F32),
            pltpu.VMEM((L, Z, UB, E), BF16),
            pltpu.VMEM((L, 2, N, IB, E), BF16),
            pltpu.VMEM((Z, UB, E), F32),
            pltpu.VMEM((Y, E, E), F32),
            pltpu.VMEM((L, 2, 4, UB, E), F32),
            pltpu.VMEM((L, 2, 4, UB, E), F32),
            pltpu.VMEM((L, 2, N, IB, E), F32),
            pltpu.VMEM((L, Y, X, IB, E), F32),
            pltpu.VMEM((L, N, IB, E), F32),
            pltpu.VMEM((L, N - 1, IB, E), F32),
            pltpu.VMEM((NQ, UB), BF16),
            pltpu.VMEM((2, N, QB, E), BF16),
            pltpu.VMEM((N, QB, E), BF16),
            pltpu.VMEM((N, QB, E), BF16),
            pltpu.VMEM((N - 1, QB, E), BF16),
            pltpu.VMEM((Z - 1, QB, E), BF16),
            pltpu.VMEM((QB, E), BF16),
            pltpu.VMEM((2, N, QB, E), BF16),
            pltpu.VMEM((UB, E), BF16),
            pltpu.VMEM((IB, E), BF16),
            pltpu.VMEM((UB, E), F32),
            pltpu.VMEM((IB, E), F32),
            dma((Z + 3,)), dma, dma((Z,)),
            dma((2,)), dma, dma,
            dma((2,)), dma((2,)),
            dma, dma((2, X)), dma, dma((2, X)),
            dma((L,)), dma((2, 4, NH)),
            dma, dma((2, Y)), dma, dma((L,)),
            dma, dma((2, 4, NH)),
            dma((5,)), dma((3,)), dma((X,)), dma((X,)),
            dma((3,)),
        ],
        compiler_params=pltpu.CompilerParams(collective_id=0, has_side_effects=True, vmem_limit_bytes=50 * 2**20),
    )(*(pltpu.with_memory_space_constraint(a, pltpu.HBM) for a in (mask, user, item, queries.reshape(1, NQ))))
    final_user, final_item, scores = pl.pallas_call(
        finish,
        out_shape=(jax.ShapeDtypeStruct((UB, E), BF16), jax.ShapeDtypeStruct((IB, E), BF16),
                   jax.ShapeDtypeStruct((IB, NQ), F32)),
        in_specs=[vmem, vmem, vmem],
        out_specs=(vmem, vmem, vmem),
        compiler_params=pltpu.CompilerParams(vmem_limit_bytes=8 * 2**20),
    )(final_user, final_item, picked.reshape(NQ, E))
    return final_user, final_item, scores.T


def solution(mesh):
    return jax.shard_map(propagate, mesh=mesh,
                         in_specs=(P('row', 'col'), P(('row', 'col'), None), P(('col', 'row'), None), P()),
                         out_specs=(P(('row', 'col'), None), P(('col', 'row'), None), P(None, ('col', 'row'))),
                         check_vma=False)
```

```python
import jax
import jax.numpy as jnp
from jax import lax
from jax.experimental import pallas as pl
from jax.experimental.pallas import tpu as pltpu
from jax.sharding import PartitionSpec as P

LAYERS = 3
Z, Y, X = 8, 4, 4
R = 2 * X
G = Y * R
UB, IB = 128, 32
E = 256
NQ = 1024
QB = NQ // G
NH = 4
H = UB // NH
F32, BF16 = jnp.float32, jnp.bfloat16
MESH = pl.DeviceIdType.MESH
CONTRACT_ROWS = (((0,), (0,)), ((), ()))
CONTRACT_LANES = (((1,), (1,)), ((), ()))


def remote(src, dst, send_sem, recv_sem, col, row):
    return pltpu.make_async_remote_copy(src_ref=src, dst_ref=dst, send_sem=send_sem, recv_sem=recv_sem,
                                        device_id=(col, row), device_id_type=MESH)


def wait_bytes(ref, sem):
    pltpu.make_async_copy(ref, ref, sem).wait()


def kernel(mask_ref, user_hbm, item_hbm, query_hbm, fu_out, fi_out, q_out,
           mask_v, user_ref, item_ref, query_ref, msend, mrecv, adj, adjt, rs_send, rs_y, rs_z, cs_send, cs_row, cs_y, invu, invi,
           eu_pan, ei_pan, up, macc, us, ur, ip, pr, iq, ir, hot, qs, qp, qt, qr, qz, qzs, qall, fu_v, fi_v, usum, isum,
           load_sem, mask_ssem, mask_rsem, rs_ssem, rs_rsem, rz_rsem, cs_ssem, cs_rsem, ei_ssem, ei_rsem, fw_ssem, fw_rsem, us_ssem, us_rsem,
           pr_ssem, pr_rsem, ip_ssem, ip_rsem, ag_ssem, ag_rsem, q_ssem, q_rsem, qg_rsem, qf_rsem, out_sem):
    col = lax.axis_index('col')
    row = lax.axis_index('row')
    z, y = lax.div(col, Y), lax.rem(col, Y)
    x, c = lax.div(row, 2), lax.rem(row, 2)
    other = 1 - c
    partner = x * 2 + other
    spot = x * Y + y

    def zat(d):
        return lax.rem(z + (d % Z), Z)

    def yat(d):
        return lax.rem(y + (d % Y), Y)

    def xat(d):
        return lax.rem(x + (d % X), X)

    def plane():
        for dx in (2, 1, 3, 0):
            for dy in (2, 1, 3, 0):
                if dy or dx:
                    yield dx * Y + dy - 1, dx, yat(dy), xat(dx)

    order = [4, 3, -3, 2, -2, 1, -1, 0]
    piece_of = {d: j for j, d in enumerate(order)}
    place = lax.rem(z, Z // 2)

    def ring_order(step, run):
        if step == 0:
            pl.when(place == 0)(lambda: run(((1,), (0,))))
            pl.when(place == Z // 2 - 1)(lambda: run(((0,), (1,))))
            pl.when((place > 0) & (place < Z // 2 - 1))(lambda: run(((0, 1),)))
        else:
            pl.when(place < Z // 4)(lambda: run(((1,), (0,))))
            pl.when(place >= Z // 4)(lambda: run(((0,), (1,))))

    early = (list(range(NH // 2)), list(range(NH // 2, NH)))
    late = (early[1], early[0])
    right, left = zat(1) * Y + y, zat(-1) * Y + y

    loads = []
    for j, d in enumerate(order):
        zc = zat(d)
        load = pltpu.make_async_copy(mask_ref.at[pl.ds(zc * (Y * UB), Y * UB)], mask_v.at[j], load_sem.at[j])
        load.start()
        loads.append(load)

    small = []
    for i, (src, dst) in enumerate(((user_hbm, user_ref), (item_hbm, item_ref), (query_hbm, query_ref))):
        small.append(pltpu.make_async_copy(src, dst, load_sem.at[Z + i]))
        small[i].start()

    barrier = pltpu.get_barrier_semaphore()
    for d in range(1, R):
        pl.semaphore_signal(barrier, inc=1, device_id=(col, lax.rem(row + d, R)), device_id_type=MESH)
    for d in range(1, Y):
        pl.semaphore_signal(barrier, inc=1, device_id=(z * Y + yat(d), row), device_id_type=MESH)
    for d in range(1, Z):
        pl.semaphore_signal(barrier, inc=1, device_id=(zat(d) * Y + y, row), device_id_type=MESH)

    ones_w = jnp.ones((8, E), BF16)
    colsum = jnp.zeros((8, E), F32)

    def send_mask(j):
        for d in (2, 1, 3):
            py = yat(d)
            remote(msend.at[py, j], mrecv.at[j, d - 1], mask_ssem, mask_rsem.at[j], z * Y + py, row).start()

    for j, d in enumerate(order):
        zc = zat(d)
        loads[j].wait()
        for p in range(Y):
            wide = mask_v[j, p * UB:(p + 1) * UB, :].astype(F32)
            block = wide.astype(BF16)
            msend[p, j] = block
            sums = lax.dot_general(ones_w, block, CONTRACT_LANES, preferred_element_type=F32)
            rs_send[p, pl.ds(zc, 1), :] = sums[0:1]
            colsum = colsum + jnp.sum(wide.reshape(UB // 8, 8, E), axis=0)
    cs_send[...] = jnp.sum(colsum, axis=0, keepdims=True)
    cs_row[row] = cs_send[...]
    for load in small:
        load.wait()
    ei_pan[0, c, spot] = item_ref[...]

    def gather_user(k):
        def send(way, step, h):
            src = eu_pan.at[k, zat(-step if way == 0 else step), pl.ds(h * H, H)]
            remote(src, src, ag_ssem, ag_rsem.at[way, step, h], right if way == 0 else left, row).start()

        def got(way, step, h):
            dst = eu_pan.at[k, zat(-step - 1 if way == 0 else step + 1), pl.ds(h * H, H)]
            wait_bytes(dst, ag_rsem.at[way, step, h])

        def begin(new_user):
            eu_pan[k, z] = new_user
            for h in range(NH):
                for way in range(2):
                    send(way, 0, (early[way] + late[way])[h])

        def hop(step):
            def run(groups):
                for ways in groups:
                    for h in range(NH):
                        for way in ways:
                            hh = (early[way] + late[way])[h]
                            got(way, step, hh)
                            if step < 2 or h < NH // 2:
                                send(way, step + 1, hh)

            ring_order(step, run)

        def last():
            for h in range(NH // 2):
                for way in range(2):
                    got(way, 3, early[way][h])

        return begin, hop, last

    pl.semaphore_wait(barrier, R - 1 + Y - 1 + Z - 1)
    for d in range(1, Y):
        remote(rs_send.at[yat(d)], rs_y.at[d - 1], rs_ssem.at[0], rs_rsem, z * Y + yat(d), row).start()
    for d in range(1, R):
        remote(cs_send, cs_row.at[row], cs_ssem.at[0], cs_rsem.at[0], col, lax.rem(row + d, R)).start()
    for d in range(1, Y):
        remote(item_ref, ei_pan.at[0, c, spot], ei_ssem, ei_rsem.at[0, 0], z * Y + yat(d), row).start()
    send_mask(0)
    begin0, hop0, last0 = gather_user(0)
    begin0(user_ref[...])
    send_mask(1)

    usum[...] = user_ref[...].astype(F32)
    isum[...] = item_ref[...].astype(F32)
    wait_bytes(rs_y, rs_rsem)
    rs_z[z] = rs_send[y] + rs_y[0] + rs_y[1] + rs_y[2]
    for d in (4, 3, 5, 2, 6, 1, 7):
        remote(rs_z.at[z], rs_z.at[z], rs_ssem.at[1], rz_rsem, zat(d) * Y + y, row).start()

    wait_bytes(ei_pan.at[0, c, pl.ds(0, Y - 1)], ei_rsem.at[0, 0])
    own = ei_pan.at[0, c, pl.ds(x * Y, Y)]
    for d in range(1, X):
        remote(own, own, ei_ssem, ei_rsem.at[0, d], col, xat(d) * 2 + c).start()
    remote(own, own, fw_ssem, fw_rsem.at[0, 0], col, partner).start()

    wait_bytes(cs_row.at[pl.ds(0, R - 1)], cs_rsem.at[0])
    deg = cs_row[0]
    for r in range(1, R):
        deg = deg + cs_row[r]
    cs_y[y] = deg
    for d in range(1, Y):
        remote(cs_y.at[y], cs_y.at[y], cs_ssem.at[1], cs_rsem.at[1], z * Y + yat(d), row).start()
    for j in range(2, Z):
        send_mask(j)

    base = (row * (Z * Y) + col) * UB
    ids = lax.broadcasted_iota(jnp.int32, (UB, NQ), 0) + base
    hot[...] = jnp.where(ids == query_ref[...], 1.0, 0.0).T.astype(BF16)

    hop0(0)
    for d in (1, 3, 2):
        rows = pl.ds(xat(-d) * Y, Y)
        wait_bytes(ei_pan.at[0, c, rows], ei_rsem.at[0, d])
        remote(ei_pan.at[0, c, rows], ei_pan.at[0, c, rows], fw_ssem, fw_rsem.at[0, d], col, partner).start()
    wait_bytes(cs_y.at[pl.ds(0, Y - 1)], cs_rsem.at[1])
    for s in range(Y):
        invi[s] = lax.rsqrt(jnp.maximum(cs_y[s], 1.0))
    wait_bytes(rs_z.at[pl.ds(0, Z - 1)], rz_rsem)
    deg = rs_z[0]
    for d in range(1, Z):
        deg = deg + rs_z[d]
    invu[...] = lax.rsqrt(jnp.maximum(deg, 1.0))

    def make_adj(j, zc):
        wait_bytes(mrecv.at[j], mask_rsem.at[j])
        iu = jnp.broadcast_to(invu[pl.ds(zc, 1), :], (UB, UB)).T
        iu = jnp.concatenate([iu, iu], axis=1)
        for d in range(Y):
            s = yat(-d)
            m = (msend[y, j] if d == 0 else mrecv[j, d - 1]).astype(F32)
            a = (iu * m) * invi[s]
            adj[s, zc] = a.astype(BF16)
            adjt[s, :, pl.ds(pl.multiple_of(zc * UB, UB), UB)] = a.T.astype(BF16)

    def user_piece(k, j):
        zc = zat(order[j])
        if k == 0:
            make_adj(j, zc)
        acc = None
        for s in range(Y):
            panel = jnp.concatenate([ei_pan[k, cc, xx * Y + s] for xx in range(X) for cc in range(2)], axis=0)
            t = jnp.dot(adj[s, zc], panel, preferred_element_type=F32)
            acc = t if acc is None else acc + t
        up[j] = acc

    def item_share(k, product, lag=Y):
        for j, dy in enumerate((2, 1, 3, 0)):
            s = yat(dy)
            part = product(s).reshape(X, 2, IB, E)
            for xx in range(X):
                for cc in range(2):
                    ip[k, cc, s * X + xx] = part[xx, cc]
            remote(ip.at[k, other, pl.ds(s * X, X)], pr.at[k, j], pr_ssem, pr_rsem.at[k % 2, j], col, partner).start()
            if j >= lag:
                item_send(k, j - lag)

    def item_parts(k):
        eu = eu_pan[k].reshape(Z * UB, E)
        item_share(k, lambda s: jnp.dot(adjt[s], eu, preferred_element_type=F32), lag=3)

    pairs = (((4, 3), (-3, 2), (-2, 1), (-1, 0)), ((0, 1), (-1, 2), (-2, 3), (-3, 4)))

    def item_pair(k, n):
        near = [zat(d) for d in pairs[k][n]]
        eu = jnp.concatenate([eu_pan[k, zc] for zc in near], axis=0)

        def add(s):
            lhs = jnp.concatenate([adjt[s, :, pl.ds(pl.multiple_of(zc * UB, UB), UB)] for zc in near], axis=1)
            part = jnp.dot(lhs, eu, preferred_element_type=F32)
            return part + macc[s] if n else part

        if n < 3:
            for s in range(Y):
                macc[s] = add(s)
        else:
            item_share(k, add)

    def item_send(k, j):
        dy = (2, 1, 3, 0)[j]
        s = yat(dy)
        wait_bytes(pr.at[k, j], pr_rsem.at[k % 2, j])
        iq[k, pl.ds(s * X, X)] = ip[k, c, pl.ds(s * X, X)] + pr[k, j]
        for dx in (2, 1, 3, 0):
            if dy or dx:
                px = xat(dx)
                remote(iq.at[k, s * X + px], ir.at[k, dy * X + dx - 1], ip_ssem, ip_rsem.at[k],
                       z * Y + s, px * 2 + c).start()

    def items_send(k, first=0):
        for j in range(first, Y):
            item_send(k, j)

    def item_total(k):
        wait_bytes(ir.at[k], ip_rsem.at[k])
        total = iq[k, y * X + x]
        for slot in range(G // 2 - 1):
            total = total + ir[k, slot]
        return total

    def gather_plane(pan, ssem, rsem):
        for slot, dx, py, px in plane():
            remote(pan.at[c, spot], pan.at[c, spot], ssem, rsem.at[dx], z * Y + py, px * 2 + c).start()

    def forward_plane(pan, rsem, fssem, frsem, dst):
        for dx in (0, 1, 3, 2):
            rows = pl.ds(xat(-dx) * Y, Y)
            wait_bytes(pan.at[c, pl.ds(0, Y if dx else Y - 1)], rsem.at[dx])
            remote(pan.at[c, rows], dst.at[c, rows], fssem, frsem.at[dx], col, partner).start()

    def wait_plane(pan, frsem):
        for dx in (0, 1, 3, 2):
            wait_bytes(pan.at[other, pl.ds(xat(-dx) * Y, Y)], frsem.at[dx])

    def user_total(k, hooks):
        def emit(way, step, h, first=False):
            rows = pl.ds(h * H, H)
            j = piece_of[4 - step] if way == 0 or step == 0 else piece_of[step - 4]
            value = up[j, h * H:(h + 1) * H]
            if not first:
                value = value + got(way, step - 1, h)
            us[k, way, step, h * H:(h + 1) * H] = value
            remote(us.at[k, way, step, rows], ur.at[k, way, step, rows], us_ssem.at[k], us_rsem.at[way, step, h],
                   right if way == 0 else left, row).start()

        def got(way, step, h):
            wait_bytes(ur.at[k, way, step, pl.ds(h * H, H)], us_rsem.at[way, step, h])
            return ur[k, way, step, h * H:(h + 1) * H]

        def hook(*at):
            if at in hooks:
                hooks[at]()

        user_piece(k, 0)
        for h in range(NH // 2):
            emit(0, 0, early[0][h], True)
            emit(1, 0, early[1][h], True)
        if k == 0:
            hook('piece', 0)
            for step in range(1, 4):
                for way in range(2):
                    user_piece(k, 2 * step - 1 + way)
                    for h in early[way] + late[way]:
                        emit(way, step, h, step == 1 and h in late[way])
                hook('piece', step)
            user_piece(k, 7)
            hook('own')
        else:
            for way in range(2):
                user_piece(k, 1 + way)
                for h in late[way]:
                    emit(way, 1, h, True)
            for step in range(1, 4):
                hook('before', step)
                if step < 3:
                    user_piece(k, 2 * step + 1)
                    user_piece(k, 2 * step + 2)
                else:
                    user_piece(k, 7)
                def run(groups):
                    for ways in groups:
                        for h in range(NH // 2):
                            for way in ways:
                                emit(way, step, early[way][h])
                        for h in range(NH // 2):
                            for way in ways:
                                if step < 3:
                                    emit(way, step + 1, late[way][h])

                ring_order(step - 1, run)
                hook('after', step)
        parts = []
        for h in range(NH):
            parts.append(up[7, h * H:(h + 1) * H] + got(0, 3, h) + got(1, 3, h))
        new_user = jnp.concatenate(parts, axis=0).astype(BF16)
        usum[...] += new_user.astype(F32)
        return new_user

    def items_next(k):
        new_item = item_total(k).astype(BF16)
        isum[...] += new_item.astype(F32)
        ei_pan[k + 1, c, spot] = new_item
        gather_plane(ei_pan.at[k + 1], ei_ssem, ei_rsem.at[(k + 1) % 2])

    def items_forward(k):
        forward_plane(ei_pan.at[k], ei_rsem.at[k % 2], fw_ssem, fw_rsem.at[k % 2], ei_pan.at[k])

    def items_wait(k):
        wait_plane(ei_pan.at[k], fw_rsem.at[k % 2])

    hop0(1)
    items_wait(0)

    new_user = user_total(0, {('piece', 0): lambda: hop0(2), ('piece', 1): last0, ('own',): lambda: item_parts(0)})
    begin1, hop1, last1 = gather_user(1)
    begin1(new_user)
    items_send(0, 1)
    hop1(0)
    item_pair(1, 0)
    hop1(1)
    item_pair(1, 1)
    items_next(0)
    hop1(2)
    item_pair(1, 2)
    last1()
    item_pair(1, 3)
    items_forward(1)
    items_send(1)
    items_wait(1)
    new_user = user_total(1, {('after', 2): lambda: items_next(1)})
    begin2, hop2, last2 = gather_user(2)
    begin2(new_user)
    items_forward(2)
    items_wait(2)

    user_total(2, {('after', 2): lambda: hop2(0), ('after', 3): lambda: hop2(1)})
    final_user = (usum[...] / (LAYERS + 1)).astype(BF16)
    fu_v[...] = final_user
    outs = [pltpu.make_async_copy(fu_v, fu_out, out_sem.at[0])]
    outs[0].start()

    qs[...] = jnp.dot(hot[...], final_user, preferred_element_type=F32).astype(BF16).reshape(2, G // 2, QB, E)
    to_partner = remote(qs.at[other], qp, q_ssem.at[0], q_rsem.at[0], col, partner)
    to_partner.start()
    hop2(2)
    to_partner.wait_recv()
    qt[...] = (qs[c].astype(F32) + qp[...].astype(F32)).astype(BF16)
    for slot, dx, py, px in plane():
        remote(qt.at[px * Y + py], qr.at[slot], q_ssem.at[1], q_rsem.at[1], z * Y + py, px * 2 + c).start()
    last2()
    item_parts(2)
    items_send(2, 1)
    wait_bytes(qr, q_rsem.at[1])
    total = qt[spot].astype(F32)
    for slot in range(G // 2 - 1):
        total = total + qr[slot].astype(F32)
    qzs[...] = total.astype(BF16)
    for t in (0, 1, 7, 2, 6, 3, 5, 4):
        def to_plane(t=t):
            remote(qzs, qz.at[lax.rem(t - z + Z, Z) - 1], q_ssem.at[2], q_rsem.at[2], t * Y + y, row).start()
        pl.when(z != t)(to_plane)
    wait_bytes(qz, q_rsem.at[2])
    for d in range(Z - 1):
        total = total + qz[d].astype(F32)
    qall[c, spot] = total.astype(BF16)
    gather_plane(qall, q_ssem.at[3], qg_rsem)
    new_item = item_total(2).astype(BF16)
    fi_v[...] = ((isum[...] + new_item.astype(F32)) / (LAYERS + 1)).astype(BF16)
    outs.append(pltpu.make_async_copy(fi_v, fi_out, out_sem.at[1]))
    outs[1].start()
    forward_plane(qall, qg_rsem, q_ssem.at[4], qf_rsem, q_out)
    outs.append(pltpu.make_async_copy(qall.at[c], q_out.at[c], out_sem.at[2]))
    outs[2].start()
    wait_plane(q_out, qf_rsem)

    wait_bytes(rs_y, rs_ssem.at[0])
    wait_bytes(rs_z.at[pl.ds(0, Z - 1)], rs_ssem.at[1])
    wait_bytes(cs_row.at[pl.ds(0, R - 1)], cs_ssem.at[0])
    wait_bytes(cs_y.at[pl.ds(0, Y - 1)], cs_ssem.at[1])
    wait_bytes(msend.at[pl.ds(0, Y - 1)], mask_ssem)
    wait_bytes(ei_pan.at[:, 0, pl.ds(0, G // 2 - 1)], ei_ssem)
    wait_bytes(ei_pan.at[:, 0], fw_ssem)
    wait_bytes(pr, pr_ssem)
    wait_bytes(ir, ip_ssem)
    wait_bytes(eu_pan.at[:, pl.ds(0, 7)], ag_ssem)
    for k in range(LAYERS):
        wait_bytes(up.at[pl.ds(0, 7)], us_ssem.at[k])
    to_partner.wait_send()
    wait_bytes(qr, q_ssem.at[1])
    wait_bytes(qz, q_ssem.at[2])
    wait_bytes(qr, q_ssem.at[3])
    wait_bytes(qt, q_ssem.at[4])
    for out in outs:
        out.wait()


def finish(user_ref, item_ref, picked_ref, fu_ref, fi_ref, sc_ref):
    fu_ref[...] = user_ref[...]
    fi_ref[...] = item_ref[...]
    sc_ref[...] = lax.dot_general(item_ref[...], picked_ref[...], CONTRACT_LANES, preferred_element_type=F32)


def propagate(mask, user, item, queries):
    dma = pltpu.SemaphoreType.DMA
    vmem, free = pl.BlockSpec(memory_space=pltpu.VMEM), pl.BlockSpec(memory_space=pl.ANY)
    L, N = LAYERS, G // 2
    final_user, final_item, picked = pl.pallas_call(
        kernel,
        out_shape=(jax.ShapeDtypeStruct((UB, E), BF16), jax.ShapeDtypeStruct((IB, E), BF16),
                   jax.ShapeDtypeStruct((2, N, QB, E), BF16)),
        in_specs=[pl.BlockSpec(memory_space=pltpu.HBM)] * 4,
        out_specs=(free, free, free),
        scratch_shapes=[
            pltpu.VMEM((Z, Y * UB, E), jnp.int32),
            pltpu.VMEM((UB, E), BF16),
            pltpu.VMEM((IB, E), BF16),
            pltpu.VMEM((1, NQ), jnp.int32),
            pltpu.VMEM((Y, Z, UB, E), BF16),
            pltpu.VMEM((Z, Y - 1, UB, E), BF16),
            pltpu.VMEM((Y, Z, UB, E), BF16),
            pltpu.VMEM((Y, E, Z * UB), BF16),
            pltpu.VMEM((Y, Z, UB), F32),
            pltpu.VMEM((Y - 1, Z, UB), F32),
            pltpu.VMEM((Z, Z, UB), F32),
            pltpu.VMEM((1, E), F32),
            pltpu.VMEM((R, 1, E), F32),
            pltpu.VMEM((Y, 1, E), F32),
            pltpu.VMEM((Z, UB), F32),
            pltpu.VMEM((Y, 1, E), F32),
            pltpu.VMEM((L, Z, UB, E), BF16),
            pltpu.VMEM((L, 2, N, IB, E), BF16),
            pltpu.VMEM((Z, UB, E), F32),
            pltpu.VMEM((Y, E, E), F32),
            pltpu.VMEM((L, 2, 4, UB, E), F32),
            pltpu.VMEM((L, 2, 4, UB, E), F32),
            pltpu.VMEM((L, 2, N, IB, E), F32),
            pltpu.VMEM((L, Y, X, IB, E), F32),
            pltpu.VMEM((L, N, IB, E), F32),
            pltpu.VMEM((L, N - 1, IB, E), F32),
            pltpu.VMEM((NQ, UB), BF16),
            pltpu.VMEM((2, N, QB, E), BF16),
            pltpu.VMEM((N, QB, E), BF16),
            pltpu.VMEM((N, QB, E), BF16),
            pltpu.VMEM((N - 1, QB, E), BF16),
            pltpu.VMEM((Z - 1, QB, E), BF16),
            pltpu.VMEM((QB, E), BF16),
            pltpu.VMEM((2, N, QB, E), BF16),
            pltpu.VMEM((UB, E), BF16),
            pltpu.VMEM((IB, E), BF16),
            pltpu.VMEM((UB, E), F32),
            pltpu.VMEM((IB, E), F32),
            dma((Z + 3,)), dma, dma((Z,)),
            dma((2,)), dma, dma,
            dma((2,)), dma((2,)),
            dma, dma((2, X)), dma, dma((2, X)),
            dma((L,)), dma((2, 4, NH)),
            dma, dma((2, Y)), dma, dma((L,)),
            dma, dma((2, 4, NH)),
            dma((5,)), dma((3,)), dma((X,)), dma((X,)),
            dma((3,)),
        ],
        compiler_params=pltpu.CompilerParams(collective_id=0, has_side_effects=True, vmem_limit_bytes=50 * 2**20),
    )(*(pltpu.with_memory_space_constraint(a, pltpu.HBM) for a in (mask, user, item, queries.reshape(1, NQ))))
    final_user, final_item, scores = pl.pallas_call(
        finish,
        out_shape=(jax.ShapeDtypeStruct((UB, E), BF16), jax.ShapeDtypeStruct((IB, E), BF16),
                   jax.ShapeDtypeStruct((IB, NQ), F32)),
        in_specs=[vmem, vmem, vmem],
        out_specs=(vmem, vmem, vmem),
        compiler_params=pltpu.CompilerParams(vmem_limit_bytes=8 * 2**20),
    )(final_user, final_item, picked.reshape(NQ, E))
    return final_user, final_item, scores.T


def solution(mesh):
    return jax.shard_map(propagate, mesh=mesh,
                         in_specs=(P('row', 'col'), P(('row', 'col'), None), P(('col', 'row'), None), P()),
                         out_specs=(P(('row', 'col'), None), P(('col', 'row'), None), P(None, ('col', 'row'))),
                         check_vma=False)
```

```python
import jax
import jax.numpy as jnp
from jax import lax
from jax.experimental import pallas as pl
from jax.experimental.pallas import tpu as pltpu
from jax.sharding import PartitionSpec as P

LAYERS = 3
Z, Y, X = 8, 4, 4
R = 2 * X
G = Y * R
UB, IB = 128, 32
E = 256
NQ = 1024
QB = NQ // G
NH = 4
H = UB // NH
F32, BF16 = jnp.float32, jnp.bfloat16
MESH = pl.DeviceIdType.MESH
CONTRACT_ROWS = (((0,), (0,)), ((), ()))
CONTRACT_LANES = (((1,), (1,)), ((), ()))


def remote(src, dst, send_sem, recv_sem, col, row):
    return pltpu.make_async_remote_copy(src_ref=src, dst_ref=dst, send_sem=send_sem, recv_sem=recv_sem,
                                        device_id=(col, row), device_id_type=MESH)


def wait_bytes(ref, sem):
    pltpu.make_async_copy(ref, ref, sem).wait()


def kernel(mask_ref, user_hbm, item_hbm, query_hbm, fu_out, fi_out, q_out,
           mask_v, user_ref, item_ref, query_ref, msend, mrecv, adj, adjt, rs_send, rs_y, rs_z, cs_send, cs_row, cs_y, invu, invi,
           eu_pan, ei_pan, up, macc, us, ur, ip, pr, iq, ir, hot, qs, qp, qt, qr, qz, qzs, qall, fu_v, fi_v, usum, isum,
           load_sem, mask_ssem, mask_rsem, rs_ssem, rs_rsem, rz_rsem, cs_ssem, cs_rsem, ei_ssem, ei_rsem, fw_ssem, fw_rsem, us_ssem, us_rsem,
           pr_ssem, pr_rsem, ip_ssem, ip_rsem, ag_ssem, ag_rsem, q_ssem, q_rsem, qg_rsem, qf_rsem, out_sem):
    col = lax.axis_index('col')
    row = lax.axis_index('row')
    z, y = lax.div(col, Y), lax.rem(col, Y)
    x, c = lax.div(row, 2), lax.rem(row, 2)
    other = 1 - c
    partner = x * 2 + other
    spot = x * Y + y

    def zat(d):
        return lax.rem(z + (d % Z), Z)

    def yat(d):
        return lax.rem(y + (d % Y), Y)

    def xat(d):
        return lax.rem(x + (d % X), X)

    def plane():
        for dx in (2, 1, 3, 0):
            for dy in (2, 1, 3, 0):
                if dy or dx:
                    yield dx * Y + dy - 1, dx, yat(dy), xat(dx)

    order = [4, 3, -3, 2, -2, 1, -1, 0]
    piece_of = {d: j for j, d in enumerate(order)}
    place = lax.rem(z, Z // 2)

    def ring_order(step, run):
        if step == 0:
            pl.when(place == 0)(lambda: run(((1,), (0,))))
            pl.when(place == Z // 2 - 1)(lambda: run(((0,), (1,))))
            pl.when((place > 0) & (place < Z // 2 - 1))(lambda: run(((0, 1),)))
        else:
            pl.when(place < Z // 4)(lambda: run(((1,), (0,))))
            pl.when(place >= Z // 4)(lambda: run(((0,), (1,))))

    early = (list(range(NH // 2)), list(range(NH // 2, NH)))
    late = (early[1], early[0])
    right, left = zat(1) * Y + y, zat(-1) * Y + y

    loads = []
    for j, d in enumerate(order):
        zc = zat(d)
        load = pltpu.make_async_copy(mask_ref.at[pl.ds(zc * (Y * UB), Y * UB)], mask_v.at[j], load_sem.at[j])
        load.start()
        loads.append(load)

    small = []
    for i, (src, dst) in enumerate(((user_hbm, user_ref), (item_hbm, item_ref), (query_hbm, query_ref))):
        small.append(pltpu.make_async_copy(src, dst, load_sem.at[Z + i]))
        small[i].start()

    barrier = pltpu.get_barrier_semaphore()
    for d in range(1, R):
        pl.semaphore_signal(barrier, inc=1, device_id=(col, lax.rem(row + d, R)), device_id_type=MESH)
    for d in range(1, Y):
        pl.semaphore_signal(barrier, inc=1, device_id=(z * Y + yat(d), row), device_id_type=MESH)
    for d in range(1, Z):
        pl.semaphore_signal(barrier, inc=1, device_id=(zat(d) * Y + y, row), device_id_type=MESH)

    ones_w = jnp.ones((8, E), BF16)
    colsum = jnp.zeros((8, E), F32)

    def send_mask(j):
        for d in (2, 1, 3):
            py = yat(d)
            remote(msend.at[py, j], mrecv.at[j, d - 1], mask_ssem, mask_rsem.at[j], z * Y + py, row).start()

    for j, d in enumerate(order):
        zc = zat(d)
        loads[j].wait()
        for p in range(Y):
            wide = mask_v[j, p * UB:(p + 1) * UB, :].astype(F32)
            block = wide.astype(BF16)
            msend[p, j] = block
            sums = lax.dot_general(ones_w, block, CONTRACT_LANES, preferred_element_type=F32)
            rs_send[p, pl.ds(zc, 1), :] = sums[0:1]
            colsum = colsum + jnp.sum(wide.reshape(UB // 8, 8, E), axis=0)
    cs_send[...] = jnp.sum(colsum, axis=0, keepdims=True)
    cs_row[row] = cs_send[...]
    for load in small:
        load.wait()
    ei_pan[0, c, spot] = item_ref[...]

    def gather_user(k):
        def send(way, step, h):
            src = eu_pan.at[k, zat(-step if way == 0 else step), pl.ds(h * H, H)]
            remote(src, src, ag_ssem, ag_rsem.at[way, step, h], right if way == 0 else left, row).start()

        def got(way, step, h):
            dst = eu_pan.at[k, zat(-step - 1 if way == 0 else step + 1), pl.ds(h * H, H)]
            wait_bytes(dst, ag_rsem.at[way, step, h])

        def begin(new_user):
            eu_pan[k, z] = new_user
            for h in range(NH):
                for way in range(2):
                    send(way, 0, (early[way] + late[way])[h])

        def hop(step):
            def run(groups):
                for ways in groups:
                    for h in range(NH):
                        for way in ways:
                            hh = (early[way] + late[way])[h]
                            got(way, step, hh)
                            if step < 2 or h < NH // 2:
                                send(way, step + 1, hh)

            ring_order(step, run)

        def last():
            for h in range(NH // 2):
                for way in range(2):
                    got(way, 3, early[way][h])

        return begin, hop, last

    pl.semaphore_wait(barrier, R - 1 + Y - 1 + Z - 1)
    for d in range(1, Y):
        remote(rs_send.at[yat(d)], rs_y.at[d - 1], rs_ssem.at[0], rs_rsem, z * Y + yat(d), row).start()
    for d in range(1, R):
        remote(cs_send, cs_row.at[row], cs_ssem.at[0], cs_rsem.at[0], col, lax.rem(row + d, R)).start()
    for d in range(1, Y):
        remote(item_ref, ei_pan.at[0, c, spot], ei_ssem, ei_rsem.at[0, 0], z * Y + yat(d), row).start()
    send_mask(0)
    begin0, hop0, last0 = gather_user(0)
    begin0(user_ref[...])
    send_mask(1)

    usum[...] = user_ref[...].astype(F32)
    isum[...] = item_ref[...].astype(F32)
    wait_bytes(rs_y, rs_rsem)
    rs_z[z] = rs_send[y] + rs_y[0] + rs_y[1] + rs_y[2]
    for d in (4, 3, 5, 2, 6, 1, 7):
        remote(rs_z.at[z], rs_z.at[z], rs_ssem.at[1], rz_rsem, zat(d) * Y + y, row).start()

    wait_bytes(ei_pan.at[0, c, pl.ds(0, Y - 1)], ei_rsem.at[0, 0])
    own = ei_pan.at[0, c, pl.ds(x * Y, Y)]
    for d in range(1, X):
        remote(own, own, ei_ssem, ei_rsem.at[0, d], col, xat(d) * 2 + c).start()
    remote(own, own, fw_ssem, fw_rsem.at[0, 0], col, partner).start()

    wait_bytes(cs_row.at[pl.ds(0, R - 1)], cs_rsem.at[0])
    deg = cs_row[0]
    for r in range(1, R):
        deg = deg + cs_row[r]
    cs_y[y] = deg
    for d in range(1, Y):
        remote(cs_y.at[y], cs_y.at[y], cs_ssem.at[1], cs_rsem.at[1], z * Y + yat(d), row).start()
    for j in range(2, Z):
        send_mask(j)

    base = (row * (Z * Y) + col) * UB
    ids = lax.broadcasted_iota(jnp.int32, (UB, NQ), 0) + base
    hot[...] = jnp.where(ids == query_ref[...], 1.0, 0.0).T.astype(BF16)

    hop0(0)
    for d in (1, 3, 2):
        rows = pl.ds(xat(-d) * Y, Y)
        wait_bytes(ei_pan.at[0, c, rows], ei_rsem.at[0, d])
        remote(ei_pan.at[0, c, rows], ei_pan.at[0, c, rows], fw_ssem, fw_rsem.at[0, d], col, partner).start()
    wait_bytes(cs_y.at[pl.ds(0, Y - 1)], cs_rsem.at[1])
    for s in range(Y):
        invi[s] = lax.rsqrt(jnp.maximum(cs_y[s], 1.0))
    wait_bytes(rs_z.at[pl.ds(0, Z - 1)], rz_rsem)
    deg = rs_z[0]
    for d in range(1, Z):
        deg = deg + rs_z[d]
    invu[...] = lax.rsqrt(jnp.maximum(deg, 1.0))

    def make_adj(j, zc):
        wait_bytes(mrecv.at[j], mask_rsem.at[j])
        iu = jnp.broadcast_to(invu[pl.ds(zc, 1), :], (UB, UB)).T
        iu = jnp.concatenate([iu, iu], axis=1)
        for d in range(Y):
            s = yat(-d)
            m = (msend[y, j] if d == 0 else mrecv[j, d - 1]).astype(F32)
            a = (iu * m) * invi[s]
            adj[s, zc] = a.astype(BF16)
            adjt[s, :, pl.ds(pl.multiple_of(zc * UB, UB), UB)] = a.T.astype(BF16)

    def user_piece(k, j):
        zc = zat(order[j])
        if k == 0:
            make_adj(j, zc)
        acc = None
        for s in range(Y):
            panel = jnp.concatenate([ei_pan[k, cc, xx * Y + s] for xx in range(X) for cc in range(2)], axis=0)
            t = jnp.dot(adj[s, zc], panel, preferred_element_type=F32)
            acc = t if acc is None else acc + t
        up[j] = acc

    def item_share(k, product, lag=Y):
        for j, dy in enumerate((2, 1, 3, 0)):
            s = yat(dy)
            part = product(s).reshape(X, 2, IB, E)
            for xx in range(X):
                for cc in range(2):
                    ip[k, cc, s * X + xx] = part[xx, cc]
            remote(ip.at[k, other, pl.ds(s * X, X)], pr.at[k, j], pr_ssem, pr_rsem.at[k % 2, j], col, partner).start()
            if j >= lag:
                item_send(k, j - lag)

    def item_parts(k):
        eu = eu_pan[k].reshape(Z * UB, E)
        item_share(k, lambda s: jnp.dot(adjt[s], eu, preferred_element_type=F32), lag=3)

    pairs = (((4, 3), (-3, 2), (-2, 1), (-1, 0)), ((0, 1), (-1, 2), (-2, 3), (-3, 4)))

    def item_pair(k, n):
        near = [zat(d) for d in pairs[k][n]]
        eu = jnp.concatenate([eu_pan[k, zc] for zc in near], axis=0)

        def add(s):
            lhs = jnp.concatenate([adjt[s, :, pl.ds(pl.multiple_of(zc * UB, UB), UB)] for zc in near], axis=1)
            part = jnp.dot(lhs, eu, preferred_element_type=F32)
            return part + macc[s] if n else part

        if n < 3:
            for s in range(Y):
                macc[s] = add(s)
        else:
            item_share(k, add)

    def item_send(k, j):
        dy = (2, 1, 3, 0)[j]
        s = yat(dy)
        wait_bytes(pr.at[k, j], pr_rsem.at[k % 2, j])
        iq[k, pl.ds(s * X, X)] = ip[k, c, pl.ds(s * X, X)] + pr[k, j]
        for dx in (2, 1, 3, 0):
            if dy or dx:
                px = xat(dx)
                remote(iq.at[k, s * X + px], ir.at[k, dy * X + dx - 1], ip_ssem, ip_rsem.at[k],
                       z * Y + s, px * 2 + c).start()

    def items_send(k, first=0):
        for j in range(first, Y):
            item_send(k, j)

    def item_total(k):
        wait_bytes(ir.at[k], ip_rsem.at[k])
        total = iq[k, y * X + x]
        for slot in range(G // 2 - 1):
            total = total + ir[k, slot]
        return total

    def gather_plane(pan, ssem, rsem):
        for slot, dx, py, px in plane():
            remote(pan.at[c, spot], pan.at[c, spot], ssem, rsem.at[dx], z * Y + py, px * 2 + c).start()

    def forward_plane(pan, rsem, fssem, frsem, dst):
        for dx in (0, 1, 3, 2):
            rows = pl.ds(xat(-dx) * Y, Y)
            wait_bytes(pan.at[c, pl.ds(0, Y if dx else Y - 1)], rsem.at[dx])
            remote(pan.at[c, rows], dst.at[c, rows], fssem, frsem.at[dx], col, partner).start()

    def wait_plane(pan, frsem):
        for dx in (0, 1, 3, 2):
            wait_bytes(pan.at[other, pl.ds(xat(-dx) * Y, Y)], frsem.at[dx])

    def user_total(k, hooks):
        def emit(way, step, h, first=False):
            rows = pl.ds(h * H, H)
            j = piece_of[4 - step] if way == 0 or step == 0 else piece_of[step - 4]
            value = up[j, h * H:(h + 1) * H]
            if not first:
                value = value + got(way, step - 1, h)
            us[k, way, step, h * H:(h + 1) * H] = value
            remote(us.at[k, way, step, rows], ur.at[k, way, step, rows], us_ssem.at[k], us_rsem.at[way, step, h],
                   right if way == 0 else left, row).start()

        def got(way, step, h):
            wait_bytes(ur.at[k, way, step, pl.ds(h * H, H)], us_rsem.at[way, step, h])
            return ur[k, way, step, h * H:(h + 1) * H]

        def hook(*at):
            if at in hooks:
                hooks[at]()

        user_piece(k, 0)
        for h in range(NH // 2):
            emit(0, 0, early[0][h], True)
            emit(1, 0, early[1][h], True)
        if k == 0:
            hook('piece', 0)
            for step in range(1, 4):
                for way in range(2):
                    user_piece(k, 2 * step - 1 + way)
                    for h in early[way] + late[way]:
                        emit(way, step, h, step == 1 and h in late[way])
                hook('piece', step)
            user_piece(k, 7)
            hook('own')
        else:
            for way in range(2):
                user_piece(k, 1 + way)
                for h in late[way]:
                    emit(way, 1, h, True)
            for step in range(1, 4):
                hook('before', step)
                if step < 3:
                    user_piece(k, 2 * step + 1)
                    user_piece(k, 2 * step + 2)
                else:
                    user_piece(k, 7)
                def run(groups):
                    for ways in groups:
                        for h in range(NH // 2):
                            for way in ways:
                                emit(way, step, early[way][h])
                        for h in range(NH // 2):
                            for way in ways:
                                if step < 3:
                                    emit(way, step + 1, late[way][h])

                ring_order(step - 1, run)
                hook('after', step)
        parts = []
        for h in range(NH):
            parts.append(up[7, h * H:(h + 1) * H] + got(0, 3, h) + got(1, 3, h))
        new_user = jnp.concatenate(parts, axis=0).astype(BF16)
        usum[...] += new_user.astype(F32)
        return new_user

    def items_next(k):
        new_item = item_total(k).astype(BF16)
        isum[...] += new_item.astype(F32)
        ei_pan[k + 1, c, spot] = new_item
        gather_plane(ei_pan.at[k + 1], ei_ssem, ei_rsem.at[(k + 1) % 2])

    def items_forward(k):
        forward_plane(ei_pan.at[k], ei_rsem.at[k % 2], fw_ssem, fw_rsem.at[k % 2], ei_pan.at[k])

    def items_wait(k):
        wait_plane(ei_pan.at[k], fw_rsem.at[k % 2])

    hop0(1)
    items_wait(0)

    new_user = user_total(0, {('piece', 0): lambda: hop0(2), ('piece', 1): last0, ('own',): lambda: (item_parts(0), items_send(0, 1))})
    begin1, hop1, last1 = gather_user(1)
    begin1(new_user)
    hop1(0)
    item_pair(1, 0)
    hop1(1)
    item_pair(1, 1)
    items_next(0)
    hop1(2)
    item_pair(1, 2)
    last1()
    item_pair(1, 3)
    items_forward(1)
    items_send(1)
    items_wait(1)
    new_user = user_total(1, {('after', 2): lambda: items_next(1)})
    begin2, hop2, last2 = gather_user(2)
    begin2(new_user)
    items_forward(2)
    items_wait(2)

    user_total(2, {('after', 2): lambda: hop2(0), ('after', 3): lambda: hop2(1)})
    final_user = (usum[...] / (LAYERS + 1)).astype(BF16)
    fu_v[...] = final_user
    outs = [pltpu.make_async_copy(fu_v, fu_out, out_sem.at[0])]
    outs[0].start()

    qs[...] = jnp.dot(hot[...], final_user, preferred_element_type=F32).astype(BF16).reshape(2, G // 2, QB, E)
    to_partner = remote(qs.at[other], qp, q_ssem.at[0], q_rsem.at[0], col, partner)
    to_partner.start()
    hop2(2)
    to_partner.wait_recv()
    qt[...] = (qs[c].astype(F32) + qp[...].astype(F32)).astype(BF16)
    for slot, dx, py, px in plane():
        remote(qt.at[px * Y + py], qr.at[slot], q_ssem.at[1], q_rsem.at[1], z * Y + py, px * 2 + c).start()
    last2()
    item_parts(2)
    items_send(2, 1)
    wait_bytes(qr, q_rsem.at[1])
    total = qt[spot].astype(F32)
    for slot in range(G // 2 - 1):
        total = total + qr[slot].astype(F32)
    qzs[...] = total.astype(BF16)
    for t in (0, 1, 7, 2, 6, 3, 5, 4):
        def to_plane(t=t):
            remote(qzs, qz.at[lax.rem(t - z + Z, Z) - 1], q_ssem.at[2], q_rsem.at[2], t * Y + y, row).start()
        pl.when(z != t)(to_plane)
    wait_bytes(qz, q_rsem.at[2])
    for d in range(Z - 1):
        total = total + qz[d].astype(F32)
    qall[c, spot] = total.astype(BF16)
    gather_plane(qall, q_ssem.at[3], qg_rsem)
    new_item = item_total(2).astype(BF16)
    fi_v[...] = ((isum[...] + new_item.astype(F32)) / (LAYERS + 1)).astype(BF16)
    outs.append(pltpu.make_async_copy(fi_v, fi_out, out_sem.at[1]))
    outs[1].start()
    forward_plane(qall, qg_rsem, q_ssem.at[4], qf_rsem, q_out)
    outs.append(pltpu.make_async_copy(qall.at[c], q_out.at[c], out_sem.at[2]))
    outs[2].start()
    wait_plane(q_out, qf_rsem)

    wait_bytes(rs_y, rs_ssem.at[0])
    wait_bytes(rs_z.at[pl.ds(0, Z - 1)], rs_ssem.at[1])
    wait_bytes(cs_row.at[pl.ds(0, R - 1)], cs_ssem.at[0])
    wait_bytes(cs_y.at[pl.ds(0, Y - 1)], cs_ssem.at[1])
    wait_bytes(msend.at[pl.ds(0, Y - 1)], mask_ssem)
    wait_bytes(ei_pan.at[:, 0, pl.ds(0, G // 2 - 1)], ei_ssem)
    wait_bytes(ei_pan.at[:, 0], fw_ssem)
    wait_bytes(pr, pr_ssem)
    wait_bytes(ir, ip_ssem)
    wait_bytes(eu_pan.at[:, pl.ds(0, 7)], ag_ssem)
    for k in range(LAYERS):
        wait_bytes(up.at[pl.ds(0, 7)], us_ssem.at[k])
    to_partner.wait_send()
    wait_bytes(qr, q_ssem.at[1])
    wait_bytes(qz, q_ssem.at[2])
    wait_bytes(qr, q_ssem.at[3])
    wait_bytes(qt, q_ssem.at[4])
    for out in outs:
        out.wait()


def finish(user_ref, item_ref, picked_ref, fu_ref, fi_ref, sc_ref):
    fu_ref[...] = user_ref[...]
    fi_ref[...] = item_ref[...]
    sc_ref[...] = lax.dot_general(item_ref[...], picked_ref[...], CONTRACT_LANES, preferred_element_type=F32)


def propagate(mask, user, item, queries):
    dma = pltpu.SemaphoreType.DMA
    vmem, free = pl.BlockSpec(memory_space=pltpu.VMEM), pl.BlockSpec(memory_space=pl.ANY)
    L, N = LAYERS, G // 2
    final_user, final_item, picked = pl.pallas_call(
        kernel,
        out_shape=(jax.ShapeDtypeStruct((UB, E), BF16), jax.ShapeDtypeStruct((IB, E), BF16),
                   jax.ShapeDtypeStruct((2, N, QB, E), BF16)),
        in_specs=[pl.BlockSpec(memory_space=pltpu.HBM)] * 4,
        out_specs=(free, free, free),
        scratch_shapes=[
            pltpu.VMEM((Z, Y * UB, E), jnp.int32),
            pltpu.VMEM((UB, E), BF16),
            pltpu.VMEM((IB, E), BF16),
            pltpu.VMEM((1, NQ), jnp.int32),
            pltpu.VMEM((Y, Z, UB, E), BF16),
            pltpu.VMEM((Z, Y - 1, UB, E), BF16),
            pltpu.VMEM((Y, Z, UB, E), BF16),
            pltpu.VMEM((Y, E, Z * UB), BF16),
            pltpu.VMEM((Y, Z, UB), F32),
            pltpu.VMEM((Y - 1, Z, UB), F32),
            pltpu.VMEM((Z, Z, UB), F32),
            pltpu.VMEM((1, E), F32),
            pltpu.VMEM((R, 1, E), F32),
            pltpu.VMEM((Y, 1, E), F32),
            pltpu.VMEM((Z, UB), F32),
            pltpu.VMEM((Y, 1, E), F32),
            pltpu.VMEM((L, Z, UB, E), BF16),
            pltpu.VMEM((L, 2, N, IB, E), BF16),
            pltpu.VMEM((Z, UB, E), F32),
            pltpu.VMEM((Y, E, E), F32),
            pltpu.VMEM((L, 2, 4, UB, E), F32),
            pltpu.VMEM((L, 2, 4, UB, E), F32),
            pltpu.VMEM((L, 2, N, IB, E), F32),
            pltpu.VMEM((L, Y, X, IB, E), F32),
            pltpu.VMEM((L, N, IB, E), F32),
            pltpu.VMEM((L, N - 1, IB, E), F32),
            pltpu.VMEM((NQ, UB), BF16),
            pltpu.VMEM((2, N, QB, E), BF16),
            pltpu.VMEM((N, QB, E), BF16),
            pltpu.VMEM((N, QB, E), BF16),
            pltpu.VMEM((N - 1, QB, E), BF16),
            pltpu.VMEM((Z - 1, QB, E), BF16),
            pltpu.VMEM((QB, E), BF16),
            pltpu.VMEM((2, N, QB, E), BF16),
            pltpu.VMEM((UB, E), BF16),
            pltpu.VMEM((IB, E), BF16),
            pltpu.VMEM((UB, E), F32),
            pltpu.VMEM((IB, E), F32),
            dma((Z + 3,)), dma, dma((Z,)),
            dma((2,)), dma, dma,
            dma((2,)), dma((2,)),
            dma, dma((2, X)), dma, dma((2, X)),
            dma((L,)), dma((2, 4, NH)),
            dma, dma((2, Y)), dma, dma((L,)),
            dma, dma((2, 4, NH)),
            dma((5,)), dma((3,)), dma((X,)), dma((X,)),
            dma((3,)),
        ],
        compiler_params=pltpu.CompilerParams(collective_id=0, has_side_effects=True, vmem_limit_bytes=50 * 2**20),
    )(*(pltpu.with_memory_space_constraint(a, pltpu.HBM) for a in (mask, user, item, queries.reshape(1, NQ))))
    final_user, final_item, scores = pl.pallas_call(
        finish,
        out_shape=(jax.ShapeDtypeStruct((UB, E), BF16), jax.ShapeDtypeStruct((IB, E), BF16),
                   jax.ShapeDtypeStruct((IB, NQ), F32)),
        in_specs=[vmem, vmem, vmem],
        out_specs=(vmem, vmem, vmem),
        compiler_params=pltpu.CompilerParams(vmem_limit_bytes=8 * 2**20),
    )(final_user, final_item, picked.reshape(NQ, E))
    return final_user, final_item, scores.T


def solution(mesh):
    return jax.shard_map(propagate, mesh=mesh,
                         in_specs=(P('row', 'col'), P(('row', 'col'), None), P(('col', 'row'), None), P()),
                         out_specs=(P(('row', 'col'), None), P(('col', 'row'), None), P(None, ('col', 'row'))),
                         check_vma=False)
```
